512 devices in a mesh: grp: 2 (over core), gx: 16 (over x, z_lo), gy: 16 (over z_hi, y).
Axes of the slice: x: 4, y: 8, z: 8 (z_hi: 2, z_lo: 4; z = z_hi * 4 + z_lo), core: 2. Of those that a mesh axis runs over, the one named last changes fastest.
Arguments:
- coarse_density: float32 [512, 512, 512], P('gx', ('grp', 'gy')), may hold values from -3 to 3
- fine_density: float32 [128, 512, 256], P('gx', 'gy', 'grp'), may hold values from -96 to 96
- fine_start: float32 [128, 512, 256], P('gx', 'gy', 'grp'), may hold values from -6 to 6
- anchor: int32 [3], replicated, may hold values from 1 to 383
Outputs:
- coarse_potential: float32 [512, 512, 512], P('gx', ('grp', 'gy'))
- fine_potential: float32 [128, 512, 256], P('gx', 'gy', 'grp')
The draws below stay inside these ranges and needn't reach their ends.
Inputs may be any that keep to these rules, and one draw needn't show every extreme that they name: Along every dimension d the coarse cells anchor[d] - 1 up to anchor[d] + (fine cells along d) / 4 lie inside the coarse grid.
All inputs are finite; a program needn't handle non-finite values.
Results may differ from the reference program's by a relative error of at most 0.00015.
Values sent between devices are 32-bit elements; how exact they have to be, the bound alone decides.
A program may use at most 64 MiB of HBM per device.

```python
import math
import jax
import jax.numpy as jnp
from jax import lax

NC = 512
RATIO = 4
SWEEPS = 8
FX = 128
FY = 512
FZ = 256
CBX = 34
CBY = 130
CBZ = 66


def block_levels(rng, shape, pieces, low, high):
    def one(dim, parts):
        steps = jax.random.uniform(jax.random.fold_in(jax.random.fold_in(rng, 6), dim), (parts,), jnp.float32, low / len(pieces), high / len(pieces))
        return jnp.repeat(jnp.exp(steps), shape[dim] // parts).reshape((-1,) + (1,) * (len(shape) - dim - 1))

    factor_of = one(*pieces[0])
    for cut in pieces[1:]:
        factor_of = factor_of * one(*cut)
    return factor_of


def gaussian(key, extent, width, reach, cuts=(), kind=jnp.bfloat16):
    values = width * jax.random.normal(key, extent, jnp.float32)
    if cuts:
        values = values * block_levels(key, extent, cuts, -0.22, 0.18)
    return jnp.clip(values, -reach, reach).astype(kind)


def setup_inputs(seed: int = 0) -> dict:
    key_list = jax.random.split(jax.random.key(seed), 5)
    coarse_density = gaussian(key_list[0], (NC, NC, NC), 0.5, 3.0, ((0, 16), (1, 32)), jnp.float32)
    fine_density = gaussian(key_list[1], (FX, FY, FZ), 16.0, 96.0, ((0, 16), (1, 16), (2, 2)), jnp.float32)
    fine_start = gaussian(key_list[2], (FX, FY, FZ), 1.0, 6.0, ((0, 16), (1, 16), (2, 2)), jnp.float32)
    anchor = jax.random.randint(key_list[3], (3,), 1, NC - max(FX, max(FY, FZ)) // RATIO).astype(jnp.int32)
    return dict(coarse_density=coarse_density, fine_density=fine_density, fine_start=fine_start, anchor=anchor)


highest = lax.Precision.HIGHEST

def sine_table(amount):
    indices = jnp.arange(amount, dtype=jnp.int32) + 1
    product = indices[:, None] * indices[None, :] % (2 * (amount + 1))
    angles = product.astype(jnp.float32) * (math.pi / (amount + 1))
    return math.sqrt(2.0 / (amount + 1)) * jnp.sin(angles)

def eigen_values(indices, amount):
    angles = (indices + 1).astype(jnp.float32) * (math.pi / (2 * (amount + 1)))
    return -4.0 * jnp.square(jnp.sin(angles))

def interpolation(fine_index, cell_count):
    scaled = 2 * fine_index + 1 + RATIO
    bottom = scaled // (2 * RATIO)
    weight = (scaled % (2 * RATIO)).astype(jnp.float32) / (2.0 * RATIO)
    column = jnp.arange(cell_count, dtype=jnp.int32)
    first_part = jnp.where(column[None, :] == bottom[:, None], 1.0 - weight[:, None], 0.0)
    second_part = jnp.where(column[None, :] == bottom[:, None] + 1, weight[:, None], 0.0)
    return first_part + second_part

def transform(values, matrix):
    values = jnp.einsum('abc,cd->abd', values, matrix, precision=highest)
    values = jnp.einsum('abc,bd->adc', values, matrix, precision=highest)
    return jnp.einsum('abc,ad->dbc', values, matrix, precision=highest)

def ghost_values(face, left_matrix, right_matrix):
    partial_value = jnp.einsum('fbc,kc->fbk', face, right_matrix, precision=highest)
    return jnp.einsum('fbk,jb->fjk', partial_value, left_matrix, precision=highest)

def reference(coarse_density, fine_density, fine_start, anchor):
    matrix = sine_table(NC)
    eigen_list = eigen_values(jnp.arange(NC, dtype=jnp.int32), NC)
    spectrum = transform(coarse_density, matrix)
    divisor = eigen_list[:, None, None] + eigen_list[None, :, None] + eigen_list[None, None, :]
    potential = transform(spectrum / divisor, matrix)
    coarse_box = lax.dynamic_slice(potential, (anchor[0] - 1, anchor[1] - 1, anchor[2] - 1), (CBX, CBY, CBZ))
    ends_x = interpolation(jnp.array([-1, FX], dtype=jnp.int32), CBX)
    ends_y = interpolation(jnp.array([-1, FY], dtype=jnp.int32), CBY)
    ends_z = interpolation(jnp.array([-1, FZ], dtype=jnp.int32), CBZ)
    inner_x = interpolation(jnp.arange(FX, dtype=jnp.int32), CBX)
    inner_y = interpolation(jnp.arange(FY, dtype=jnp.int32), CBY)
    inner_z = interpolation(jnp.arange(FZ, dtype=jnp.int32), CBZ)
    face_x = jnp.einsum('fa,abc->fbc', ends_x, coarse_box, precision=highest)
    face_y = jnp.einsum('fb,abc->fac', ends_y, coarse_box, precision=highest)
    face_z = jnp.einsum('fc,abc->fab', ends_z, coarse_box, precision=highest)
    ghost_x = ghost_values(face_x, inner_y, inner_z)
    ghost_y = ghost_values(face_y, inner_x, inner_z)
    ghost_z = ghost_values(face_z, inner_x, inner_y)
    padded = jnp.zeros((FX + 2, FY + 2, FZ + 2), jnp.float32)
    padded = padded.at[1:-1, 1:-1, 1:-1].set(fine_start)
    padded = padded.at[0, 1:-1, 1:-1].set(ghost_x[0]).at[-1, 1:-1, 1:-1].set(ghost_x[1])
    padded = padded.at[1:-1, 0, 1:-1].set(ghost_y[0]).at[1:-1, -1, 1:-1].set(ghost_y[1])
    padded = padded.at[1:-1, 1:-1, 0].set(ghost_z[0]).at[1:-1, 1:-1, -1].set(ghost_z[1])
    source = fine_density / (RATIO * RATIO)
    for sweep in range(SWEEPS):
        summed = padded[2:, 1:-1, 1:-1] + padded[:-2, 1:-1, 1:-1]
        summed = summed + padded[1:-1, 2:, 1:-1] + padded[1:-1, :-2, 1:-1]
        summed = summed + padded[1:-1, 1:-1, 2:] + padded[1:-1, 1:-1, :-2]
        padded = padded.at[1:-1, 1:-1, 1:-1].set((summed - source) / 6.0)
    return (potential, padded[1:-1, 1:-1, 1:-1])
```

```python
import functools
import math

import jax
import jax.numpy as jnp
import numpy as np
from jax import lax
from jax.experimental import pallas as pl
from jax.experimental.pallas import tpu as pltpu
from jax.sharding import PartitionSpec as P

MESH = pl.DeviceIdType.MESH
NC = 512
F32 = jnp.float32
BF16 = jnp.bfloat16


def tables():
    index = np.arange(1, NC + 1, dtype=np.int64)
    angle = (index[:, None] * index[None, :]) % (2 * (NC + 1))
    sine = math.sqrt(2.0 / (NC + 1)) * np.sin(angle * (math.pi / (NC + 1)))
    sine = sine.astype(np.float32)
    high = sine.astype(jnp.bfloat16)
    low = (sine - high.astype(np.float32)).astype(jnp.bfloat16)
    lam = 4.0 * np.sin(index * (math.pi / (2 * (NC + 1)))) ** 2
    return high, low, lam.astype(np.float32)


def split(value):
    high = value.astype(BF16)
    low = (value - high.astype(F32)).astype(BF16)
    return high, low


def dot3(a, b, dims):
    ah, al = a
    bh, bl = b
    dd = functools.partial(
        lax.dot_general, dimension_numbers=(dims, ((), ())), preferred_element_type=F32
    )
    return dd(ah, bh) + (dd(al, bh) + dd(ah, bl))


NN = ((1,), (0,))
NT = ((1,), (1,))
TN = ((0,), (0,))


def swap_groups(source, target):
    lane = lax.broadcasted_iota(jnp.int32, (8, 128), 1) // 16

    def step(index, carry):
        at = index // 8
        bt = (index // 2) % 4
        row = pl.multiple_of((index % 2) * 8, 8)
        cols = pl.ds(pl.multiple_of(bt * 128, 128), 128)
        outs = pl.ds(pl.multiple_of(at * 128, 128), 128)
        v = [source[at * 8 + q, pl.ds(row, 8), cols] for q in range(8)]
        for bit in (1, 2, 4):
            upper = (lane & bit) != 0
            for i in range(8):
                if i & bit:
                    continue
                a, c = v[i], v[i | bit]
                v[i] = jnp.where(upper, pltpu.roll(c, 16 * bit, 1), a)
                v[i | bit] = jnp.where(upper, c, pltpu.roll(a, 128 - 16 * bit, 1))
        for q in range(8):
            target[bt * 8 + q, pl.ds(row, 8), outs] = v[q]
        return carry

    lax.fori_loop(0, 32, step, 0)


def device(core, x, y, z):
    return (core, x * 4 + z % 4, (z // 4) * 8 + y)


ORDER = [
    (dy, side, core) for dy in (4, 3, 5, 2, 6, 1, 7, 0) for side in (0, 1) for core in (0, 1)
]


def shuffled():
    return list(ORDER[i] for i in np.random.RandomState(3).permutation(len(ORDER)))


def coarse_kernel(
    x_ref, sh_ref, sl_ref, lamr_ref, lamc_ref, lamq_ref, out_ref,
    za, zb, dd, u, dtab, m1, r1, m2, r2, dint,
    s1, q1, s2, q2, s3, q3, s4, q4,
):
    core = lax.axis_index("grp")
    gx = lax.axis_index("gx")
    gy = lax.axis_index("gy")
    x, zl = gx // 4, gx % 4
    y, zh = gy % 8, gy // 8
    z = zh * 4 + zl
    me = core * 16 + gy
    zv = (z + 6) % 8
    lv, hv = zv % 4, zv // 4
    mid = core * 16 + hv * 8 + y
    pv = x * 4 + lv

    def to_mid(o):
        dy, side, oc = o
        ty = (y + dy) % 8
        tc = (core + oc) % 2
        return device(tc, x, ty, (zl + 4 * side + 2) % 8), tc * 16 + side * 8 + ty

    def to_real(o):
        dy, side, oc = o
        ty = (y + dy) % 8
        tc = (core + oc) % 2
        return device(tc, x, ty, lv + 4 * side), tc * 16 + side * 8 + ty

    def to_row(q):
        return device(core, q // 4, y, (q % 4 + 4 * hv + 2) % 8)

    barrier = pltpu.get_barrier_semaphore()
    peers = shuffled()
    for o in peers:
        pl.semaphore_signal(barrier, inc=1, device_id=to_mid(o)[0], device_id_type=MESH)
    for k in range(1, 16):
        pl.semaphore_signal(barrier, inc=1, device_id=to_row((pv + k) % 16), device_id_type=MESH)

    s_pair = (sh_ref[...], sl_ref[...])
    value = x_ref[...].reshape(512, 512)
    za[...] = dot3(split(value), s_pair, NN).reshape(32, 16, 512)
    swap_groups(za, zb)

    pl.semaphore_wait(barrier, 47)

    t1 = []
    for i, o in enumerate(peers):
        target, block = to_mid(o)
        copy = pltpu.make_async_remote_copy(
            src_ref=zb.at[block], dst_ref=dd.at[me], send_sem=s1.at[i], recv_sem=q1.at[me],
            device_id=target, device_id_type=MESH,
        )
        copy.start()
        t1.append(copy)

    mu = lamr_ref[...] + lamc_ref[pl.ds(pl.multiple_of(mid * 16, 16), 16), :]

    def table(i, g):
        d = 1.0 / (1.0 + (mu + g))
        dtab[i] = d
        return (mu + g) * d

    lax.fori_loop(0, 31, table, jnp.ones((16, 512), F32))
    muq = lamq_ref[...] + lamc_ref[pl.ds(mid * 16 + pv, 1), :]
    c = 0.5 * muq
    c1 = c
    r32 = 2.0 * (1.0 + c)
    for _ in range(4):
        c = 2.0 * c * (c + 2.0)
        r32 = r32 * (2.0 * (1.0 + c))
    c = 2.0 * c * (c + 2.0)
    g = jnp.ones((4, 128), F32)
    for i in range(15):
        d = 1.0 / (1.0 + (2.0 * c + g))
        dint[i] = d
        g = (2.0 * c + g) * d
    dint[15] = 1.0 / (r32 * (1.0 + c1) + c + g)

    for s in range(32):
        pltpu.make_async_remote_copy(
            src_ref=dd.at[s], dst_ref=dd.at[s], send_sem=s1.at[s], recv_sem=q1.at[s],
            device_id=(core, gx, gy), device_id_type=MESH,
        ).wait_recv()

    value = dd[...].reshape(512, 512)
    u[...] = dot3(split(value), s_pair, TN).reshape(32, 16, 512)

    first = -u[0]
    u[0] = first
    q0 = dtab[30]

    def forward(i, carry):
        yv, q, e = carry
        w = u[i]
        yv = dtab[i - 1] * yv - w
        u[i] = yv
        q = q * dtab[30 - i]
        return yv, q, e - q * w

    yv, _, e = lax.fori_loop(1, 31, forward, (first, q0, q0 * first))
    b = q0 * yv - u[31]
    for j in range(4):
        m1[pl.ds(j, 16, stride=8), :] = e[:, 128 * j : 128 * j + 128]
        m1[pl.ds(4 + j, 16, stride=8), :] = b[:, 128 * j : 128 * j + 128]
    t2 = []
    for k in range(1, 16):
        q = (pv + k) % 16
        copy = pltpu.make_async_remote_copy(
            src_ref=m1.at[pl.ds(pl.multiple_of(q * 8, 8), 8), :], dst_ref=r1.at[pv],
            send_sem=s2.at[k], recv_sem=q2.at[pv], device_id=to_row(q), device_id_type=MESH,
        )
        copy.start()
        t2.append(copy)
    r1[pv] = m1[pl.ds(pl.multiple_of(pv * 8, 8), 8), :]
    for k in range(1, 16):
        q = (pv + k) % 16
        pltpu.make_async_remote_copy(
            src_ref=r1.at[q], dst_ref=r1.at[q], send_sem=s2.at[k], recv_sem=q2.at[q],
            device_id=(core, gx, gy), device_id_type=MESH,
        ).wait_recv()
    ys = []
    prev = None
    for p in range(16):
        h = r1[p, 4:8, :]
        if p < 15:
            h = h + r1[p + 1, 0:4, :]
        h = r32 * h
        prev = h if p == 0 else h + dint[p - 1] * prev
        ys.append(prev)
    sol = [None] * 16
    sol[15] = dint[15] * ys[15]
    for p in range(14, -1, -1):
        sol[p] = dint[p] * (sol[p + 1] + ys[p])
    for p in range(16):
        m2[p, 0:4, :] = sol[p - 1] if p else jnp.zeros((4, 128), F32)
        m2[p, 4:8, :] = sol[p]
    t3 = []
    for k in range(1, 16):
        q = (pv + k) % 16
        copy = pltpu.make_async_remote_copy(
            src_ref=m2.at[q], dst_ref=r2.at[pl.ds(pl.multiple_of(pv * 8, 8), 8), :],
            send_sem=s3.at[k], recv_sem=q3.at[pv], device_id=to_row(q), device_id_type=MESH,
        )
        copy.start()
        t3.append(copy)
    r2[pl.ds(pl.multiple_of(pv * 8, 8), 8), :] = m2[pv]
    for k in range(1, 16):
        q = (pv + k) % 16
        view = r2.at[pl.ds(pl.multiple_of(q * 8, 8), 8), :]
        pltpu.make_async_remote_copy(
            src_ref=view, dst_ref=view, send_sem=s3.at[k], recv_sem=q3.at[q],
            device_id=(core, gx, gy), device_id_type=MESH,
        ).wait_recv()
    left = jnp.concatenate([r2[pl.ds(j, 16, stride=8), :] for j in range(4)], axis=1)
    right = jnp.concatenate([r2[pl.ds(4 + j, 16, stride=8), :] for j in range(4)], axis=1)

    def spread(i, t):
        u[i] = u[i] + t
        return dtab[i] * t

    lax.fori_loop(0, 31, spread, left)
    u[31] = right

    def backward(k, v):
        i = 30 - k
        v = dtab[i] * (v + u[i])
        u[i] = v
        return v

    lax.fori_loop(0, 31, backward, right)

    for copy in t1:
        copy.wait_send()
    value = u[...].reshape(512, 512)
    zb[...] = dot3(s_pair, split(value), NT).reshape(32, 16, 512)
    t4 = []
    for i, o in enumerate(peers):
        target, block = to_real(o)
        copy = pltpu.make_async_remote_copy(
            src_ref=zb.at[block], dst_ref=za.at[mid], send_sem=s4.at[i], recv_sem=q4.at[mid],
            device_id=target, device_id_type=MESH,
        )
        copy.start()
        t4.append(copy)
    for s in range(32):
        pltpu.make_async_remote_copy(
            src_ref=za.at[s], dst_ref=za.at[s], send_sem=s4.at[s], recv_sem=q4.at[s],
            device_id=(core, gx, gy), device_id_type=MESH,
        ).wait_recv()
    swap_groups(za, dd)
    value = dd[...].reshape(512, 512)
    out_ref[...] = dot3(split(value), s_pair, NN).reshape(32, 16, 512)
    for copy in t2 + t3 + t4:
        copy.wait_send()


def coarse(density):
    high, low, lam = tables()
    vm = pl.BlockSpec(memory_space=pltpu.VMEM)
    big = pltpu.VMEM((32, 16, 512), F32)
    dma = pltpu.SemaphoreType.DMA
    return pl.pallas_call(
        coarse_kernel,
        out_shape=jax.ShapeDtypeStruct((32, 16, 512), F32),
        in_specs=[vm] * 6,
        out_specs=vm,
        scratch_shapes=[
            big, big, big, big, pltpu.VMEM((31, 16, 512), F32),
            pltpu.VMEM((128, 128), F32), pltpu.VMEM((16, 8, 128), F32),
            pltpu.VMEM((16, 8, 128), F32), pltpu.VMEM((128, 128), F32),
            pltpu.VMEM((16, 4, 128), F32),
            dma((32,)), dma((32,)), dma((16,)), dma((16,)), dma((16,)), dma((16,)),
            dma((32,)), dma((32,)),
        ],
        compiler_params=pltpu.CompilerParams(
            collective_id=0, has_side_effects=True, vmem_limit_bytes=40 << 20
        ),
    )(density, jnp.asarray(high), jnp.asarray(low), jnp.asarray(lam.reshape(1, 512)),
      jnp.asarray(lam.reshape(512, 1)), jnp.asarray(lam.reshape(4, 128)))


RATIO = 4
SWEEPS = 8


highest = lax.Precision.HIGHEST


def with_halo(block, sides, width):
    for axis, dim in sides:
        count = lax.axis_size(axis)
        forward = [(i, i + 1) for i in range(count - 1)]
        backward = [(target, source) for source, target in forward]
        low = lax.ppermute(
            lax.slice_in_dim(block, block.shape[dim] - width, None, axis=dim), axis, forward
        )
        high = lax.ppermute(lax.slice_in_dim(block, 0, width, axis=dim), axis, backward)
        block = jnp.concatenate([low, block, high], axis=dim)
    return block


def sine_table(amount):
    indices = jnp.arange(amount, dtype=jnp.int32) + 1
    product = indices[:, None] * indices[None, :] % (2 * (amount + 1))
    angles = product.astype(jnp.float32) * (math.pi / (amount + 1))
    return math.sqrt(2.0 / (amount + 1)) * jnp.sin(angles)


def eigen_values(indices, amount):
    angles = (indices + 1).astype(jnp.float32) * (math.pi / (2 * (amount + 1)))
    return -4.0 * jnp.square(jnp.sin(angles))


def interpolation(fine_index, cell_count):
    scaled = 2 * fine_index + 1 + RATIO
    bottom = scaled // (2 * RATIO)
    weight = (scaled % (2 * RATIO)).astype(jnp.float32) / (2.0 * RATIO)
    column = jnp.arange(cell_count, dtype=jnp.int32)
    first_part = jnp.where(column[None, :] == bottom[:, None], 1.0 - weight[:, None], 0.0)
    second_part = jnp.where(column[None, :] == bottom[:, None] + 1, weight[:, None], 0.0)
    return first_part + second_part


def ghost_values(face, left_matrix, right_matrix):
    partial_value = jnp.einsum("fbc,kc->fbk", face, right_matrix, precision=highest)
    return jnp.einsum("fbk,jb->fjk", partial_value, left_matrix, precision=highest)


def neighbours(padded):
    summed = padded[2:, 1:-1, 1:-1] + padded[:-2, 1:-1, 1:-1]
    summed = summed + padded[1:-1, 2:, 1:-1] + padded[1:-1, :-2, 1:-1]
    return summed + padded[1:-1, 1:-1, 2:] + padded[1:-1, 1:-1, :-2]


def selection(first_global, length, window_start, window_length):
    here = first_global + jnp.arange(length, dtype=jnp.int32)
    window = window_start + jnp.arange(window_length, dtype=jnp.int32)
    return (here[:, None] == window[None, :]).astype(jnp.float32)


def body(coarse_density, fine_density, fine_start, anchor):
    cell_count = coarse_density.shape[2]
    coarse_rows = coarse_density.shape[0]
    coarse_cols = coarse_density.shape[1]
    potential = coarse(coarse_density)
    fine_rows, fine_cols, fine_depth = fine_start.shape
    total_x = fine_rows * lax.axis_size("gx")
    total_y = fine_cols * lax.axis_size("gy")
    total_z = fine_depth * lax.axis_size("grp")
    bound_x = total_x // RATIO + 2
    bound_y = total_y // RATIO + 2
    bound_z = total_z // RATIO + 2
    ends_x = interpolation(jnp.array([-1, total_x], dtype=jnp.int32), bound_x)
    ends_y = interpolation(jnp.array([-1, total_y], dtype=jnp.int32), bound_y)
    ends_z = interpolation(jnp.array([-1, total_z], dtype=jnp.int32), bound_z)
    coarse_x_start = lax.axis_index("gx") * coarse_rows
    coarse_y_start = lax.axis_index(("grp", "gy")) * coarse_cols
    pick_x = selection(coarse_x_start, coarse_rows, anchor[0] - 1, bound_x)
    pick_y = selection(coarse_y_start, coarse_cols, anchor[1] - 1, bound_y)
    pick_z = selection(0, cell_count, anchor[2] - 1, bound_z)
    weight_x = jnp.dot(ends_x, pick_x.T, precision=highest)
    weight_y = jnp.dot(ends_y, pick_y.T, precision=highest)
    weight_z = jnp.dot(ends_z, pick_z.T, precision=highest)
    partial_x = jnp.einsum("fx,xyz->fyz", weight_x, potential, precision=highest)
    partial_x = jnp.einsum("fyz,yb->fbz", partial_x, pick_y, precision=highest)
    partial_y = jnp.einsum("fy,xyz->fxz", weight_y, potential, precision=highest)
    partial_y = jnp.einsum("fxz,xa->faz", partial_y, pick_x, precision=highest)
    partial_z = jnp.einsum("fz,xyz->fxy", weight_z, potential, precision=highest)
    partial_z = jnp.einsum("fxy,xa->fay", partial_z, pick_x, precision=highest)
    place_y = selection(coarse_y_start, coarse_cols, 0, cell_count)
    partial_z = jnp.einsum("fay,yg->fag", partial_z, place_y, precision=highest)
    planes = lax.psum((partial_x, partial_y, partial_z), ("grp", "gx", "gy"))
    face_x = lax.dynamic_slice_in_dim(planes[0], anchor[2] - 1, bound_z, 2)
    face_y = lax.dynamic_slice_in_dim(planes[1], anchor[2] - 1, bound_z, 2)
    face_z = lax.dynamic_slice_in_dim(planes[2], anchor[1] - 1, bound_y, 2)
    start_x = lax.axis_index("gx") * fine_rows
    start_y = lax.axis_index("gy") * fine_cols
    start_z = lax.axis_index("grp") * fine_depth
    values = fine_start
    density_wide = with_halo(fine_density, (("grp", 2), ("gx", 0), ("gy", 1)), 1)
    index_x = start_x - 1 + jnp.arange(fine_rows + 2 * 1, dtype=jnp.int32)
    index_y = start_y - 1 + jnp.arange(fine_cols + 2 * 1, dtype=jnp.int32)
    index_z = start_z - 1 + jnp.arange(fine_depth + 2 * 1, dtype=jnp.int32)
    inner_x = interpolation(index_x, bound_x)
    inner_y = interpolation(index_y, bound_y)
    inner_z = interpolation(index_z, bound_z)
    ghost_x = ghost_values(face_x, inner_y, inner_z)
    ghost_y = ghost_values(face_y, inner_x, inner_z)
    ghost_z = ghost_values(face_z, inner_x, inner_y)
    boundary = jnp.where((index_x == 0)[:, None, None], ghost_x[0][None], 0.0)
    boundary = boundary + jnp.where((index_x == total_x - 1)[:, None, None], ghost_x[1][None], 0.0)
    boundary = boundary + jnp.where((index_y == 0)[None, :, None], ghost_y[0][:, None, :], 0.0)
    boundary = boundary + jnp.where(
        (index_y == total_y - 1)[None, :, None], ghost_y[1][:, None, :], 0.0
    )
    boundary = boundary + jnp.where((index_z == 0)[None, None, :], ghost_z[0][:, :, None], 0.0)
    boundary = boundary + jnp.where(
        (index_z == total_z - 1)[None, None, :], ghost_z[1][:, :, None], 0.0
    )
    inside_x = (index_x >= 0) & (index_x < total_x)
    inside_y = (index_y >= 0) & (index_y < total_y)
    inside_z = (index_z >= 0) & (index_z < total_z)
    inside = inside_x[:, None, None] & inside_y[None, :, None] & inside_z[None, None, :]
    boundary_wide, inside = (boundary, inside)
    source_wide = boundary_wide - density_wide / (RATIO * RATIO)
    source_core = source_wide[1:-1, 1:-1, 1:-1]
    for sweep in range(SWEEPS // 2):
        margin_values = with_halo(values, (("grp", 2), ("gx", 0), ("gy", 1)), 2)
        first_pass = jnp.where(inside, (neighbours(margin_values) + source_wide) / 6.0, 0.0)
        values = (neighbours(first_pass) + source_core) / 6.0
    return (potential, values)


def solution(mesh):
    return jax.shard_map(
        body,
        mesh=mesh,
        in_specs=(P("gx", ("grp", "gy"), None), P("gx", "gy", "grp"), P("gx", "gy", "grp"), P()),
        out_specs=(P("gx", ("grp", "gy"), None), P("gx", "gy", "grp")),
        check_vma=False,
    )
```

```python
import functools
import math

import jax
import jax.numpy as jnp
import numpy as np
from jax import lax
from jax.experimental import pallas as pl
from jax.experimental.pallas import tpu as pltpu
from jax.sharding import PartitionSpec as P

MESH = pl.DeviceIdType.MESH
NC = 512
F32 = jnp.float32
BF16 = jnp.bfloat16


def tables():
    index = np.arange(1, NC + 1, dtype=np.int64)
    angle = (index[:, None] * index[None, :]) % (2 * (NC + 1))
    sine = math.sqrt(2.0 / (NC + 1)) * np.sin(angle * (math.pi / (NC + 1)))
    sine = sine.astype(np.float32)
    high = sine.astype(jnp.bfloat16)
    low = (sine - high.astype(np.float32)).astype(jnp.bfloat16)
    lam = 4.0 * np.sin(index * (math.pi / (2 * (NC + 1)))) ** 2
    return high, low, lam.astype(np.float32)


def split(value):
    high = value.astype(BF16)
    low = (value - high.astype(F32)).astype(BF16)
    return high, low


def dot3(a, b, dims):
    ah, al = a
    bh, bl = b
    dd = functools.partial(
        lax.dot_general, dimension_numbers=(dims, ((), ())), preferred_element_type=F32
    )
    return dd(ah, bh) + (dd(al, bh) + dd(ah, bl))


def mm(a, b, dims):
    return lax.dot_general(a, b, (dims, ((), ())), preferred_element_type=F32)


def full(a, b, dims):
    return lax.dot_general(
        a, b, (dims, ((), ())), precision=lax.Precision.HIGHEST, preferred_element_type=F32
    )


NN = ((1,), (0,))
NT = ((1,), (1,))
TN = ((0,), (0,))


def exchange(v, lane):
    v = list(v)
    for bit in (1, 2, 4):
        upper = (lane & bit) != 0
        for i in range(8):
            if i & bit:
                continue
            a, c = v[i], v[i | bit]
            v[i] = jnp.where(upper, pltpu.roll(c, 16 * bit, 1), a)
            v[i | bit] = jnp.where(upper, c, pltpu.roll(a, 128 - 16 * bit, 1))
    return v


def swap_groups(source, target):
    lane = lax.broadcasted_iota(jnp.int32, (8, 128), 1) // 16

    def step(index, carry):
        at = index // 8
        bt = (index // 2) % 4
        row = pl.multiple_of((index % 2) * 8, 8)
        cols = pl.ds(pl.multiple_of(bt * 128, 128), 128)
        outs = pl.ds(pl.multiple_of(at * 128, 128), 128)
        v = [source[at * 8 + q, pl.ds(row, 8), cols] for q in range(8)]
        v = exchange(v, lane)
        for q in range(8):
            target[bt * 8 + q, pl.ds(row, 8), outs] = v[q]
        return carry

    lax.fori_loop(0, 32, step, 0)


def device(core, x, y, z):
    return (core, x * 4 + z % 4, (z // 4) * 8 + y)


ORDER = [
    (dy, side, core) for dy in (4, 3, 5, 2, 6, 1, 7, 0) for side in (0, 1) for core in (0, 1)
]


def shuffled():
    return list(ORDER[i] for i in np.random.RandomState(3).permutation(len(ORDER)))


def kernel(
    anchor, x_ref, fd_ref, fs_ref, sh_ref, sl_ref, lamr_ref, lamc_ref, lamq_ref, out_ref, fine_ref,
    za, zb, dd, u, dtab, m1, r1, m2, r2, dint, uh, ul, myh, myl, mz, mzth, mztl, wall, wys,
    mzx, rzx, my, ry, m5, r5, m6, r6, es, et, ed,
    s1, q1, s2, q2, s3, q3, s4, q4, sh1, qh1, sd, qd, sz, qz, sy, qy, s5, q5, s6, q6,
):
    core = lax.axis_index("grp")
    gx = lax.axis_index("gx")
    gy = lax.axis_index("gy")
    x, zl = gx // 4, gx % 4
    y, zh = gy % 8, gy // 8
    z = zh * 4 + zl
    me = core * 16 + gy
    zv = (z + 6) % 8
    lv, hv = zv % 4, zv // 4
    mid = core * 16 + hv * 8 + y
    pv = x * 4 + lv

    def to_mid(o):
        dy, side, oc = o
        ty = (y + dy) % 8
        tc = (core + oc) % 2
        return device(tc, x, ty, (zl + 4 * side + 2) % 8), tc * 16 + side * 8 + ty

    def to_real(o):
        dy, side, oc = o
        ty = (y + dy) % 8
        tc = (core + oc) % 2
        return device(tc, x, ty, lv + 4 * side), tc * 16 + side * 8 + ty

    def to_row(q):
        return device(core, q // 4, y, (q % 4 + 4 * hv + 2) % 8)

    def real_row(q):
        return device(core, q // 4, y, q % 4 + 4 * zh)

    here = (core, gx, gy)
    partner = (1 - core, gx, gy)
    own = pl.ds(pl.multiple_of(core * 128, 128), 128)
    sides = [(ox, oy) for ox in (-1, 0, 1) for oy in (-1, 0, 1) if (ox, oy) != (0, 0)]

    def beside(ox, oy):
        return (core, (gx + ox + 16) % 16, (gy + oy + 16) % 16)

    a0, a1, a2 = anchor[0], anchor[1], anchor[2]
    barrier = pltpu.get_barrier_semaphore()
    pl.semaphore_signal(barrier, inc=1, device_id=partner, device_id_type=MESH)
    for side in sides:
        pl.semaphore_signal(barrier, inc=1, device_id=beside(*side), device_id_type=MESH)
    for k in range(1, 16):
        pl.semaphore_signal(
            barrier, inc=1, device_id=real_row((gx + k) % 16), device_id_type=MESH
        )
    peers = shuffled()
    for o in peers:
        pl.semaphore_signal(barrier, inc=1, device_id=to_mid(o)[0], device_id_type=MESH)
    for k in range(1, 16):
        pl.semaphore_signal(barrier, inc=1, device_id=to_row((pv + k) % 16), device_id_type=MESH)

    s_pair = (sh_ref[...], sl_ref[...])
    value = x_ref[...].reshape(512, 512)
    za[...] = dot3(split(value), s_pair, NN).reshape(32, 16, 512)
    swap_groups(za, zb)

    pl.semaphore_wait(barrier, 71)

    t1 = []
    for i, o in enumerate(peers):
        target, block = to_mid(o)
        copy = pltpu.make_async_remote_copy(
            src_ref=zb.at[block], dst_ref=dd.at[me], send_sem=s1.at[i], recv_sem=q1.at[me],
            device_id=target, device_id_type=MESH,
        )
        copy.start()
        t1.append(copy)

    es[8:16, 8:40, own] = fs_ref[...]
    ed[8:16, 8:40, own] = fd_ref[...]
    halo = []
    for k, (ox, oy) in enumerate(sides):
        rows = {-1: pl.ds(0, 8), 0: pl.ds(0, 32), 1: pl.ds(24, 8)}[oy]
        to_rows = {-1: pl.ds(40, 8), 0: pl.ds(8, 32), 1: pl.ds(0, 8)}[oy]
        layers = {-1: pl.ds(16, 8), 0: pl.ds(8, 8), 1: pl.ds(0, 8)}[ox]
        for part, (src, dst) in enumerate(((fs_ref, es), (fd_ref, ed))):
            copy = pltpu.make_async_remote_copy(
                src_ref=src.at[:, rows, :], dst_ref=dst.at[layers, to_rows, own],
                send_sem=sh1.at[2 * k + part], recv_sem=qh1.at[2 * k + part],
                device_id=beside(ox, oy), device_id_type=MESH,
            )
            copy.start()
            halo.append(copy)

    def face_tables():
        def cells(rows, cols, first):
            grid = lax.broadcasted_iota(jnp.int32, (rows, cols), 0)
            return jnp.where(grid == first, 1.0, 0.0).astype(BF16)

        lane = lax.broadcasted_iota(jnp.int32, (512, 256), 1)
        pick = cells(512, 256, a1 - 3 + 8 * (lane // 16) + lane % 16)
        myh[...] = mm(sh_ref[...], pick, NN).astype(BF16)
        myl[...] = mm(sl_ref[...], pick, NN).astype(BF16)
        lane = lax.broadcasted_iota(jnp.int32, (512, 128), 1)
        pick = cells(512, 128, a2 - 1 + 30 * core + lane)
        mz[...] = (mm(sh_ref[...], pick, NN) + mm(sl_ref[...], pick, NN)).reshape(32, 16, 128)
        pick = cells(512, 128, a2 - 1 + 30 * (lane // 64) + lane % 64)
        mine = pl.ds(pl.multiple_of(mid * 16, 16), 16)
        high = mm(sh_ref[mine, :], pick, NN).astype(BF16)
        low = mm(sl_ref[mine, :], pick, NN).astype(BF16)
        mzth[...] = jnp.concatenate([high] * 32, axis=0)
        mztl[...] = jnp.concatenate([low] * 32, axis=0)

        def weights(cell, first, boxes, low_face, high_face):
            low_w = jnp.where(cell == first, 0.625, 0.0) + jnp.where(cell == first + 1, 0.375, 0.0)
            high_w = jnp.where(cell == first + boxes, 0.375, 0.0) + jnp.where(
                cell == first + boxes + 1, 0.625, 0.0
            )
            return jnp.where(low_face, low_w, 0.0) + jnp.where(high_face, high_w, 0.0)

        row = lax.broadcasted_iota(jnp.int32, (16, 512), 0)
        cell = lax.broadcasted_iota(jnp.int32, (16, 512), 1)
        wy = weights(cell, a1 - 1, 128, row == 0, row == 1).astype(BF16)
        wys[...] = mm(wy, sh_ref[...], NN) + mm(wy, sl_ref[...], NN)
        wz = weights(cell, a2 - 1, 64, row == 0, row == 1).astype(BF16)
        wz = mm(wz, sh_ref[...], NN) + mm(wz, sl_ref[...], NN)
        lane = lax.broadcasted_iota(jnp.int32, (512, 512), 1)
        pick = cells(512, 512, mid * 16 + lane % 16)
        wzh, wzl = split(wz)
        wz = mm(wzh, pick, NN) + mm(wzl, pick, NN)
        row = lax.broadcasted_iota(jnp.int32, (32, 512), 0)
        lane = lax.broadcasted_iota(jnp.int32, (32, 512), 1)
        for f in range(2):
            wall[32 * f : 32 * f + 32, :] = jnp.where(row == lane // 16, wz[f : f + 1, :], 0.0)
        wx = weights(32 * pv + lane // 16, a0 - 1, 32, row < 16, row >= 16)
        wall[64:96, :] = jnp.where(row % 16 == lane % 16, wx, 0.0)

    mu = lamr_ref[...] + lamc_ref[pl.ds(pl.multiple_of(mid * 16, 16), 16), :]

    def table(i, g):
        d = 1.0 / (1.0 + (mu + g))
        dtab[i] = d
        return (mu + g) * d

    lax.fori_loop(0, 31, table, jnp.ones((16, 512), F32))
    muq = lamq_ref[...] + lamc_ref[pl.ds(mid * 16 + pv, 1), :]
    c = 0.5 * muq
    c1 = c
    r32 = 2.0 * (1.0 + c)
    for _ in range(4):
        c = 2.0 * c * (c + 2.0)
        r32 = r32 * (2.0 * (1.0 + c))
    c = 2.0 * c * (c + 2.0)
    g = jnp.ones((4, 128), F32)
    for i in range(15):
        d = 1.0 / (1.0 + (2.0 * c + g))
        dint[i] = d
        g = (2.0 * c + g) * d
    dint[15] = 1.0 / (r32 * (1.0 + c1) + c + g)

    face_tables()
    for s in range(32):
        pltpu.make_async_remote_copy(
            src_ref=dd.at[s], dst_ref=dd.at[s], send_sem=s1.at[s], recv_sem=q1.at[s],
            device_id=(core, gx, gy), device_id_type=MESH,
        ).wait_recv()

    value = dd[...].reshape(512, 512)
    u[...] = dot3(split(value), s_pair, TN).reshape(32, 16, 512)

    first = -u[0]
    u[0] = first
    q0 = dtab[30]

    def forward(i, carry):
        yv, q, e = carry
        w = u[i]
        yv = dtab[i - 1] * yv - w
        u[i] = yv
        q = q * dtab[30 - i]
        return yv, q, e - q * w

    yv, _, e = lax.fori_loop(1, 31, forward, (first, q0, q0 * first))
    b = q0 * yv - u[31]
    for j in range(4):
        m1[pl.ds(j, 16, stride=8), :] = e[:, 128 * j : 128 * j + 128]
        m1[pl.ds(4 + j, 16, stride=8), :] = b[:, 128 * j : 128 * j + 128]
    t2 = []
    for k in range(1, 16):
        q = (pv + k) % 16
        copy = pltpu.make_async_remote_copy(
            src_ref=m1.at[pl.ds(pl.multiple_of(q * 8, 8), 8), :], dst_ref=r1.at[pv],
            send_sem=s2.at[k], recv_sem=q2.at[pv], device_id=to_row(q), device_id_type=MESH,
        )
        copy.start()
        t2.append(copy)
    for copy in halo:
        copy.wait_recv()
    pair = []
    for k, ref in enumerate((es, ed)):
        copy = pltpu.make_async_remote_copy(
            src_ref=ref.at[:, :, own], dst_ref=ref.at[:, :, own], send_sem=sd.at[k],
            recv_sem=qd.at[k], device_id=partner, device_id_type=MESH,
        )
        copy.start()
        pair.append(copy)
    r1[pv] = m1[pl.ds(pl.multiple_of(pv * 8, 8), 8), :]
    for k in range(1, 16):
        q = (pv + k) % 16
        pltpu.make_async_remote_copy(
            src_ref=r1.at[q], dst_ref=r1.at[q], send_sem=s2.at[k], recv_sem=q2.at[q],
            device_id=(core, gx, gy), device_id_type=MESH,
        ).wait_recv()
    ys = []
    prev = None
    for p in range(16):
        h = r1[p, 4:8, :]
        if p < 15:
            h = h + r1[p + 1, 0:4, :]
        h = r32 * h
        prev = h if p == 0 else h + dint[p - 1] * prev
        ys.append(prev)
    sol = [None] * 16
    sol[15] = dint[15] * ys[15]
    for p in range(14, -1, -1):
        sol[p] = dint[p] * (sol[p + 1] + ys[p])
    for p in range(16):
        m2[p, 0:4, :] = sol[p - 1] if p else jnp.zeros((4, 128), F32)
        m2[p, 4:8, :] = sol[p]
    t3 = []
    for k in range(1, 16):
        q = (pv + k) % 16
        copy = pltpu.make_async_remote_copy(
            src_ref=m2.at[q], dst_ref=r2.at[pl.ds(pl.multiple_of(pv * 8, 8), 8), :],
            send_sem=s3.at[k], recv_sem=q3.at[pv], device_id=to_row(q), device_id_type=MESH,
        )
        copy.start()
        t3.append(copy)
    r2[pl.ds(pl.multiple_of(pv * 8, 8), 8), :] = m2[pv]
    for k in range(1, 16):
        q = (pv + k) % 16
        view = r2.at[pl.ds(pl.multiple_of(q * 8, 8), 8), :]
        pltpu.make_async_remote_copy(
            src_ref=view, dst_ref=view, send_sem=s3.at[k], recv_sem=q3.at[q],
            device_id=(core, gx, gy), device_id_type=MESH,
        ).wait_recv()
    left = jnp.concatenate([r2[pl.ds(j, 16, stride=8), :] for j in range(4)], axis=1)
    right = jnp.concatenate([r2[pl.ds(4 + j, 16, stride=8), :] for j in range(4)], axis=1)

    def spread(i, t):
        u[i] = u[i] + t
        return dtab[i] * t

    lax.fori_loop(0, 31, spread, left)
    u[31] = right

    def backward(k, v):
        i = 30 - k
        v = dtab[i] * (v + u[i])
        u[i] = v
        return v

    lax.fori_loop(0, 31, backward, right)

    high, low = split(u[...].reshape(512, 512))
    uh[...] = high
    ul[...] = low
    u_pair = (uh[...], ul[...])
    rows = dot3(split(wall[...]), u_pair, NN)
    rows = dot3(split(rows), (myh[...], myl[...]), NN)
    lane = lax.broadcasted_iota(jnp.int32, (8, 128), 1) // 16
    for face in range(2):
        for t in range(2):
            cols = slice(128 * t, 128 * t + 128)
            v = [rows[32 * face + 8 * h : 32 * face + 8 * h + 8, cols] for h in range(4)]
            v += [rows[64 + 8 * h : 72 + 8 * h, cols] for h in range(4)]
            for q, w in enumerate(exchange(v, lane)):
                mzx[16 * face + 8 * t + q] = w
    ay = dot3(split(wys[...]), u_pair, NT)
    row = lax.broadcasted_iota(jnp.int32, (32, 512), 0)
    lanes = lax.broadcasted_iota(jnp.int32, (32, 512), 1)
    half = lax.broadcasted_iota(jnp.int32, (16, 128), 1) < 64
    for f in range(2):
        part = jnp.where(row == lanes // 16, ay[f : f + 1, :], 0.0)
        part = dot3(split(part), (mzth[...], mztl[...]), NN)
        top, bottom = part[:16], part[16:]
        my[f, 0] = jnp.where(half, top, pltpu.roll(bottom, 64, 1))
        my[f, 1] = jnp.where(half, pltpu.roll(top, 64, 1), bottom)
    tz = []
    for i, o in enumerate(peers):
        target, block = to_real(o)
        copy = pltpu.make_async_remote_copy(
            src_ref=mzx.at[block], dst_ref=rzx.at[mid], send_sem=sz.at[i], recv_sem=qz.at[mid],
            device_id=target, device_id_type=MESH,
        )
        copy.start()
        tz.append(copy)
    for f in range(2):
        for g in range(2):
            copy = pltpu.make_async_remote_copy(
                src_ref=my.at[f, g], dst_ref=ry.at[mid], send_sem=sy.at[2 * f + g],
                recv_sem=qy.at[mid], device_id=device(g, x, 7 * f, lv + 4 * f),
                device_id_type=MESH,
            )
            copy.start()
            tz.append(copy)

    for copy in t1:
        copy.wait_send()
    zb[...] = dot3(s_pair, u_pair, NT).reshape(32, 16, 512)
    t4 = []
    for i, o in enumerate(peers):
        target, block = to_real(o)
        copy = pltpu.make_async_remote_copy(
            src_ref=zb.at[block], dst_ref=za.at[mid], send_sem=s4.at[i], recv_sem=q4.at[mid],
            device_id=target, device_id_type=MESH,
        )
        copy.start()
        t4.append(copy)

    def arrived(ref, sem, index):
        pltpu.make_async_remote_copy(
            src_ref=ref.at[index], dst_ref=ref.at[index], send_sem=sem.at[index],
            recv_sem=sem.at[index], device_id=here, device_id_type=MESH,
        ).wait_recv()

    for s in range(32):
        arrived(rzx, qz, s)
    zsum = rzx[0]
    for s in range(1, 32):
        zsum = zsum + rzx[s]
    got = rzx[...].reshape(256, 128)
    parts = [full(got, mz[:, 8 * k : 8 * k + 8, :].reshape(256, 128), TN) for k in range(2)]
    for f in range(2):
        m6[f] = parts[0][64 + 32 * f : 80 + 32 * f] + parts[1][80 + 32 * f : 96 + 32 * f]
    row = lax.broadcasted_iota(jnp.int32, (128, 32), 0)
    col = lax.broadcasted_iota(jnp.int32, (128, 32), 1)
    pick = jnp.where(a0 - 3 + 2 * (row // 8) + row % 8 == 32 * gx + col, 1.0, 0.0)
    spread_z = jnp.concatenate([jnp.where(lane == h, zsum, 0.0) for h in range(4)], axis=0)
    m5[:, 0] = full(pick, spread_z, NN).reshape(16, 8, 128)
    m5[:, 1] = jnp.zeros((16, 8, 128), F32)
    at_y = (gy == 0) | (gy == 15)

    @pl.when(at_y)
    def _():
        for s in range(32):
            arrived(ry, qy, s)
        ysum = ry[0]
        for s in range(1, 32):
            ysum = ysum + ry[s]
        top = full(pick[:, :16], ysum, NN)
        bottom = full(pick[:, 16:], ysum, NN)
        left_half = lax.broadcasted_iota(jnp.int32, (128, 128), 1) < 64
        m5[:, 1] = jnp.where(left_half, top, bottom).reshape(16, 8, 128)

    t5 = []
    for k in range(1, 16):
        q = (gx + k) % 16
        copy = pltpu.make_async_remote_copy(
            src_ref=m5.at[q], dst_ref=r5.at[gx], send_sem=s5.at[k], recv_sem=q5.at[gx],
            device_id=real_row(q), device_id_type=MESH,
        )
        copy.start()
        t5.append(copy)
    r5[gx] = m5[gx]
    for f in range(2):
        end = 15 * f
        copy = pltpu.make_async_remote_copy(
            src_ref=m6.at[f], dst_ref=r6.at[gx], send_sem=s6.at[f], recv_sem=q6.at[gx],
            device_id=real_row(end), device_id_type=MESH,
        )

        @pl.when(gx != end)
        def _():
            copy.start()

        @pl.when(gx == end)
        def _():
            r6[gx] = m6[f]

    for k in range(1, 16):
        arrived(r5, q5, (gx + k) % 16)
    for copy in pair:
        copy.wait()

    def interpolate(rows, cols, fine, cell):
        scaled = 2 * fine + 5
        bottom = scaled // 8
        t = (scaled % 8).astype(F32) * 0.125
        return jnp.where(cell == bottom, 1.0 - t, 0.0) + jnp.where(cell == bottom + 1, t, 0.0)

    def grid(shape):
        return (lax.broadcasted_iota(jnp.int32, shape, 0), lax.broadcasted_iota(jnp.int32, shape, 1))

    row, col = grid((24, 8))
    int_x = interpolate(24, 8, row, col)
    row, col = grid((48, 128))
    int_y = jnp.where(col < 64, interpolate(48, 128, row, col % 16), 0.0)
    row, col = grid((128, 256))
    int_z = interpolate(128, 256, col, row % 64 + 30 * core)
    zb5 = r5[0, 0]
    yb5 = r5[0, 1]
    for s in range(1, 16):
        zb5 = zb5 + r5[s, 0]
        yb5 = yb5 + r5[s, 1]
    ghost_z = full(int_y, full(int_x, zb5, NN), NT)
    lane2 = lax.broadcasted_iota(jnp.int32, (48, 128), 1)
    edge = 127 * core
    for k in range(24):
        ed[k] = ed[k] * (-1.0 / 16.0)
        ed[k, :, own] = ed[k, :, own] + jnp.where(lane2 == edge, ghost_z[:, k : k + 1], 0.0)

    @pl.when(at_y)
    def _():
        ghost_y = full(full(int_x, yb5, NN), int_z, NN)
        for f in range(2):
            @pl.when(gy == 15 * f)
            def _():
                inner = 8 + 31 * f
                for k in range(24):
                    ed[k, inner : inner + 1, :] = ed[k, inner : inner + 1, :] + ghost_y[k : k + 1]

    for f in range(2):
        @pl.when(gx == 15 * f)
        def _():
            for k in range(16):
                if k != 15 * f:
                    arrived(r6, q6, k)
            xb6 = r6[0]
            for s in range(1, 16):
                xb6 = xb6 + r6[s]
            row, col = grid((48, 16))
            near_y = interpolate(48, 16, row, col)
            row, col = grid((128, 256))
            near_z = jnp.where(row < 64, interpolate(128, 256, col, row + 30 * core), 0.0)
            inner = 8 + 7 * f
            ed[inner] = ed[inner] + full(full(near_y, xb6, NN), near_z, NN)

    row = lax.broadcasted_iota(jnp.int32, (48, 256), 0)
    col = lax.broadcasted_iota(jnp.int32, (48, 256), 1)
    inside_y = (row + 32 * gy >= 8) & (row + 32 * gy < 520)

    def inside_x(k):
        return (k + 8 * gx >= 8) & (k + 8 * gx < 136)

    for k in range(24):
        es[k] = jnp.where(inside_y & inside_x(k), es[k], 0.0)

    def sweep(source, target, k):
        v = source[k]
        total = source[k - 1] + source[k + 1]
        total = total + (pltpu.roll(v, 1, 0) + pltpu.roll(v, 47, 0))
        total = total + jnp.where(col == 0, 0.0, pltpu.roll(v, 1, 1))
        total = total + jnp.where(col == 255, 0.0, pltpu.roll(v, 255, 1))
        factor = jnp.where(inside_y & inside_x(k), 1.0 / 6.0, 0.0)
        target[k] = (total + ed[k]) * factor

    def two(j, carry):
        def one(k, c):
            sweep(es, et, k)
            return c

        def other(k, c):
            sweep(et, es, k)
            return c

        lax.fori_loop(2 * j + 1, 23 - 2 * j, one, 0)
        lax.fori_loop(2 * j + 2, 22 - 2 * j, other, 0)
        return carry

    lax.fori_loop(0, 4, two, 0)
    fine_ref[...] = es[8:16, 8:40, own]

    for s in range(32):
        arrived(za, q4, s)
    swap_groups(za, dd)
    value = dd[...].reshape(512, 512)
    out_ref[...] = dot3(split(value), s_pair, NN).reshape(32, 16, 512)
    for copy in t2 + t3 + t4 + tz + t5 + halo:
        copy.wait_send()
    for f in range(2):
        @pl.when(gx != 15 * f)
        def _():
            pltpu.make_async_remote_copy(
                src_ref=m6.at[f], dst_ref=r6.at[gx], send_sem=s6.at[f], recv_sem=q6.at[gx],
                device_id=real_row(15 * f), device_id_type=MESH,
            ).wait_send()


def body(density, fine_density, fine_start, anchor):
    high, low, lam = tables()
    vm = pl.BlockSpec(memory_space=pltpu.VMEM)
    dma = pltpu.SemaphoreType.DMA

    def f32(*shape):
        return pltpu.VMEM(shape, F32)

    def b16(*shape):
        return pltpu.VMEM(shape, BF16)

    big = f32(32, 16, 512)
    return pl.pallas_call(
        kernel,
        out_shape=(
            jax.ShapeDtypeStruct((32, 16, 512), F32), jax.ShapeDtypeStruct((8, 32, 128), F32)
        ),
        in_specs=[pl.BlockSpec(memory_space=pltpu.SMEM)] + [vm] * 8,
        out_specs=(vm, vm),
        scratch_shapes=[
            big, big, big, big, f32(31, 16, 512),
            f32(128, 128), f32(16, 8, 128), f32(16, 8, 128), f32(128, 128), f32(16, 4, 128),
            b16(512, 512), b16(512, 512), b16(512, 256), b16(512, 256), f32(32, 16, 128),
            b16(512, 128), b16(512, 128), f32(96, 512), f32(16, 512),
            f32(32, 8, 128), f32(32, 8, 128), f32(2, 2, 16, 128), f32(32, 16, 128),
            f32(16, 2, 8, 128), f32(16, 2, 8, 128), f32(2, 16, 128), f32(16, 16, 128),
            f32(24, 48, 256), f32(24, 48, 256), f32(24, 48, 256),
            dma((32,)), dma((32,)), dma((16,)), dma((16,)), dma((16,)), dma((16,)),
            dma((32,)), dma((32,)), dma((16,)), dma((16,)), dma((2,)), dma((2,)),
            dma((32,)), dma((32,)), dma((4,)), dma((32,)), dma((16,)), dma((16,)),
            dma((2,)), dma((16,)),
        ],
        compiler_params=pltpu.CompilerParams(
            collective_id=0, has_side_effects=True, vmem_limit_bytes=56 << 20
        ),
    )(anchor, density, fine_density, fine_start, jnp.asarray(high), jnp.asarray(low),
      jnp.asarray(lam.reshape(1, 512)), jnp.asarray(lam.reshape(512, 1)),
      jnp.asarray(lam.reshape(4, 128)))


def solution(mesh):
    return jax.shard_map(
        body,
        mesh=mesh,
        in_specs=(P("gx", ("grp", "gy"), None), P("gx", "gy", "grp"), P("gx", "gy", "grp"), P()),
        out_specs=(P("gx", ("grp", "gy"), None), P("gx", "gy", "grp")),
        check_vma=False,
    )
```

```python
import functools
import math

import jax
import jax.numpy as jnp
import numpy as np
from jax import lax
from jax.experimental import pallas as pl
from jax.experimental.pallas import tpu as pltpu
from jax.sharding import PartitionSpec as P

MESH = pl.DeviceIdType.MESH
NC = 512
F32 = jnp.float32
BF16 = jnp.bfloat16


def tables():
    index = np.arange(1, NC + 1, dtype=np.int64)
    angle = (index[:, None] * index[None, :]) % (2 * (NC + 1))
    sine = math.sqrt(2.0 / (NC + 1)) * np.sin(angle * (math.pi / (NC + 1)))
    sine = sine.astype(np.float32)
    high = sine.astype(jnp.bfloat16)
    low = (sine - high.astype(np.float32)).astype(jnp.bfloat16)
    lam = 4.0 * np.sin(index * (math.pi / (2 * (NC + 1)))) ** 2
    return high, low, lam.astype(np.float32)


def split(value):
    high = value.astype(BF16)
    low = (value - high.astype(F32)).astype(BF16)
    return high, low


def dot3(a, b, dims):
    ah, al = a
    bh, bl = b
    dd = functools.partial(
        lax.dot_general, dimension_numbers=(dims, ((), ())), preferred_element_type=F32
    )
    return dd(ah, bh) + (dd(al, bh) + dd(ah, bl))


def mm(a, b, dims):
    return lax.dot_general(a, b, (dims, ((), ())), preferred_element_type=F32)


def full(a, b, dims):
    return lax.dot_general(
        a, b, (dims, ((), ())), precision=lax.Precision.HIGHEST, preferred_element_type=F32
    )


NN = ((1,), (0,))
NT = ((1,), (1,))
TN = ((0,), (0,))


def exchange(v, lane):
    v = list(v)
    for bit in (1, 2, 4):
        upper = (lane & bit) != 0
        for i in range(8):
            if i & bit:
                continue
            a, c = v[i], v[i | bit]
            v[i] = jnp.where(upper, pltpu.roll(c, 16 * bit, 1), a)
            v[i | bit] = jnp.where(upper, c, pltpu.roll(a, 128 - 16 * bit, 1))
    return v


def swap_groups(source, target):
    lane = lax.broadcasted_iota(jnp.int32, (8, 128), 1) // 16

    def step(at, carry):
        outs = pl.ds(pl.multiple_of(at * 128, 128), 128)
        for bt in range(4):
            for row in (0, 8):
                v = [source[at * 8 + q, row : row + 8, 128 * bt : 128 * bt + 128] for q in range(8)]
                for q, w in enumerate(exchange(v, lane)):
                    target[bt * 8 + q, row : row + 8, outs] = w
        return carry

    lax.fori_loop(0, 4, step, 0)


def device(core, x, y, z):
    return (core, x * 4 + z % 4, (z // 4) * 8 + y)


ORDER = [
    (dy, side, core) for dy in (4, 3, 5, 2, 6, 1, 7, 0) for side in (0, 1) for core in (0, 1)
]


def shuffled():
    return list(ORDER[i] for i in np.random.RandomState(3).permutation(len(ORDER)))


def kernel(
    anchor, lamr_ref, lamc_ref, lamq_ref, x_hbm, fd_hbm, fs_hbm, sh_hbm, sl_hbm, out_ref, fine_ref,
    x_ref, fd_ref, fs_ref, sh_ref, sl_ref,
    za, zb, dd, u, dtab, m1, r1, m2, r2, dint, uh, ul, myh, myl, mz, mzth, mztl, wall, wys,
    mzx, rzx, my, ry, m5, r5, m6, r6, es, et, ed, fa, fb, fr, trace, tin,
    s1, q1, s2, q2, s3, q3, s4, q4, sh1, qh1, sd, qd, sz, qz, sy, qy, s5, q5, s6, q6, sin,
    st, qt, se, qe,
):
    core = lax.axis_index("grp")
    gx = lax.axis_index("gx")
    gy = lax.axis_index("gy")
    x, zl = gx // 4, gx % 4
    y, zh = gy % 8, gy // 8
    z = zh * 4 + zl
    me = core * 16 + gy
    zv = (z + 6) % 8
    lv, hv = zv % 4, zv // 4
    mid = core * 16 + hv * 8 + y
    pv = x * 4 + lv

    def to_mid(o):
        dy, side, oc = o
        ty = (y + dy) % 8
        tc = (core + oc) % 2
        return device(tc, x, ty, (zl + 4 * side + 2) % 8), tc * 16 + side * 8 + ty

    def to_real(o):
        dy, side, oc = o
        ty = (y + dy) % 8
        tc = (core + oc) % 2
        return device(tc, x, ty, lv + 4 * side), tc * 16 + side * 8 + ty

    def to_row(q):
        return device(core, q // 4, y, (q % 4 + 4 * hv + 2) % 8)

    def real_row(q):
        return device(core, q // 4, y, q % 4 + 4 * zh)

    here = (core, gx, gy)
    partner = (1 - core, gx, gy)
    own = pl.ds(pl.multiple_of(core * 128, 128), 128)

    def beside(ox, oy):
        return (core, (gx + ox + 16) % 16, (gy + oy + 16) % 16)

    a0, a1, a2 = anchor[0], anchor[1], anchor[2]
    barrier = pltpu.get_barrier_semaphore()
    pl.semaphore_signal(barrier, inc=1, device_id=partner, device_id_type=MESH)
    for oy in (-1, 1):
        pl.semaphore_signal(barrier, inc=1, device_id=beside(0, oy), device_id_type=MESH)
    for k in range(1, 16):
        pl.semaphore_signal(
            barrier, inc=1, device_id=real_row((gx + k) % 16), device_id_type=MESH
        )
    peers = shuffled()
    for o in peers:
        pl.semaphore_signal(barrier, inc=1, device_id=to_mid(o)[0], device_id_type=MESH)
    for k in range(1, 16):
        pl.semaphore_signal(barrier, inc=1, device_id=to_row((pv + k) % 16), device_id_type=MESH)

    fetch = []
    for k, (src, dst) in enumerate((
        (x_hbm, x_ref), (sh_hbm, sh_ref), (sl_hbm, sl_ref), (fd_hbm, fd_ref), (fs_hbm, fs_ref)
    )):
        copy = pltpu.make_async_copy(src, dst, sin.at[k])
        copy.start()
        fetch.append(copy)
    for copy in fetch[:3]:
        copy.wait()
    s_pair = (sh_ref[...], sl_ref[...])
    value = x_ref[...].reshape(512, 512)
    za[...] = dot3(split(value), s_pair, NN).reshape(32, 16, 512)
    swap_groups(za, zb)
    fetch[3].wait()
    fetch[4].wait()
    fa[1:9, 8:40, own] = fs_ref[...]
    fr[1:9, 8:40, own] = fd_ref[...]

    pl.semaphore_wait(barrier, 65)

    halo = []
    for k, oy in enumerate((-1, 1)):
        rows = pl.ds(0, 8) if oy < 0 else pl.ds(24, 8)
        to_rows = pl.ds(40, 8) if oy < 0 else pl.ds(0, 8)
        for part, (src, dst) in enumerate(((fs_ref, fa), (fd_ref, fr))):
            copy = pltpu.make_async_remote_copy(
                src_ref=src.at[:, rows, :], dst_ref=dst.at[pl.ds(1, 8), to_rows, own],
                send_sem=sh1.at[2 * k + part], recv_sem=qh1.at[2 * k + part],
                device_id=beside(0, oy), device_id_type=MESH,
            )
            copy.start()
            halo.append(copy)
    t1 = []
    for i, o in enumerate(peers):
        target, block = to_mid(o)
        copy = pltpu.make_async_remote_copy(
            src_ref=zb.at[block], dst_ref=dd.at[me], send_sem=s1.at[i], recv_sem=q1.at[me],
            device_id=target, device_id_type=MESH,
        )
        copy.start()
        t1.append(copy)

    def face_tables():
        def cells(rows, cols, first):
            grid = lax.broadcasted_iota(jnp.int32, (rows, cols), 0)
            return jnp.where(grid == first, 1.0, 0.0).astype(BF16)

        lane = lax.broadcasted_iota(jnp.int32, (512, 256), 1)
        pick = cells(512, 256, a1 - 3 + 8 * (lane // 16) + lane % 16)
        myh[...] = mm(sh_ref[...], pick, NN).astype(BF16)
        myl[...] = mm(sl_ref[...], pick, NN).astype(BF16)
        lane = lax.broadcasted_iota(jnp.int32, (512, 128), 1)
        pick = cells(512, 128, a2 - 1 + 30 * core + lane)
        mz[...] = (mm(sh_ref[...], pick, NN) + mm(sl_ref[...], pick, NN)).reshape(32, 16, 128)
        pick = cells(512, 128, a2 - 1 + 30 * (lane // 64) + lane % 64)
        mine = pl.ds(pl.multiple_of(mid * 16, 16), 16)
        high = mm(sh_ref[mine, :], pick, NN).astype(BF16)
        low = mm(sl_ref[mine, :], pick, NN).astype(BF16)
        mzth[...] = jnp.concatenate([high] * 32, axis=0)
        mztl[...] = jnp.concatenate([low] * 32, axis=0)

        def weights(cell, first, boxes, low_face, high_face):
            low_w = jnp.where(cell == first, 0.625, 0.0) + jnp.where(cell == first + 1, 0.375, 0.0)
            high_w = jnp.where(cell == first + boxes, 0.375, 0.0) + jnp.where(
                cell == first + boxes + 1, 0.625, 0.0
            )
            return jnp.where(low_face, low_w, 0.0) + jnp.where(high_face, high_w, 0.0)

        row = lax.broadcasted_iota(jnp.int32, (16, 512), 0)
        cell = lax.broadcasted_iota(jnp.int32, (16, 512), 1)
        wy = weights(cell, a1 - 1, 128, row == 0, row == 1).astype(BF16)
        wys[...] = mm(wy, sh_ref[...], NN) + mm(wy, sl_ref[...], NN)
        wz = weights(cell, a2 - 1, 64, row == 0, row == 1).astype(BF16)
        wz = mm(wz, sh_ref[...], NN) + mm(wz, sl_ref[...], NN)
        lane = lax.broadcasted_iota(jnp.int32, (512, 512), 1)
        pick = cells(512, 512, mid * 16 + lane % 16)
        wzh, wzl = split(wz)
        wz = mm(wzh, pick, NN) + mm(wzl, pick, NN)
        row = lax.broadcasted_iota(jnp.int32, (32, 512), 0)
        lane = lax.broadcasted_iota(jnp.int32, (32, 512), 1)
        for f in range(2):
            wall[32 * f : 32 * f + 32, :] = jnp.where(row == lane // 16, wz[f : f + 1, :], 0.0)
        wx = weights(32 * pv + lane // 16, a0 - 1, 32, row < 16, row >= 16)
        wall[64:96, :] = jnp.where(row % 16 == lane % 16, wx, 0.0)

    mu = lamr_ref[...] + lamc_ref[pl.ds(pl.multiple_of(mid * 16, 16), 16), :]

    def table(i, g):
        d = 1.0 / (1.0 + (mu + g))
        dtab[i] = d
        return (mu + g) * d

    lax.fori_loop(0, 31, table, jnp.ones((16, 512), F32))
    muq = lamq_ref[...] + lamc_ref[pl.ds(mid * 16 + pv, 1), :]
    c = 0.5 * muq
    c1 = c
    r32 = 2.0 * (1.0 + c)
    for _ in range(4):
        c = 2.0 * c * (c + 2.0)
        r32 = r32 * (2.0 * (1.0 + c))
    c = 2.0 * c * (c + 2.0)
    g = jnp.ones((4, 128), F32)
    for i in range(15):
        d = 1.0 / (1.0 + (2.0 * c + g))
        dint[i] = d
        g = (2.0 * c + g) * d
    dint[15] = 1.0 / (r32 * (1.0 + c1) + c + g)

    face_tables()
    for copy in halo:
        copy.wait_recv()
    pair = []
    for k, ref in enumerate((fa, fr)):
        view = ref.at[pl.ds(1, 8), :, own]
        copy = pltpu.make_async_remote_copy(
            src_ref=view, dst_ref=view, send_sem=sd.at[k], recv_sem=qd.at[k],
            device_id=partner, device_id_type=MESH,
        )
        copy.start()
        pair.append(copy)
    for copy in pair:
        copy.wait()
    fine_row = lax.broadcasted_iota(jnp.int32, (48, 256), 0) + 32 * gy
    fine_col = lax.broadcasted_iota(jnp.int32, (48, 256), 1)
    inside_y = (fine_row >= 8) & (fine_row < 520)
    sixth = jnp.where(inside_y, 1.0 / 6.0, 0.0)

    def layer(source, extra, k):
        v = source[k]
        total = (source[k - 1] + source[k + 1]) + extra[k]
        total = total + (pltpu.roll(v, 1, 0) + pltpu.roll(v, 47, 0))
        total = total + jnp.where(fine_col == 0, 0.0, pltpu.roll(v, 1, 1))
        return total + jnp.where(fine_col == 255, 0.0, pltpu.roll(v, 255, 1))

    for k in (0, 9):
        fa[k] = jnp.zeros((48, 256), F32)
        fb[k] = jnp.zeros((48, 256), F32)
    for k in range(1, 9):
        fa[k] = jnp.where(inside_y, fa[k], 0.0)
        fr[k] = fr[k] * (-1.0 / 16.0)
        es[k + 7] = fa[k]

    def alone(j, carry):
        for part, (source, target) in enumerate(((fa, fb), (fb, fa))):
            trace[0, 2 * j + part] = source[1]
            trace[1, 2 * j + part] = source[8]

            def four(k, c):
                for m in range(4):
                    index = 1 + 4 * k + m
                    target[index] = layer(source, fr, index) * sixth
                return c

            lax.fori_loop(0, 2, four, 0)
        return carry

    lax.fori_loop(0, 4, alone, 0)
    for s in range(32):
        pltpu.make_async_remote_copy(
            src_ref=dd.at[s], dst_ref=dd.at[s], send_sem=s1.at[s], recv_sem=q1.at[s],
            device_id=(core, gx, gy), device_id_type=MESH,
        ).wait_recv()

    value = dd[...].reshape(512, 512)
    u[...] = dot3(split(value), s_pair, TN).reshape(32, 16, 512)

    first = -u[0]
    u[0] = first
    q0 = dtab[30]

    def forward(i, carry):
        yv, q, e = carry
        w = u[i]
        yv = dtab[i - 1] * yv - w
        u[i] = yv
        q = q * dtab[30 - i]
        return yv, q, e - q * w

    yv, _, e = lax.fori_loop(1, 31, forward, (first, q0, q0 * first))
    b = q0 * yv - u[31]
    for j in range(4):
        m1[pl.ds(j, 16, stride=8), :] = e[:, 128 * j : 128 * j + 128]
        m1[pl.ds(4 + j, 16, stride=8), :] = b[:, 128 * j : 128 * j + 128]
    t2 = []
    for k in range(1, 16):
        q = (pv + k) % 16
        copy = pltpu.make_async_remote_copy(
            src_ref=m1.at[pl.ds(pl.multiple_of(q * 8, 8), 8), :], dst_ref=r1.at[pv],
            send_sem=s2.at[k], recv_sem=q2.at[pv], device_id=to_row(q), device_id_type=MESH,
        )
        copy.start()
        t2.append(copy)
    tt = []
    for side, ox in enumerate((-1, 1)):
        copy = pltpu.make_async_remote_copy(
            src_ref=trace.at[side, :, :, own], dst_ref=tin.at[1 - side, :, :, own],
            send_sem=st.at[side], recv_sem=qt.at[1 - side], device_id=beside(ox, 0),
            device_id_type=MESH,
        )
        copy.start()
        tt.append(copy)
    r1[pv] = m1[pl.ds(pl.multiple_of(pv * 8, 8), 8), :]
    for k in range(1, 16):
        q = (pv + k) % 16
        pltpu.make_async_remote_copy(
            src_ref=r1.at[q], dst_ref=r1.at[q], send_sem=s2.at[k], recv_sem=q2.at[q],
            device_id=(core, gx, gy), device_id_type=MESH,
        ).wait_recv()
    ys = []
    prev = None
    for p in range(16):
        h = r1[p, 4:8, :]
        if p < 15:
            h = h + r1[p + 1, 0:4, :]
        h = r32 * h
        prev = h if p == 0 else h + dint[p - 1] * prev
        ys.append(prev)
    sol = [None] * 16
    sol[15] = dint[15] * ys[15]
    for p in range(14, -1, -1):
        sol[p] = dint[p] * (sol[p + 1] + ys[p])
    for p in range(16):
        m2[p, 0:4, :] = sol[p - 1] if p else jnp.zeros((4, 128), F32)
        m2[p, 4:8, :] = sol[p]
    t3 = []
    for k in range(1, 16):
        q = (pv + k) % 16
        copy = pltpu.make_async_remote_copy(
            src_ref=m2.at[q], dst_ref=r2.at[pl.ds(pl.multiple_of(pv * 8, 8), 8), :],
            send_sem=s3.at[k], recv_sem=q3.at[pv], device_id=to_row(q), device_id_type=MESH,
        )
        copy.start()
        t3.append(copy)
    r2[pl.ds(pl.multiple_of(pv * 8, 8), 8), :] = m2[pv]
    for k in range(1, 16):
        q = (pv + k) % 16
        view = r2.at[pl.ds(pl.multiple_of(q * 8, 8), 8), :]
        pltpu.make_async_remote_copy(
            src_ref=view, dst_ref=view, send_sem=s3.at[k], recv_sem=q3.at[q],
            device_id=(core, gx, gy), device_id_type=MESH,
        ).wait_recv()
    left = jnp.concatenate([r2[pl.ds(j, 16, stride=8), :] for j in range(4)], axis=1)
    right = jnp.concatenate([r2[pl.ds(4 + j, 16, stride=8), :] for j in range(4)], axis=1)

    def spread(i, t):
        u[i] = u[i] + t
        return dtab[i] * t

    lax.fori_loop(0, 31, spread, left)
    u[31] = right

    def backward(k, v):
        i = 30 - k
        v = dtab[i] * (v + u[i])
        u[i] = v
        return v

    lax.fori_loop(0, 31, backward, right)

    high, low = split(u[...].reshape(512, 512))
    uh[...] = high
    ul[...] = low
    u_pair = (uh[...], ul[...])
    rows = dot3(split(wall[...]), u_pair, NN)
    rows = dot3(split(rows), (myh[...], myl[...]), NN)
    lane = lax.broadcasted_iota(jnp.int32, (8, 128), 1) // 16
    for face in range(2):
        for t in range(2):
            cols = slice(128 * t, 128 * t + 128)
            v = [rows[32 * face + 8 * h : 32 * face + 8 * h + 8, cols] for h in range(4)]
            v += [rows[64 + 8 * h : 72 + 8 * h, cols] for h in range(4)]
            for q, w in enumerate(exchange(v, lane)):
                mzx[16 * face + 8 * t + q] = w
    ay = dot3(split(wys[...]), u_pair, NT)
    row = lax.broadcasted_iota(jnp.int32, (32, 512), 0)
    lanes = lax.broadcasted_iota(jnp.int32, (32, 512), 1)
    half = lax.broadcasted_iota(jnp.int32, (16, 128), 1) < 64
    for f in range(2):
        part = jnp.where(row == lanes // 16, ay[f : f + 1, :], 0.0)
        part = dot3(split(part), (mzth[...], mztl[...]), NN)
        top, bottom = part[:16], part[16:]
        my[f, 0] = jnp.where(half, top, pltpu.roll(bottom, 64, 1))
        my[f, 1] = jnp.where(half, pltpu.roll(top, 64, 1), bottom)
    tz = []
    for i, o in enumerate(peers):
        target, block = to_real(o)
        copy = pltpu.make_async_remote_copy(
            src_ref=mzx.at[block], dst_ref=rzx.at[mid], send_sem=sz.at[i], recv_sem=qz.at[mid],
            device_id=target, device_id_type=MESH,
        )
        copy.start()
        tz.append(copy)
    for f in range(2):
        for g in range(2):
            copy = pltpu.make_async_remote_copy(
                src_ref=my.at[f, g], dst_ref=ry.at[mid], send_sem=sy.at[2 * f + g],
                recv_sem=qy.at[mid], device_id=device(g, x, 7 * f, lv + 4 * f),
                device_id_type=MESH,
            )
            copy.start()
            tz.append(copy)

    for copy in t1:
        copy.wait_send()
    zb[...] = dot3(s_pair, u_pair, NT).reshape(32, 16, 512)
    t4 = []
    for i, o in enumerate(peers):
        target, block = to_real(o)
        copy = pltpu.make_async_remote_copy(
            src_ref=zb.at[block], dst_ref=za.at[mid], send_sem=s4.at[i], recv_sem=q4.at[mid],
            device_id=target, device_id_type=MESH,
        )
        copy.start()
        t4.append(copy)

    te = []
    for side in range(2):
        pltpu.make_async_remote_copy(
            src_ref=trace.at[side, :, :, own], dst_ref=tin.at[side, :, :, own],
            send_sem=st.at[side], recv_sem=qt.at[side], device_id=here, device_id_type=MESH,
        ).wait_recv()
        view = tin.at[side, :, :, own]
        copy = pltpu.make_async_remote_copy(
            src_ref=view, dst_ref=view, send_sem=se.at[side], recv_sem=qe.at[side],
            device_id=partner, device_id_type=MESH,
        )
        copy.start()
        te.append(copy)
    def arrived(ref, sem, index):
        pltpu.make_async_remote_copy(
            src_ref=ref.at[index], dst_ref=ref.at[index], send_sem=sem.at[index],
            recv_sem=sem.at[index], device_id=here, device_id_type=MESH,
        ).wait_recv()

    for s in range(32):
        arrived(rzx, qz, s)
    zsum = rzx[0]
    for s in range(1, 32):
        zsum = zsum + rzx[s]
    got = rzx[...].reshape(256, 128)
    parts = [full(got, mz[:, 8 * k : 8 * k + 8, :].reshape(256, 128), TN) for k in range(2)]
    for f in range(2):
        m6[f] = parts[0][64 + 32 * f : 80 + 32 * f] + parts[1][80 + 32 * f : 96 + 32 * f]
    row = lax.broadcasted_iota(jnp.int32, (128, 32), 0)
    col = lax.broadcasted_iota(jnp.int32, (128, 32), 1)
    pick = jnp.where(a0 - 3 + 2 * (row // 8) + row % 8 == 32 * gx + col, 1.0, 0.0)
    spread_z = jnp.concatenate([jnp.where(lane == h, zsum, 0.0) for h in range(4)], axis=0)
    m5[:, 0] = full(pick, spread_z, NN).reshape(16, 8, 128)
    m5[:, 1] = jnp.zeros((16, 8, 128), F32)
    at_y = (gy == 0) | (gy == 15)

    @pl.when(at_y)
    def _():
        for s in range(32):
            arrived(ry, qy, s)
        ysum = ry[0]
        for s in range(1, 32):
            ysum = ysum + ry[s]
        top = full(pick[:, :16], ysum, NN)
        bottom = full(pick[:, 16:], ysum, NN)
        left_half = lax.broadcasted_iota(jnp.int32, (128, 128), 1) < 64
        m5[:, 1] = jnp.where(left_half, top, bottom).reshape(16, 8, 128)

    t5 = []
    for k in range(1, 16):
        q = (gx + k) % 16
        copy = pltpu.make_async_remote_copy(
            src_ref=m5.at[q], dst_ref=r5.at[gx], send_sem=s5.at[k], recv_sem=q5.at[gx],
            device_id=real_row(q), device_id_type=MESH,
        )
        copy.start()
        t5.append(copy)
    r5[gx] = m5[gx]
    for f in range(2):
        end = 15 * f
        copy = pltpu.make_async_remote_copy(
            src_ref=m6.at[f], dst_ref=r6.at[gx], send_sem=s6.at[f], recv_sem=q6.at[gx],
            device_id=real_row(end), device_id_type=MESH,
        )

        @pl.when(gx != end)
        def _():
            copy.start()

        @pl.when(gx == end)
        def _():
            r6[gx] = m6[f]

    for k in range(1, 16):
        arrived(r5, q5, (gx + k) % 16)

    def interpolate(rows, cols, fine, cell):
        scaled = 2 * fine + 5
        bottom = scaled // 8
        t = (scaled % 8).astype(F32) * 0.125
        return jnp.where(cell == bottom, 1.0 - t, 0.0) + jnp.where(cell == bottom + 1, t, 0.0)

    def grid(shape):
        return (lax.broadcasted_iota(jnp.int32, shape, 0), lax.broadcasted_iota(jnp.int32, shape, 1))

    row, col = grid((24, 8))
    int_x = interpolate(24, 8, row, col)
    row, col = grid((48, 128))
    int_y = jnp.where(col < 64, interpolate(48, 128, row, col % 16), 0.0)
    row, col = grid((128, 256))
    int_z = interpolate(128, 256, col, row % 64 + 30 * core)
    zb5 = r5[0, 0]
    yb5 = r5[0, 1]
    for s in range(1, 16):
        zb5 = zb5 + r5[s, 0]
        yb5 = yb5 + r5[s, 1]
    ghost_z = full(int_y, full(int_x, zb5, NN), NT)
    lane2 = lax.broadcasted_iota(jnp.int32, (48, 128), 1)
    edge = 127 * core
    for k in range(24):
        ed[k] = fr[k - 7] if 8 <= k < 16 else jnp.zeros((48, 256), F32)
        ed[k, :, own] = ed[k, :, own] + jnp.where(lane2 == edge, ghost_z[:, k : k + 1], 0.0)

    @pl.when(at_y)
    def _():
        ghost_y = full(full(int_x, yb5, NN), int_z, NN)
        for f in range(2):
            @pl.when(gy == 15 * f)
            def _():
                inner = 8 + 31 * f
                for k in range(24):
                    ed[k, inner : inner + 1, :] = ed[k, inner : inner + 1, :] + ghost_y[k : k + 1]

    for f in range(2):
        @pl.when(gx == 15 * f)
        def _():
            for k in range(16):
                if k != 15 * f:
                    arrived(r6, q6, k)
            xb6 = r6[0]
            for s in range(1, 16):
                xb6 = xb6 + r6[s]
            row, col = grid((48, 16))
            near_y = interpolate(48, 16, row, col)
            row, col = grid((128, 256))
            near_z = jnp.where(row < 64, interpolate(128, 256, col, row + 30 * core), 0.0)
            inner = 8 + 7 * f
            ed[inner] = ed[inner] + full(full(near_y, xb6, NN), near_z, NN)

    for copy in te:
        copy.wait_recv()

    def inside_x(k):
        return (k + 8 * gx >= 8) & (k + 8 * gx < 136)

    for k in list(range(8)) + list(range(16, 24)):
        es[k] = jnp.zeros((48, 256), F32)
    ends = (jnp.where(gx == 0, 0.0, sixth), jnp.where(gx == 15, 0.0, sixth))
    for j in range(8):
        source, target = ((es, et), (et, es))[j % 2]

        def two(k, c, source=source, target=target, j=j):
            for m in range(2):
                index = j + 1 + 2 * k + m
                target[index] = layer(source, ed, index) * jnp.where(inside_x(index), sixth, 0.0)
            return c

        lax.fori_loop(0, 11 - j, two, 0)
        target[8] = target[8] + tin[0, j] * ends[0]
        target[15] = target[15] + tin[1, j] * ends[1]
    fine_ref[...] = es[8:16, 8:40, own]

    for s in range(32):
        arrived(za, q4, s)
    swap_groups(za, dd)
    value = dd[...].reshape(512, 512)
    out_ref[...] = dot3(split(value), s_pair, NN).reshape(32, 16, 512)
    for copy in t2 + t3 + t4 + tz + t5 + halo + tt + te:
        copy.wait_send()
    for f in range(2):
        @pl.when(gx != 15 * f)
        def _():
            pltpu.make_async_remote_copy(
                src_ref=m6.at[f], dst_ref=r6.at[gx], send_sem=s6.at[f], recv_sem=q6.at[gx],
                device_id=real_row(15 * f), device_id_type=MESH,
            ).wait_send()


def body(density, fine_density, fine_start, anchor):
    high, low, lam = tables()
    vm = pl.BlockSpec(memory_space=pltpu.VMEM)
    dma = pltpu.SemaphoreType.DMA

    def f32(*shape):
        return pltpu.VMEM(shape, F32)

    def b16(*shape):
        return pltpu.VMEM(shape, BF16)

    big = f32(32, 16, 512)
    return pl.pallas_call(
        kernel,
        out_shape=(
            jax.ShapeDtypeStruct((32, 16, 512), F32), jax.ShapeDtypeStruct((8, 32, 128), F32)
        ),
        in_specs=[pl.BlockSpec(memory_space=pltpu.SMEM)] + [vm] * 3
        + [pl.BlockSpec(memory_space=pl.ANY)] * 5,
        out_specs=(vm, vm),
        scratch_shapes=[
            big, f32(8, 32, 128), f32(8, 32, 128), b16(512, 512), b16(512, 512),
            big, big, big, big, f32(31, 16, 512),
            f32(128, 128), f32(16, 8, 128), f32(16, 8, 128), f32(128, 128), f32(16, 4, 128),
            b16(512, 512), b16(512, 512), b16(512, 256), b16(512, 256), f32(32, 16, 128),
            b16(512, 128), b16(512, 128), f32(96, 512), f32(16, 512),
            f32(32, 8, 128), f32(32, 8, 128), f32(2, 2, 16, 128), f32(32, 16, 128),
            f32(16, 2, 8, 128), f32(16, 2, 8, 128), f32(2, 16, 128), f32(16, 16, 128),
            f32(24, 48, 256), f32(24, 48, 256), f32(24, 48, 256),
            f32(10, 48, 256), f32(10, 48, 256), f32(10, 48, 256),
            f32(2, 8, 48, 256), f32(2, 8, 48, 256),
            dma((32,)), dma((32,)), dma((16,)), dma((16,)), dma((16,)), dma((16,)),
            dma((32,)), dma((32,)), dma((4,)), dma((4,)), dma((2,)), dma((2,)),
            dma((32,)), dma((32,)), dma((4,)), dma((32,)), dma((16,)), dma((16,)),
            dma((2,)), dma((16,)), dma((5,)), dma((2,)), dma((2,)), dma((2,)), dma((2,)),
        ],
        compiler_params=pltpu.CompilerParams(
            collective_id=0, has_side_effects=True, vmem_limit_bytes=56 << 20
        ),
    )(anchor, jnp.asarray(lam.reshape(1, 512)), jnp.asarray(lam.reshape(512, 1)),
      jnp.asarray(lam.reshape(4, 128)), density, fine_density, fine_start,
      jnp.asarray(high), jnp.asarray(low))


def solution(mesh):
    return jax.shard_map(
        body,
        mesh=mesh,
        in_specs=(P("gx", ("grp", "gy"), None), P("gx", "gy", "grp"), P("gx", "gy", "grp"), P()),
        out_specs=(P("gx", ("grp", "gy"), None), P("gx", "gy", "grp")),
        check_vma=False,
    )
```

```python
import functools
import math

import jax
import jax.numpy as jnp
import numpy as np
from jax import lax
from jax.experimental import pallas as pl
from jax.experimental.pallas import tpu as pltpu
from jax.sharding import PartitionSpec as P

MESH = pl.DeviceIdType.MESH
NC = 512
F32 = jnp.float32
CUT1, CUT4A, CUT4B = 32, 16, 32
WIDE = 4
BF16 = jnp.bfloat16


def tables():
    index = np.arange(1, NC + 1, dtype=np.int64)
    angle = (index[:, None] * index[None, :]) % (2 * (NC + 1))
    sine = math.sqrt(2.0 / (NC + 1)) * np.sin(angle * (math.pi / (NC + 1)))
    sine = sine.astype(np.float32)
    high = sine.astype(jnp.bfloat16)
    low = (sine - high.astype(np.float32)).astype(jnp.bfloat16)
    lam = 4.0 * np.sin(index * (math.pi / (2 * (NC + 1)))) ** 2
    return high, low, lam.astype(np.float32)


def split(value):
    high = value.astype(BF16)
    low = (value - high.astype(F32)).astype(BF16)
    return high, low


def dot3(a, b, dims):
    ah, al = a
    bh, bl = b
    dd = functools.partial(
        lax.dot_general, dimension_numbers=(dims, ((), ())), preferred_element_type=F32
    )
    return dd(ah, bh) + (dd(al, bh) + dd(ah, bl))


def mm(a, b, dims):
    return lax.dot_general(a, b, (dims, ((), ())), preferred_element_type=F32)


def full(a, b, dims):
    return lax.dot_general(
        a, b, (dims, ((), ())), precision=lax.Precision.HIGHEST, preferred_element_type=F32
    )


NN = ((1,), (0,))
NT = ((1,), (1,))
TN = ((0,), (0,))


def exchange(v, lane):
    v = list(v)
    for bit in (1, 2, 4, 8):
        upper = (lane & bit) != 0
        for i in range(16):
            if i & bit:
                continue
            a, c = v[i], v[i | bit]
            v[i] = jnp.where(upper, pltpu.roll(c, 8 * bit, 1), a)
            v[i | bit] = jnp.where(upper, c, pltpu.roll(a, 128 - 8 * bit, 1))
    return v


def exchange8(v, lane):
    v = list(v)
    for bit in (1, 2, 4):
        upper = (lane & bit) != 0
        for i in range(8):
            if i & bit:
                continue
            a, c = v[i], v[i | bit]
            v[i] = jnp.where(upper, pltpu.roll(c, 16 * bit, 1), a)
            v[i | bit] = jnp.where(upper, c, pltpu.roll(a, 128 - 16 * bit, 1))
    return v


def swap_groups(source, target, first, out_first):
    lane = lax.broadcasted_iota(jnp.int32, (8, 128), 1) // 8
    for a in range(2):
        for b in range(2):
            cols = slice(first + 128 * b, first + 128 * b + 128)
            outs = slice(out_first + 128 * a, out_first + 128 * a + 128)
            for row in (0, 8):
                v = [source[16 * a + q, row : row + 8, cols] for q in range(16)]
                for q, w in enumerate(exchange(v, lane)):
                    target[16 * b + q, row : row + 8, outs] = w


def device(core, x, y, z):
    return (core, x * 4 + z % 4, (z // 4) * 8 + y)


ORDER = [
    (dy, side, core) for dy in (4, 3, 5, 2, 6, 1, 7, 0) for side in (0, 1) for core in (0, 1)
]
PEERS = [ORDER[i] for i in np.random.RandomState(3).permutation(32)]


def kernel(
    anchor_hbm, lamr_hbm, lamc_hbm, lamq_hbm, x_hbm, fd_hbm, fs_hbm, sh_hbm, sl_hbm, out_ref, fine_ref,
    anchor, lamr_ref, lamc_ref, lamq_ref, x_ref, fd_ref, fs_ref, sh_ref, sl_ref,
    za, zb, dd, gg, u, dtab, m1, r1, m2, r2, dint, rint, uh, ul, myh, myl, mz, mzy, mzt, wall, wys,
    mzx, rzx, my, ry, m5, r5, m6, r6, es, et, ed, fa, fb, fr, trace, tin, gz, ya, yb, yd,
    s1, q1, s2, q2, s3, q3, s4, q4, sh1, qh1, sd, qd, sz, qz, sy, qy, s5, q5, s6, q6, sin,
    st, qt, se, qe,
):
    core = lax.axis_index("grp")
    gx = lax.axis_index("gx")
    gy = lax.axis_index("gy")
    x, zl = gx // 4, gx % 4
    y, zh = gy % 8, gy // 8
    z = zh * 4 + zl
    me = core * 16 + gy
    zv = (z + 6) % 8
    lv, hv = zv % 4, zv // 4
    mid = core * 16 + hv * 8 + y
    pv = x * 4 + lv

    def to_mid(o):
        dy, side, oc = o
        ty = (y + dy + core * (8 - 2 * dy)) % 8
        tc = (core + oc) % 2
        return device(tc, x, ty, (zl + 4 * side + 2) % 8), tc * 16 + side * 8 + ty

    def to_real(o):
        dy, side, oc = o
        ty = (y + dy + core * (8 - 2 * dy)) % 8
        tc = (core + oc) % 2
        return device(tc, x, ty, lv + 4 * side), tc * 16 + side * 8 + ty

    def to_row(q):
        return device(core, q // 4, y, (q % 4 + 4 * hv + 2) % 8)

    def real_row(q):
        return device(core, q // 4, y, q % 4 + 4 * zh)

    here = (core, gx, gy)
    partner = (1 - core, gx, gy)
    own = pl.ds(pl.multiple_of(core * 128, 128), 128)

    def beside(ox, oy):
        return (core, (gx + ox + 16) % 16, (gy + oy + 16) % 16)

    fetch = []
    mine = [pl.ds(pl.multiple_of(256 * h + 8 * mid, 8), 8) for h in range(2)]
    for k, (src, dst) in enumerate((
        (x_hbm, x_ref), (sh_hbm, sh_ref), (sl_hbm, sl_ref), (fd_hbm, fd_ref), (fs_hbm, fs_ref),
        (lamr_hbm, lamr_ref), (lamq_hbm, lamq_ref), (lamc_hbm.at[mine[0], :], lamc_ref.at[0]),
        (lamc_hbm.at[mine[1], :], lamc_ref.at[1]), (anchor_hbm, anchor),
    )):
        copy = pltpu.make_async_copy(src, dst, sin.at[k])
        copy.start()
        fetch.append(copy)
    barrier = pltpu.get_barrier_semaphore()
    for o in PEERS:
        pl.semaphore_signal(barrier, inc=1, device_id=to_mid(o)[0], device_id_type=MESH)
    pl.semaphore_signal(barrier, inc=1, device_id=partner, device_id_type=MESH)
    for oy in (-1, 1):
        pl.semaphore_signal(barrier, inc=1, device_id=beside(0, oy), device_id_type=MESH)
    for k in range(1, 16):
        pl.semaphore_signal(barrier, inc=1, device_id=to_row((pv + k) % 16), device_id_type=MESH)
        pl.semaphore_signal(barrier, inc=1, device_id=real_row((gx + k) % 16), device_id_type=MESH)

    def arrived(ref, sem, index):
        pltpu.make_async_remote_copy(
            src_ref=ref.at[index], dst_ref=ref.at[index], send_sem=sem.at[index],
            recv_sem=sem.at[index], device_id=here, device_id_type=MESH,
        ).wait_recv()

    def send(src, dst, send_sem, recv_sem, target):
        copy = pltpu.make_async_remote_copy(
            src_ref=src, dst_ref=dst, send_sem=send_sem, recv_sem=recv_sem,
            device_id=target, device_id_type=MESH,
        )
        copy.start()
        return copy

    for copy in fetch[:3]:
        copy.wait()
    s_pair = (sh_ref[...], sl_ref[...])
    x_pair = split(x_ref[...].reshape(512, 512))
    halves = [slice(0, 256), slice(256, 512)]

    def forward_third(h):
        cols = tuple(part[:, halves[h]] for part in s_pair)
        za[:, :, halves[h]] = dot3(x_pair, cols, NN).reshape(32, 16, 256)
        swap_groups(za, zb.at[h], 256 * h, 0)

    t1 = [[], []]

    def send_first(h, lo, hi):
        for i in range(lo, hi):
            target, block = to_mid(PEERS[i])
            t1[h].append(
                send(zb.at[h, block], dd.at[h, me], s1.at[h, i], q1.at[h, me], target)
            )

    forward_third(0)
    for copy in fetch[3:]:
        copy.wait()
    a0, a1, a2 = anchor[0], anchor[1], anchor[2]
    fa[1:9, 8:40, own] = fs_ref[...]
    fr[1:9, 8:40, own] = fd_ref[...]
    pl.semaphore_wait(barrier, 65)
    halo = []
    for k, oy in enumerate((-1, 1)):
        rows = pl.ds(0, 8) if oy < 0 else pl.ds(24, 8)
        to_rows = pl.ds(40, 8) if oy < 0 else pl.ds(0, 8)
        for part, (src, dst) in enumerate(((fs_ref, fa), (fd_ref, fr))):
            halo.append(send(
                src.at[:, rows, :], dst.at[pl.ds(1, 8), to_rows, own],
                sh1.at[2 * k + part], qh1.at[2 * k + part], beside(0, oy),
            ))
    send_first(0, 0, 32)
    forward_third(1)
    send_first(1, 0, CUT1)
    for h in range(2):
        mu = lamr_ref[0:1, :] + jnp.concatenate([lamc_ref[h]] * 4, axis=1)

        def table(i, g, h=h, mu=mu):
            d = 1.0 / (1.0 + (mu + g))
            dtab[h, i] = d
            return (mu + g) * d

        lax.fori_loop(0, 31, table, jnp.ones((8, 512), F32))
        odd = pv % 2 == 1
        muq = jnp.where(odd, lamq_ref[2:4, :], lamq_ref[0:2, :]) + lamc_ref[h, pl.ds(pv // 2, 1), :]
        c = 0.5 * muq
        c1 = c
        r32 = 2.0 * (1.0 + c)
        for _ in range(4):
            c = 2.0 * c * (c + 2.0)
            r32 = r32 * (2.0 * (1.0 + c))
        c = 2.0 * c * (c + 2.0)
        rint[h] = r32
        g = jnp.ones((2, 128), F32)
        for i in range(15):
            d = 1.0 / (1.0 + (2.0 * c + g))
            dint[h, i] = d
            g = (2.0 * c + g) * d
        dint[h, 15] = 1.0 / (r32 * (1.0 + c1) + c + g)
    def cells(rows, cols, first):
        grid = lax.broadcasted_iota(jnp.int32, (rows, cols), 0)
        return jnp.where(grid == first, 1.0, 0.0).astype(BF16)

    lane = lax.broadcasted_iota(jnp.int32, (512, 256), 1)
    pick = cells(512, 256, a1 - 3 + 8 * (lane // 16) + lane % 16)
    myh[...] = mm(sh_ref[...], pick, NN).astype(BF16)
    myl[...] = mm(sl_ref[...], pick, NN).astype(BF16)
    lane = lax.broadcasted_iota(jnp.int32, (512, 128), 1)
    pick = cells(512, 128, a2 - 1 + 30 * core + lane)
    mz[...] = mm(sh_ref[...], pick, NN) + mm(sl_ref[...], pick, NN)
    pick = cells(512, 128, a2 - 1 + 30 * (lane // 64) + lane % 64)
    mzy[...] = mm(sh_ref[...], pick, NN) + mm(sl_ref[...], pick, NN)
    for h in range(2):
        high, low = split(jnp.concatenate([mzy[mine[h], :]] * 32, axis=0))
        mzt[h, 0] = high
        mzt[h, 1] = low

    def weights(cell, first, boxes, low_face, high_face):
        low_w = jnp.where(cell == first, 0.625, 0.0) + jnp.where(cell == first + 1, 0.375, 0.0)
        high_w = jnp.where(cell == first + boxes, 0.375, 0.0) + jnp.where(
            cell == first + boxes + 1, 0.625, 0.0
        )
        return jnp.where(low_face, low_w, 0.0) + jnp.where(high_face, high_w, 0.0)

    row = lax.broadcasted_iota(jnp.int32, (16, 512), 0)
    cell = lax.broadcasted_iota(jnp.int32, (16, 512), 1)
    wy = weights(cell, a1 - 1, 128, row == 0, row == 1).astype(BF16)
    wys[...] = mm(wy, sh_ref[...], NN) + mm(wy, sl_ref[...], NN)
    wz = weights(cell, a2 - 1, 64, row == 0, row == 1).astype(BF16)
    wz = mm(wz, sh_ref[...], NN) + mm(wz, sl_ref[...], NN)
    lane = lax.broadcasted_iota(jnp.int32, (512, 512), 1)
    pick = cells(512, 512, 256 * (lane // 256) + 8 * mid + lane % 8)
    wzh, wzl = split(wz)
    wz = mm(wzh, pick, NN) + mm(wzl, pick, NN)
    row = lax.broadcasted_iota(jnp.int32, (32, 256), 0)
    lane = lax.broadcasted_iota(jnp.int32, (32, 256), 1)
    row2 = lax.broadcasted_iota(jnp.int32, (16, 256), 0)
    lane2 = lax.broadcasted_iota(jnp.int32, (16, 256), 1)
    wx = weights(32 * pv + lane2 // 8, a0 - 1, 32, row2 < 8, row2 >= 8)
    wx = jnp.where(row2 % 8 == lane2 % 8, wx, 0.0)
    for h in range(2):
        for f in range(2):
            wall[h, 32 * f : 32 * f + 32, :] = jnp.where(
                row == lane // 8, wz[f : f + 1, halves[h]], 0.0
            )
        wall[h, 64:80, :] = wx
    for copy in halo:
        copy.wait_recv()
    pair = []
    for k, ref in enumerate((fa, fr)):
        view = ref.at[pl.ds(1, 8), :, own]
        copy = pltpu.make_async_remote_copy(
            src_ref=view, dst_ref=view, send_sem=sd.at[k], recv_sem=qd.at[k],
            device_id=partner, device_id_type=MESH,
        )
        copy.start()
        pair.append(copy)
    for copy in pair:
        copy.wait()
    fine_row = lax.broadcasted_iota(jnp.int32, (48, 256), 0) + 32 * gy
    fine_col = lax.broadcasted_iota(jnp.int32, (48, 256), 1)
    inside_y = (fine_row >= 8) & (fine_row < 520)
    sixth = jnp.where(inside_y, 1.0 / 6.0, 0.0)

    def layer(source, extra, k):
        v = source[k]
        total = (source[k - 1] + source[k + 1]) + extra[k]
        total = total + (pltpu.roll(v, 1, 0) + pltpu.roll(v, 47, 0))
        total = total + jnp.where(fine_col == 0, 0.0, pltpu.roll(v, 1, 1))
        return total + jnp.where(fine_col == 255, 0.0, pltpu.roll(v, 255, 1))

    for k in (0, 9):
        fa[k] = jnp.zeros((48, 256), F32)
        fb[k] = jnp.zeros((48, 256), F32)
    for k in range(1, 9):
        fa[k] = jnp.where(inside_y, fa[k], 0.0)
        fr[k] = fr[k] * (-1.0 / 16.0)
        es[k + 7] = fa[k]

    def alone(j, carry):
        for part, (source, target) in enumerate(((fa, fb), (fb, fa))):
            trace[0, 2 * j + part] = source[1]
            trace[1, 2 * j + part] = source[8]

            def four(k, c):
                for m in range(4):
                    index = 1 + 4 * k + m
                    target[index] = layer(source, fr, index) * sixth
                return c

            lax.fori_loop(0, 2, four, 0)
        return carry

    lax.fori_loop(0, 4, alone, 0)

    t2 = []
    t4 = [[], []]

    def second_and_eliminate(h):
        value = dd[h].reshape(512, 256)
        u[h] = dot3(split(value), s_pair, TN).reshape(32, 8, 512)
        first = -u[h, 0]
        u[h, 0] = first
        q0 = dtab[h, 30]

        def forward(i, carry):
            yv, q, e = carry
            w = u[h, i]
            yv = dtab[h, i - 1] * yv - w
            u[h, i] = yv
            q = q * dtab[h, 30 - i]
            return yv, q, e - q * w

        yv, _, e = lax.fori_loop(1, 31, forward, (first, q0, q0 * first))
        b = q0 * yv - u[h, 31]
        for j in range(4):
            start = 8 * (j // 2) + j % 2 + 4 * h
            m1[pl.ds(start, 8, stride=16), :] = e[:, 128 * j : 128 * j + 128]
            m1[pl.ds(start + 2, 8, stride=16), :] = b[:, 128 * j : 128 * j + 128]

    def send_ends():
        for k in range(1, 16):
            q = (pv + k) % 16
            t2.append(send(
                m1.at[pl.ds(pl.multiple_of(q * 8, 8), 8), :], r1.at[pv], s2.at[k], q2.at[pv],
                to_row(q),
            ))
        r1[pv] = m1[pl.ds(pl.multiple_of(pv * 8, 8), 8), :]

    def separators():
        for h in range(2):
            ys = []
            prev = None
            for p in range(16):
                end = r1[p, 4 * h + 2 : 4 * h + 4, :]
                if p < 15:
                    end = end + r1[p + 1, 4 * h : 4 * h + 2, :]
                end = rint[h] * end
                prev = end if p == 0 else end + dint[h, p - 1] * prev
                ys.append(prev)
            m2[0, 4 * h : 4 * h + 2, :] = jnp.zeros((2, 128), F32)
            sol = dint[h, 15] * ys[15]
            m2[15, 4 * h + 2 : 4 * h + 4, :] = sol
            for p in range(14, -1, -1):
                sol = dint[h, p] * (sol + ys[p])
                m2[p + 1, 4 * h : 4 * h + 2, :] = sol
                m2[p, 4 * h + 2 : 4 * h + 4, :] = sol
        for k in range(1, 16):
            q = (pv + k) % 16
            t2.append(send(
                m2.at[q], r2.at[pl.ds(pl.multiple_of(pv * 8, 8), 8), :], s3.at[k], q3.at[pv],
                to_row(q),
            ))
        r2[pl.ds(pl.multiple_of(pv * 8, 8), 8), :] = m2[pv]

    def wait_separators():
        for k in range(1, 16):
            q = (pv + k) % 16
            view = r2.at[pl.ds(pl.multiple_of(q * 8, 8), 8), :]
            pltpu.make_async_remote_copy(
                src_ref=view, dst_ref=view, send_sem=s3.at[k], recv_sem=q3.at[q],
                device_id=here, device_id_type=MESH,
            ).wait_recv()

    def substitute(h):
        starts = [8 * (j // 2) + j % 2 + 4 * h for j in range(4)]
        left = jnp.concatenate([r2[pl.ds(j, 8, stride=16), :] for j in starts], axis=1)
        right = jnp.concatenate([r2[pl.ds(j + 2, 8, stride=16), :] for j in starts], axis=1)

        def spread(i, t):
            u[h, i] = u[h, i] + t
            return dtab[h, i] * t

        lax.fori_loop(0, 31, spread, left)
        u[h, 31] = right

        def backward(k, v):
            i = 30 - k
            v = dtab[h, i] * (v + u[h, i])
            u[h, i] = v
            return v

        lax.fori_loop(0, 31, backward, right)
        high, low = split(u[h].reshape(256, 512))
        uh[h] = high
        ul[h] = low

    def inverse_second(h):
        for copy in t1[h]:
            copy.wait_send()
        zb[h] = dot3(s_pair, (uh[h], ul[h]), NT).reshape(32, 16, 256)

    def send_last(h, lo, hi):
        for i in range(lo, hi):
            target, block = to_real(PEERS[i])
            t4[h].append(
                send(zb.at[h, block], gg.at[h, mid], s4.at[h, i], q4.at[h, mid], target)
            )

    tt = []

    def send_traces(part):
        sweeps = pl.ds(4 * part, 4)
        for side, ox in enumerate((-1, 1)):
            tt.append(send(
                trace.at[side, sweeps, :, own], tin.at[1 - side, sweeps, :, own],
                st.at[side, part], qt.at[1 - side, part], beside(ox, 0),
            ))

    for s in range(32):
        arrived(dd.at[0], q1.at[0], s)
    second_and_eliminate(0)
    for s in range(32):
        arrived(dd.at[1], q1.at[1], s)
    second_and_eliminate(1)
    send_ends()
    send_traces(0)
    send_traces(1)
    for k in range(1, 16):
        arrived(r1, q2, (pv + k) % 16)
    separators()
    wait_separators()
    substitute(0)
    inverse_second(0)
    send_last(0, 0, CUT4A)
    substitute(1)
    face = []
    line = []
    cut_x = []
    row = lax.broadcasted_iota(jnp.int32, (32, 256), 0)
    lanes = lax.broadcasted_iota(jnp.int32, (32, 256), 1)

    def faces(h):
        pair_h = (uh[h], ul[h])
        rows = dot3(split(wall[h]), pair_h, NN)
        face.append(rows[:64])
        cut_x.append(rows[64:])
        ay = dot3(split(wys[...]), pair_h, NT)
        both = jnp.concatenate(
            [jnp.where(row == lanes // 8, ay[f : f + 1, :], 0.0) for f in range(2)], axis=0
        )
        line.append(dot3(split(both), (mzt[h, 0], mzt[h, 1]), NN))

    faces(0)
    faces(1)
    rows = jnp.concatenate([face[0] + face[1], cut_x[0], cut_x[1]], axis=0)
    rows = dot3(split(rows), (myh[...], myl[...]), NN)
    lane = lax.broadcasted_iota(jnp.int32, (8, 128), 1) // 16
    for f in range(2):
        for t in range(2):
            cols = slice(128 * t, 128 * t + 128)
            v = [rows[32 * f + 8 * k : 32 * f + 8 * k + 8, cols] for k in range(4)]
            for g in range(2):
                for h in range(2):
                    start = 64 + 16 * h + 8 * g
                    v.append(rows[start : start + 8, cols])
            for q, w in enumerate(exchange8(v, lane)):
                mzx[16 * f + 8 * t + q] = w
    line_sum = line[0] + line[1]
    half = lax.broadcasted_iota(jnp.int32, (16, 128), 1) < 64
    for f in range(2):
        top, bottom = line_sum[32 * f : 32 * f + 16], line_sum[32 * f + 16 : 32 * f + 32]
        my[f, 0] = jnp.where(half, top, pltpu.roll(bottom, 64, 1))
        my[f, 1] = jnp.where(half, pltpu.roll(top, 64, 1), bottom)
    tz = []
    for i, o in enumerate(PEERS):
        target, block = to_real(o)
        tz.append(send(mzx.at[block], rzx.at[mid], sz.at[i], qz.at[mid], target))
    for f in range(2):
        for g in range(2):
            tz.append(send(
                my.at[f, g], ry.at[mid], sy.at[2 * f + g], qy.at[mid],
                device(g, x, 7 * f, lv + 4 * f),
            ))
    send_last(0, CUT4A, 32)
    inverse_second(1)
    send_last(1, 0, CUT4B)
    te = []
    for part in range(2):
        sweeps = pl.ds(4 * part, 4)
        for side in range(2):
            view = tin.at[side, sweeps, :, own]
            pltpu.make_async_remote_copy(
                src_ref=view, dst_ref=view, send_sem=st.at[side, part],
                recv_sem=qt.at[side, part], device_id=here, device_id_type=MESH,
            ).wait_recv()
            te.append(send(view, view, se.at[side, part], qe.at[side, part], partner))
    for copy in te:
        copy.wait_recv()
    def factor(k):
        inside_x = (k + 8 * gx >= 8) & (k + 8 * gx < 136)
        return jnp.where(inside_x, sixth, 0.0)

    ends = (jnp.where(gx == 0, 0.0, sixth), jnp.where(gx == 15, 0.0, sixth))
    for k in (4, 5, 6, 7, 16, 17, 18, 19):
        es[k] = jnp.zeros((48, 256), F32)
        ed[k] = jnp.zeros((48, 256), F32)
    for k in (3, 4, 5, 6, 17, 18, 19, 20):
        et[k] = jnp.zeros((48, 256), F32)
    for k in range(8, 16):
        ed[k] = fr[k - 7]
    for j in range(8):
        source, target = ((es, et), (et, es))[j % 2]
        depth = min(j + 1, 7 - j)

        def some(k, c, source=source, target=target, first=8 - depth, step=WIDE):
            for m in range(step):
                index = first + step * k + m
                target[index] = layer(source, ed, index) * factor(index)
            return c

        layers = 8 + 2 * depth
        lax.fori_loop(0, layers // WIDE, some, 0)
        if layers % WIDE:
            some(0, 0, first=8 - depth + layers // WIDE * WIDE, step=layers % WIDE)
        target[8] = target[8] + tin[0, j] * ends[0]
        target[15] = target[15] + tin[1, j] * ends[1]
    for s in range(32):
        arrived(rzx, qz, s)
    zsum = rzx[0]
    for s in range(1, 32):
        zsum = zsum + rzx[s]
    got = rzx[...].reshape(256, 128)
    parts = [full(got, mz[256 * k : 256 * k + 256, :], TN) for k in range(2)]
    for f in range(2):
        m6[f] = parts[0][64 + 32 * f : 80 + 32 * f] + parts[1][80 + 32 * f : 96 + 32 * f]
    row = lax.broadcasted_iota(jnp.int32, (128, 32), 0)
    col = lax.broadcasted_iota(jnp.int32, (128, 32), 1)
    pick = jnp.where(a0 - 3 + 2 * (row // 8) + row % 8 == 32 * gx + col, 1.0, 0.0)
    spread_z = jnp.concatenate([jnp.where(lane == h, zsum, 0.0) for h in range(4)], axis=0)
    m5[:, 0] = full(pick, spread_z, NN).reshape(16, 8, 128)
    m5[:, 1] = jnp.zeros((16, 8, 128), F32)
    at_y = (gy == 0) | (gy == 15)

    @pl.when(at_y)
    def _():
        for s in range(32):
            arrived(ry, qy, s)
        ysum = ry[0]
        for s in range(1, 32):
            ysum = ysum + ry[s]
        top = full(pick[:, :16], ysum, NN)
        bottom = full(pick[:, 16:], ysum, NN)
        left_half = lax.broadcasted_iota(jnp.int32, (128, 128), 1) < 64
        m5[:, 1] = jnp.where(left_half, top, bottom).reshape(16, 8, 128)

    t5 = []
    for k in range(1, 16):
        q = (gx + k) % 16
        copy = pltpu.make_async_remote_copy(
            src_ref=m5.at[q], dst_ref=r5.at[gx], send_sem=s5.at[k], recv_sem=q5.at[gx],
            device_id=real_row(q), device_id_type=MESH,
        )
        copy.start()
        t5.append(copy)
    r5[gx] = m5[gx]
    for f in range(2):
        end = 15 * f
        copy = pltpu.make_async_remote_copy(
            src_ref=m6.at[f], dst_ref=r6.at[gx], send_sem=s6.at[f], recv_sem=q6.at[gx],
            device_id=real_row(end), device_id_type=MESH,
        )

        @pl.when(gx != end)
        def _():
            copy.start()

        @pl.when(gx == end)
        def _():
            r6[gx] = m6[f]


    send_last(1, CUT4B, 32)
    for s in range(32):
        arrived(gg.at[0], q4.at[0], s)
    def inverse_third(h):
        swap_groups(gg.at[h], za, 0, 256 * h)
        rows_h = tuple(part[halves[h], :] for part in s_pair)
        return dot3(split(za[:, :, halves[h]].reshape(512, 256)), rows_h, NN).reshape(32, 16, 512)

    out_ref[...] = inverse_third(0)
    for s in range(32):
        arrived(gg.at[1], q4.at[1], s)
    out_ref[...] = out_ref[...] + inverse_third(1)
    for k in range(1, 16):
        arrived(r5, q5, (gx + k) % 16)
    def interpolate(fine, cell):
        scaled = 2 * fine + 5
        bottom = scaled // 8
        t = (scaled % 8).astype(F32) * 0.125
        return jnp.where(cell == bottom, 1.0 - t, 0.0) + jnp.where(cell == bottom + 1, t, 0.0)

    def grid(shape):
        return (lax.broadcasted_iota(jnp.int32, shape, 0), lax.broadcasted_iota(jnp.int32, shape, 1))

    row, col = grid((24, 8))
    int_x = interpolate(row, col)
    row, col = grid((128, 128))
    int_y = jnp.where((col < 64) & (row < 48), interpolate(row, col % 16), 0.0)
    zb5 = r5[0, 0]
    yb5 = r5[0, 1]
    for s in range(1, 16):
        zb5 = zb5 + r5[s, 0]
        yb5 = yb5 + r5[s, 1]
    ghost_z = full(full(int_x, zb5, NN), int_y, NT)
    row, col = grid((24, 128))
    inside = (row + 8 * gx >= 8) & (row + 8 * gx < 136) & (col < 48)
    inside = inside & (col + 32 * gy >= 8) & (col + 32 * gy < 520)
    sixth_z = jnp.where(inside, 1.0 / 6.0, 0.0)
    plane = []
    for j in range(8):
        new = []
        for k in range(j + 1):
            total = ghost_z if k == 0 else plane[k - 1]
            if k + 1 < j:
                total = total + plane[k + 1]
            if k < j:
                v = plane[k]
                total = total + (pltpu.roll(v, 1, 0) + pltpu.roll(v, 23, 0))
                total = total + (pltpu.roll(v, 1, 1) + pltpu.roll(v, 127, 1))
            new.append(total * sixth_z)
        plane = new
    for k in range(8):
        gz[pl.ds(k, 24, stride=8), :] = plane[k]
    row, col = grid((8, 128))
    place = jnp.where(col == jnp.where(core == 0, row, 127 - row), 1.0, 0.0)
    for k in range(8):
        part = full(gz[8 * (k + 8) : 8 * (k + 8) + 8, :], place, TN)
        fine_ref[k] = es[k + 8, 8:40, own] + part[8:40]

    row, col = grid((128, 256))
    int_z = interpolate(col, row % 64 + 30 * core)

    row8 = lax.broadcasted_iota(jnp.int32, (8, 256), 0)
    col8 = lax.broadcasted_iota(jnp.int32, (8, 256), 1)
    for f in range(2):
        @pl.when(gy == 15 * f)
        def _():
            ghost_y = full(full(int_x, yb5, NN), int_z, NN)
            edge = 7 * f
            for k in range(24):
                yd[k] = jnp.where(row8 == edge, ghost_y[k : k + 1], 0.0)
            for j in range(8):
                source, target = ((ya, yb), (yb, ya))[j % 2]

                def one(k, c, source=source, target=target, j=j):
                    total = yd[k]
                    if j:
                        v = source[k]
                        total = total + source[k - 1] + source[k + 1]
                        total = total + jnp.where(row8 == 0, 0.0, pltpu.roll(v, 1, 0))
                        total = total + jnp.where(row8 == 7, 0.0, pltpu.roll(v, 7, 0))
                        total = total + jnp.where(col8 == 0, 0.0, pltpu.roll(v, 1, 1))
                        total = total + jnp.where(col8 == 255, 0.0, pltpu.roll(v, 255, 1))
                    inside_x = (k + 8 * gx >= 8) & (k + 8 * gx < 136)
                    target[k] = total * jnp.where(inside_x, 1.0 / 6.0, 0.0)
                    return c

                for k in range(j + 1, 23 - j):
                    one(k, 0)
            rows = pl.ds(24 * f, 8)
            for k in range(8):
                fine_ref[k, rows, :] = fine_ref[k, rows, :] + ya[k + 8, :, own]

    for f in range(2):
        @pl.when(gx == 15 * f)
        def _():
            for k in range(16):
                if k != 15 * f:
                    arrived(r6, q6, k)
            xb6 = r6[0]
            for s in range(1, 16):
                xb6 = xb6 + r6[s]
            row, col = grid((48, 16))
            near_y = interpolate(row, col)
            row, col = grid((128, 256))
            near_z = jnp.where(row < 64, int_z, 0.0)
            ghost_x = full(full(near_y, xb6, NN), near_z, NN)
            for k in range(1, 9):
                fr[k] = jnp.zeros((48, 256), F32)
                fa[k] = jnp.zeros((48, 256), F32)
                fb[k] = jnp.zeros((48, 256), F32)
            fr[1 + 7 * f] = ghost_x
            for j in range(8):
                source, target = ((fa, fb), (fb, fa))[j % 2]
                for k in range(j + 1):
                    index = 8 - k if f else 1 + k
                    target[index] = layer(source, fr, index) * sixth
            for k in range(8):
                fine_ref[k] = fine_ref[k] + fa[k + 1, 8:40, own]

    for copy in t2 + t4[0] + t4[1] + tz + t5 + halo + tt + te:
        copy.wait_send()
    for f in range(2):
        @pl.when(gx != 15 * f)
        def _():
            pltpu.make_async_remote_copy(
                src_ref=m6.at[f], dst_ref=r6.at[gx], send_sem=s6.at[f], recv_sem=q6.at[gx],
                device_id=real_row(15 * f), device_id_type=MESH,
            ).wait_send()


def body(density, fine_density, fine_start, anchor):
    high, low, lam = tables()
    vm = pl.BlockSpec(memory_space=pltpu.VMEM)
    dma = pltpu.SemaphoreType.DMA

    def f32(*shape):
        return pltpu.VMEM(shape, F32)

    def b16(*shape):
        return pltpu.VMEM(shape, BF16)

    big = f32(32, 16, 512)
    return pl.pallas_call(
        kernel,
        out_shape=(
            jax.ShapeDtypeStruct((32, 16, 512), F32), jax.ShapeDtypeStruct((8, 32, 128), F32)
        ),
        in_specs=[pl.BlockSpec(memory_space=pl.ANY)] * 9,
        out_specs=(vm, vm),
        scratch_shapes=[
            pltpu.SMEM((3,), jnp.int32), f32(8, 512), f32(2, 8, 128), f32(8, 128),
            big, f32(8, 32, 128), f32(8, 32, 128), b16(512, 512), b16(512, 512),
            big, f32(2, 32, 16, 256), f32(2, 32, 16, 256), f32(2, 32, 16, 256),
            f32(2, 32, 8, 512), f32(2, 31, 8, 512),
            f32(128, 128), f32(16, 8, 128), f32(16, 8, 128), f32(128, 128),
            f32(2, 16, 2, 128), f32(2, 2, 128),
            b16(2, 256, 512), b16(2, 256, 512), b16(512, 256), b16(512, 256),
            f32(512, 128), f32(512, 128), b16(2, 2, 256, 128), f32(2, 80, 256), f32(16, 512),
            f32(32, 8, 128), f32(32, 8, 128), f32(2, 2, 16, 128), f32(32, 16, 128),
            f32(16, 2, 8, 128), f32(16, 2, 8, 128), f32(2, 16, 128), f32(16, 16, 128),
            f32(24, 48, 256), f32(24, 48, 256), f32(24, 48, 256),
            f32(10, 48, 256), f32(10, 48, 256), f32(10, 48, 256),
            f32(2, 8, 48, 256), f32(2, 8, 48, 256), f32(192, 128),
            f32(24, 8, 256), f32(24, 8, 256), f32(24, 8, 256),
            dma((2, 32)), dma((2, 32)), dma((16,)), dma((16,)), dma((16,)), dma((16,)),
            dma((2, 32)), dma((2, 32)), dma((4,)), dma((4,)), dma((2,)), dma((2,)),
            dma((32,)), dma((32,)), dma((4,)), dma((32,)), dma((16,)), dma((16,)),
            dma((2,)), dma((16,)), dma((10,)), dma((2, 2)), dma((2, 2)), dma((2, 2)), dma((2, 2)),
        ],
        compiler_params=pltpu.CompilerParams(
            collective_id=0, has_side_effects=True, vmem_limit_bytes=56 << 20
        ),
    )(anchor, jnp.asarray(np.tile(lam.reshape(1, 512), (8, 1))),
      jnp.asarray(np.tile(lam.reshape(512, 1), (1, 128))),
      jnp.asarray(np.tile(lam.reshape(4, 128), (2, 1))), density, fine_density, fine_start,
      jnp.asarray(high), jnp.asarray(low))


def solution(mesh):
    return jax.shard_map(
        body,
        mesh=mesh,
        in_specs=(P("gx", ("grp", "gy"), None), P("gx", "gy", "grp"), P("gx", "gy", "grp"), P()),
        out_specs=(P("gx", ("grp", "gy"), None), P("gx", "gy", "grp")),
        check_vma=False,
    )
```

```python
import functools
import math

import jax
import jax.numpy as jnp
import numpy as np
from jax import lax
from jax.experimental import pallas as pl
from jax.experimental.pallas import tpu as pltpu
from jax.sharding import PartitionSpec as P

MESH = pl.DeviceIdType.MESH
NC = 512
F32 = jnp.float32
CUT1, CUT4A, CUT4B = 32, 16, 32
WIDE = 4
BF16 = jnp.bfloat16


def tables():
    index = np.arange(1, NC + 1, dtype=np.int64)
    angle = (index[:, None] * index[None, :]) % (2 * (NC + 1))
    sine = math.sqrt(2.0 / (NC + 1)) * np.sin(angle * (math.pi / (NC + 1)))
    sine = sine.astype(np.float32)
    high = sine.astype(jnp.bfloat16)
    low = (sine - high.astype(np.float32)).astype(jnp.bfloat16)
    lam = 4.0 * np.sin(index * (math.pi / (2 * (NC + 1)))) ** 2
    return high, low, lam.astype(np.float32)


def split(value):
    high = value.astype(BF16)
    low = (value - high.astype(F32)).astype(BF16)
    return high, low


def dot3(a, b, dims):
    ah, al = a
    bh, bl = b
    dd = functools.partial(
        lax.dot_general, dimension_numbers=(dims, ((), ())), preferred_element_type=F32
    )
    return dd(ah, bh) + (dd(al, bh) + dd(ah, bl))


def mm(a, b, dims):
    return lax.dot_general(a, b, (dims, ((), ())), preferred_element_type=F32)


def full(a, b, dims):
    return lax.dot_general(
        a, b, (dims, ((), ())), precision=lax.Precision.HIGHEST, preferred_element_type=F32
    )


NN = ((1,), (0,))
NT = ((1,), (1,))
TN = ((0,), (0,))


def exchange(v, lane):
    v = list(v)
    for bit in (1, 2, 4, 8):
        upper = (lane & bit) != 0
        for i in range(16):
            if i & bit:
                continue
            a, c = v[i], v[i | bit]
            v[i] = jnp.where(upper, pltpu.roll(c, 8 * bit, 1), a)
            v[i | bit] = jnp.where(upper, c, pltpu.roll(a, 128 - 8 * bit, 1))
    return v


def exchange8(v, lane):
    v = list(v)
    for bit in (1, 2, 4):
        upper = (lane & bit) != 0
        for i in range(8):
            if i & bit:
                continue
            a, c = v[i], v[i | bit]
            v[i] = jnp.where(upper, pltpu.roll(c, 16 * bit, 1), a)
            v[i | bit] = jnp.where(upper, c, pltpu.roll(a, 128 - 16 * bit, 1))
    return v


def swap_groups(source, target, first, out_first):
    lane = lax.broadcasted_iota(jnp.int32, (8, 128), 1) // 8
    for a in range(2):
        for b in range(2):
            cols = slice(first + 128 * b, first + 128 * b + 128)
            outs = slice(out_first + 128 * a, out_first + 128 * a + 128)
            for row in (0, 8):
                v = [source[16 * a + q, row : row + 8, cols] for q in range(16)]
                for q, w in enumerate(exchange(v, lane)):
                    target[16 * b + q, row : row + 8, outs] = w


def device(core, x, y, z):
    return (core, x * 4 + z % 4, (z // 4) * 8 + y)


ORDER = [
    (dy, side, core) for dy in (4, 3, 5, 2, 6, 1, 7, 0) for side in (0, 1) for core in (0, 1)
]
PEERS = [ORDER[i] for i in np.random.RandomState(3).permutation(32)]


def kernel(
    anchor_hbm, lamr_hbm, lamc_hbm, lamq_hbm, x_hbm, fd_hbm, fs_hbm, sh_hbm, sl_hbm, out_ref, fine_ref,
    anchor, lamr_ref, lamc_ref, lamq_ref, x_ref, fd_ref, fs_ref, sh_ref, sl_ref,
    za, zb, dd, gg, u, dtab, m1, r1, m2, r2, dint, rint, uh, ul, myh, myl, mz, wall, wys,
    mzx, rzx, my, ry, m5, r5, m6, r6, es, et, ed, fa, fb, fr, trace, tin, gz, ya, yb, yd,
    s1, q1, s2, q2, s3, q3, s4, q4, sh1, qh1, sd, qd, sz, qz, sy, qy, s5, q5, s6, q6, sin,
    st, qt, se, qe, sv, qv,
):
    core = lax.axis_index("grp")
    gx = lax.axis_index("gx")
    gy = lax.axis_index("gy")
    x, zl = gx // 4, gx % 4
    y, zh = gy % 8, gy // 8
    z = zh * 4 + zl
    me = core * 16 + gy
    zv = (z + 6) % 8
    lv, hv = zv % 4, zv // 4
    mid = core * 16 + hv * 8 + y
    pv = x * 4 + lv

    def to_mid(o):
        dy, side, oc = o
        ty = (y + dy + core * (8 - 2 * dy)) % 8
        tc = (core + oc) % 2
        return device(tc, x, ty, (zl + 4 * side + 2) % 8), tc * 16 + side * 8 + ty

    def to_real(o):
        dy, side, oc = o
        ty = (y + dy + core * (8 - 2 * dy)) % 8
        tc = (core + oc) % 2
        return device(tc, x, ty, lv + 4 * side), tc * 16 + side * 8 + ty

    def to_row(q):
        return device(core, q // 4, y, (q % 4 + 4 * hv + 2) % 8)

    def real_row(q):
        return device(core, q // 4, y, q % 4 + 4 * zh)

    here = (core, gx, gy)
    partner = (1 - core, gx, gy)
    own = pl.ds(pl.multiple_of(core * 128, 128), 128)

    def beside(ox, oy):
        return (core, (gx + ox + 16) % 16, (gy + oy + 16) % 16)

    fetch = []
    mine = [pl.ds(pl.multiple_of(256 * h + 8 * mid, 8), 8) for h in range(2)]
    for k, (src, dst) in enumerate((
        (x_hbm, x_ref), (sh_hbm, sh_ref), (sl_hbm, sl_ref), (fd_hbm, fd_ref), (fs_hbm, fs_ref),
        (lamr_hbm, lamr_ref), (lamq_hbm, lamq_ref), (lamc_hbm.at[mine[0], :], lamc_ref.at[0]),
        (lamc_hbm.at[mine[1], :], lamc_ref.at[1]), (anchor_hbm, anchor),
    )):
        copy = pltpu.make_async_copy(src, dst, sin.at[k])
        copy.start()
        fetch.append(copy)
    barrier = pltpu.get_barrier_semaphore()
    for o in PEERS:
        pl.semaphore_signal(barrier, inc=1, device_id=to_mid(o)[0], device_id_type=MESH)
    pl.semaphore_signal(barrier, inc=1, device_id=partner, device_id_type=MESH)
    for oy in (-1, 1):
        pl.semaphore_signal(barrier, inc=1, device_id=beside(0, oy), device_id_type=MESH)
    for k in range(1, 16):
        pl.semaphore_signal(barrier, inc=1, device_id=to_row((pv + k) % 16), device_id_type=MESH)
        pl.semaphore_signal(barrier, inc=1, device_id=real_row((gx + k) % 16), device_id_type=MESH)

    def arrived(ref, sem, index):
        pltpu.make_async_remote_copy(
            src_ref=ref.at[index], dst_ref=ref.at[index], send_sem=sem.at[index],
            recv_sem=sem.at[index], device_id=here, device_id_type=MESH,
        ).wait_recv()

    has_y = (gy > 0, gy < 15)
    has_x = (gx > 0, gx < 15)

    def prepare(src, dst, send_sem, recv_sem, target):
        return pltpu.make_async_remote_copy(
            src_ref=src, dst_ref=dst, send_sem=send_sem, recv_sem=recv_sem,
            device_id=target, device_id_type=MESH,
        )

    def send(*args):
        copy = prepare(*args)
        copy.start()
        return copy

    for copy in fetch[:3]:
        copy.wait()
    s_pair = (sh_ref[...], sl_ref[...])
    x_pair = split(x_ref[...].reshape(512, 512))
    halves = [slice(0, 256), slice(256, 512)]

    def forward_third(h):
        cols = tuple(part[:, halves[h]] for part in s_pair)
        za[:, :, halves[h]] = dot3(x_pair, cols, NN).reshape(32, 16, 256)
        swap_groups(za, zb.at[h], 256 * h, 0)

    t1 = [[], []]

    def send_first(h, lo, hi):
        for i in range(lo, hi):
            target, block = to_mid(PEERS[i])
            t1[h].append(
                send(zb.at[h, block], dd.at[h, me], s1.at[h, i], q1.at[h, me], target)
            )

    forward_third(0)
    for copy in fetch[3:]:
        copy.wait()
    a0, a1, a2 = anchor[0], anchor[1], anchor[2]
    fa[1:9, 8:40, own] = fs_ref[...]
    fr[1:9, 8:40, own] = fd_ref[...]
    pl.semaphore_wait(barrier, 65)
    halo = []
    for k, oy in enumerate((-1, 1)):
        rows = pl.ds(0, 8) if oy < 0 else pl.ds(24, 8)
        to_rows = pl.ds(40, 8) if oy < 0 else pl.ds(0, 8)
        for part, (src, dst) in enumerate(((fs_ref, fa), (fd_ref, fr))):
            copy = prepare(
                src.at[:, rows, :], dst.at[pl.ds(1, 8), to_rows, own],
                sh1.at[2 * k + part], qh1.at[2 * k + part], beside(0, oy),
            )
            pl.when(has_y[k])(copy.start)
            halo.append((copy, has_y[k], has_y[1 - k]))
    send_first(0, 0, 32)
    forward_third(1)
    send_first(1, 0, CUT1)
    for h in range(2):
        mu = lamr_ref[0:1, :] + jnp.concatenate([lamc_ref[h]] * 4, axis=1)

        def table(i, g, h=h, mu=mu):
            d = 1.0 / (1.0 + (mu + g))
            dtab[h, i] = d
            return (mu + g) * d

        lax.fori_loop(0, 31, table, jnp.ones((8, 512), F32))
        odd = pv % 2 == 1
        muq = jnp.where(odd, lamq_ref[2:4, :], lamq_ref[0:2, :]) + lamc_ref[h, pl.ds(pv // 2, 1), :]
        c = 0.5 * muq
        c1 = c
        r32 = 2.0 * (1.0 + c)
        for _ in range(4):
            c = 2.0 * c * (c + 2.0)
            r32 = r32 * (2.0 * (1.0 + c))
        c = 2.0 * c * (c + 2.0)
        rint[h] = r32
        g = jnp.ones((2, 128), F32)
        for i in range(15):
            d = 1.0 / (1.0 + (2.0 * c + g))
            dint[h, i] = d
            g = (2.0 * c + g) * d
        dint[h, 15] = 1.0 / (r32 * (1.0 + c1) + c + g)
    def cells(rows, cols, first):
        grid = lax.broadcasted_iota(jnp.int32, (rows, cols), 0)
        return jnp.where(grid == first, 1.0, 0.0).astype(BF16)

    lane = lax.broadcasted_iota(jnp.int32, (512, 256), 1)
    pick = cells(512, 256, a1 - 3 + 8 * (lane // 16) + lane % 16)
    myh[...] = mm(sh_ref[...], pick, NN).astype(BF16)
    myl[...] = mm(sl_ref[...], pick, NN).astype(BF16)
    lane = lax.broadcasted_iota(jnp.int32, (512, 128), 1)
    pick = cells(512, 128, a2 - 1 + 30 * core + lane)
    mz[...] = mm(sh_ref[...], pick, NN) + mm(sl_ref[...], pick, NN)
    def weights(cell, first, boxes, low_face, high_face):
        low_w = jnp.where(cell == first, 0.625, 0.0) + jnp.where(cell == first + 1, 0.375, 0.0)
        high_w = jnp.where(cell == first + boxes, 0.375, 0.0) + jnp.where(
            cell == first + boxes + 1, 0.625, 0.0
        )
        return jnp.where(low_face, low_w, 0.0) + jnp.where(high_face, high_w, 0.0)

    row = lax.broadcasted_iota(jnp.int32, (16, 512), 0)
    cell = lax.broadcasted_iota(jnp.int32, (16, 512), 1)
    wy = weights(cell, a1 - 1, 128, row == 0, row == 1).astype(BF16)
    wys[...] = mm(wy, sh_ref[...], NN) + mm(wy, sl_ref[...], NN)
    wz = weights(cell, a2 - 1, 64, row == 0, row == 1).astype(BF16)
    wz = mm(wz, sh_ref[...], NN) + mm(wz, sl_ref[...], NN)
    lane = lax.broadcasted_iota(jnp.int32, (512, 512), 1)
    pick = cells(512, 512, 256 * (lane // 256) + 8 * mid + lane % 8)
    wzh, wzl = split(wz)
    wz = mm(wzh, pick, NN) + mm(wzl, pick, NN)
    row = lax.broadcasted_iota(jnp.int32, (32, 256), 0)
    lane = lax.broadcasted_iota(jnp.int32, (32, 256), 1)
    row2 = lax.broadcasted_iota(jnp.int32, (16, 256), 0)
    lane2 = lax.broadcasted_iota(jnp.int32, (16, 256), 1)
    wx = weights(32 * pv + lane2 // 8, a0 - 1, 32, row2 < 8, row2 >= 8)
    wx = jnp.where(row2 % 8 == lane2 % 8, wx, 0.0)
    for h in range(2):
        for f in range(2):
            wall[h, 32 * f : 32 * f + 32, :] = jnp.where(
                row == lane // 8, wz[f : f + 1, halves[h]], 0.0
            )
        wall[h, 64:80, :] = wx
    for copy, _, comes in halo:
        pl.when(comes)(copy.wait_recv)
    pair = []
    for k, ref in enumerate((fa, fr)):
        view = ref.at[pl.ds(1, 8), :, own]
        copy = pltpu.make_async_remote_copy(
            src_ref=view, dst_ref=view, send_sem=sd.at[k], recv_sem=qd.at[k],
            device_id=partner, device_id_type=MESH,
        )
        copy.start()
        pair.append(copy)
    for copy in pair:
        copy.wait()
    fine_row = lax.broadcasted_iota(jnp.int32, (48, 256), 0) + 32 * gy
    fine_col = lax.broadcasted_iota(jnp.int32, (48, 256), 1)
    inside_y = (fine_row >= 8) & (fine_row < 520)
    sixth = jnp.where(inside_y, 1.0 / 6.0, 0.0)

    def layer(source, extra, k):
        v = source[k]
        total = (source[k - 1] + source[k + 1]) + extra[k]
        total = total + (pltpu.roll(v, 1, 0) + pltpu.roll(v, 47, 0))
        total = total + jnp.where(fine_col == 0, 0.0, pltpu.roll(v, 1, 1))
        return total + jnp.where(fine_col == 255, 0.0, pltpu.roll(v, 255, 1))

    for k in (0, 9):
        fa[k] = jnp.zeros((48, 256), F32)
        fb[k] = jnp.zeros((48, 256), F32)
    for k in range(1, 9):
        fa[k] = jnp.where(inside_y, fa[k], 0.0)
        fr[k] = jnp.where(inside_y, fr[k], 0.0) * (-1.0 / 16.0)
        es[k + 7] = fa[k]

    def alone(j, carry):
        for part, (source, target) in enumerate(((fa, fb), (fb, fa))):
            trace[0, 2 * j + part] = source[1]
            trace[1, 2 * j + part] = source[8]

            def four(k, c):
                for m in range(4):
                    index = 1 + 4 * k + m
                    target[index] = layer(source, fr, index) * sixth
                return c

            lax.fori_loop(0, 2, four, 0)
        return carry

    lax.fori_loop(0, 4, alone, 0)

    t2 = []
    t4 = [[], []]

    def second_and_eliminate(h):
        value = dd[h].reshape(512, 256)
        u[h] = dot3(split(value), s_pair, TN).reshape(32, 8, 512)
        first = -u[h, 0]
        u[h, 0] = first
        q0 = dtab[h, 30]

        def forward(i, carry):
            yv, q, e = carry
            w = u[h, i]
            yv = dtab[h, i - 1] * yv - w
            u[h, i] = yv
            q = q * dtab[h, 30 - i]
            return yv, q, e - q * w

        yv, _, e = lax.fori_loop(1, 31, forward, (first, q0, q0 * first))
        b = q0 * yv - u[h, 31]
        for j in range(4):
            start = 8 * (j // 2) + j % 2 + 4 * h
            m1[pl.ds(start, 8, stride=16), :] = e[:, 128 * j : 128 * j + 128]
            m1[pl.ds(start + 2, 8, stride=16), :] = b[:, 128 * j : 128 * j + 128]

    def send_ends():
        for k in range(1, 16):
            q = (pv + k) % 16
            t2.append(send(
                m1.at[pl.ds(pl.multiple_of(q * 8, 8), 8), :], r1.at[pv], s2.at[k], q2.at[pv],
                to_row(q),
            ))
        r1[pv] = m1[pl.ds(pl.multiple_of(pv * 8, 8), 8), :]

    def separators():
        for h in range(2):
            ys = []
            prev = None
            for p in range(16):
                end = r1[p, 4 * h + 2 : 4 * h + 4, :]
                if p < 15:
                    end = end + r1[p + 1, 4 * h : 4 * h + 2, :]
                end = rint[h] * end
                prev = end if p == 0 else end + dint[h, p - 1] * prev
                ys.append(prev)
            m2[0, 4 * h : 4 * h + 2, :] = jnp.zeros((2, 128), F32)
            sol = dint[h, 15] * ys[15]
            m2[15, 4 * h + 2 : 4 * h + 4, :] = sol
            for p in range(14, -1, -1):
                sol = dint[h, p] * (sol + ys[p])
                m2[p + 1, 4 * h : 4 * h + 2, :] = sol
                m2[p, 4 * h + 2 : 4 * h + 4, :] = sol
        for k in range(1, 16):
            q = (pv + k) % 16
            t2.append(send(
                m2.at[q], r2.at[pl.ds(pl.multiple_of(pv * 8, 8), 8), :], s3.at[k], q3.at[pv],
                to_row(q),
            ))
        r2[pl.ds(pl.multiple_of(pv * 8, 8), 8), :] = m2[pv]

    def wait_separators():
        for k in range(1, 16):
            q = (pv + k) % 16
            view = r2.at[pl.ds(pl.multiple_of(q * 8, 8), 8), :]
            pltpu.make_async_remote_copy(
                src_ref=view, dst_ref=view, send_sem=s3.at[k], recv_sem=q3.at[q],
                device_id=here, device_id_type=MESH,
            ).wait_recv()

    def substitute(h):
        starts = [8 * (j // 2) + j % 2 + 4 * h for j in range(4)]
        left = jnp.concatenate([r2[pl.ds(j, 8, stride=16), :] for j in starts], axis=1)
        right = jnp.concatenate([r2[pl.ds(j + 2, 8, stride=16), :] for j in starts], axis=1)

        def spread(i, t):
            u[h, i] = u[h, i] + t
            return dtab[h, i] * t

        lax.fori_loop(0, 31, spread, left)
        u[h, 31] = right

        def backward(k, v):
            i = 30 - k
            v = dtab[h, i] * (v + u[h, i])
            u[h, i] = v
            return v

        lax.fori_loop(0, 31, backward, right)
        high, low = split(u[h].reshape(256, 512))
        uh[h] = high
        ul[h] = low

    def inverse_second(h):
        for copy in t1[h]:
            copy.wait_send()
        zb[h] = dot3(s_pair, (uh[h], ul[h]), NT).reshape(32, 16, 256)

    def send_last(h, lo, hi):
        for i in range(lo, hi):
            target, block = to_real(PEERS[i])
            t4[h].append(
                send(zb.at[h, block], gg.at[h, mid], s4.at[h, i], q4.at[h, mid], target)
            )

    tt = []

    def send_traces(part):
        sweeps = pl.ds(4 * part, 4)
        for side, ox in enumerate((-1, 1)):
            copy = prepare(
                trace.at[side, sweeps, pl.ds(8, 32), own],
                tin.at[1 - side, sweeps, pl.ds(8, 32), own],
                st.at[side, part], qt.at[1 - side, part], beside(ox, 0),
            )
            pl.when(has_x[side])(copy.start)
            tt.append((copy, has_x[side]))

    for s in range(32):
        arrived(dd.at[0], q1.at[0], s)
    second_and_eliminate(0)
    for s in range(32):
        arrived(dd.at[1], q1.at[1], s)
    second_and_eliminate(1)
    send_ends()
    send_traces(0)
    send_traces(1)
    for k in range(1, 16):
        arrived(r1, q2, (pv + k) % 16)
    separators()
    wait_separators()
    substitute(0)
    inverse_second(0)
    send_last(0, 0, CUT4A)
    for part in range(2):
        sweeps = pl.ds(4 * part, 4)
        for side in range(2):
            view = tin.at[side, sweeps, pl.ds(8, 32), own]
            copy = pltpu.make_async_remote_copy(
                src_ref=view, dst_ref=view, send_sem=st.at[side, part],
                recv_sem=qt.at[side, part], device_id=here, device_id_type=MESH,
            )
            pl.when(has_x[side])(copy.wait_recv)
    for side in range(2):
        @pl.when(jnp.logical_not(has_x[side]))
        def _():
            tin[side, :, 8:40, own] = jnp.zeros((8, 32, 128), F32)

        @pl.when(jnp.logical_not(has_y[side]))
        def _():
            tin[:, :, 40 * side : 40 * side + 8, own] = jnp.zeros((2, 8, 8, 128), F32)

    for k, oy in enumerate((-1, 1)):
        rows = pl.ds(8, 8) if oy < 0 else pl.ds(32, 8)
        to_rows = pl.ds(40, 8) if oy < 0 else pl.ds(0, 8)
        copy = prepare(
            tin.at[:, :, rows, own], tin.at[:, :, to_rows, own], sv.at[k], qv.at[k], beside(0, oy)
        )
        pl.when(has_y[k])(copy.start)
        tt.append((copy, has_y[k]))
    substitute(1)
    face = []
    cut_x = []

    def faces(h):
        pair_h = (uh[h], ul[h])
        rows = dot3(split(wall[h]), pair_h, NN)
        face.append(rows[:64])
        cut_x.append(rows[64:])
        line = dot3(split(wys[...]), pair_h, NT)
        for f in range(2):
            for t in range(2):
                my[f, 2 * h + t : 2 * h + t + 1, :] = line[f : f + 1, 128 * t : 128 * t + 128]

    faces(0)
    faces(1)
    rows = jnp.concatenate([face[0] + face[1], cut_x[0], cut_x[1]], axis=0)
    rows = dot3(split(rows), (myh[...], myl[...]), NN)
    lane = lax.broadcasted_iota(jnp.int32, (8, 128), 1) // 16
    for f in range(2):
        for t in range(2):
            cols = slice(128 * t, 128 * t + 128)
            v = [rows[32 * f + 8 * k : 32 * f + 8 * k + 8, cols] for k in range(4)]
            for g in range(2):
                for h in range(2):
                    start = 64 + 16 * h + 8 * g
                    v.append(rows[start : start + 8, cols])
            for q, w in enumerate(exchange8(v, lane)):
                mzx[16 * f + 8 * t + q] = w
    tz = []
    for i, o in enumerate(PEERS):
        target, block = to_real(o)
        tz.append(send(mzx.at[block], rzx.at[mid], sz.at[i], qz.at[mid], target))
    for f in range(2):
        for g in range(2):
            tz.append(send(
                my.at[f], ry.at[mid], sy.at[2 * f + g], qy.at[mid],
                device(g, x, 7 * f, lv + 4 * f),
            ))
    send_last(0, CUT4A, 32)
    inverse_second(1)
    send_last(1, 0, CUT4B)
    for k in range(2):
        view = tin.at[:, :, pl.ds(40 - 40 * k, 8), own]
        copy = pltpu.make_async_remote_copy(
            src_ref=view, dst_ref=view, send_sem=sv.at[k], recv_sem=qv.at[k], device_id=here,
            device_id_type=MESH,
        )
        pl.when(has_y[1 - k])(copy.wait_recv)
    view = tin.at[:, :, :, own]
    te = send(view, view, se.at[0], qe.at[0], partner)
    te.wait_recv()
    def factor(k):
        inside_x = (k + 8 * gx >= 8) & (k + 8 * gx < 136)
        return jnp.where(inside_x, sixth, 0.0)

    ends = (jnp.where(gx == 0, 0.0, sixth), jnp.where(gx == 15, 0.0, sixth))
    for k in (4, 5, 6, 7, 16, 17, 18, 19):
        es[k] = jnp.zeros((48, 256), F32)
        ed[k] = jnp.zeros((48, 256), F32)
    for k in (3, 4, 5, 6, 17, 18, 19, 20):
        et[k] = jnp.zeros((48, 256), F32)
    for k in range(8, 16):
        ed[k] = fr[k - 7]
    for j in range(8):
        source, target = ((es, et), (et, es))[j % 2]
        depth = min(j + 1, 7 - j)

        def some(k, c, source=source, target=target, first=8 - depth, step=WIDE):
            for m in range(step):
                index = first + step * k + m
                target[index] = layer(source, ed, index) * factor(index)
            return c

        layers = 8 + 2 * depth
        lax.fori_loop(0, layers // WIDE, some, 0)
        if layers % WIDE:
            some(0, 0, first=8 - depth + layers // WIDE * WIDE, step=layers % WIDE)
        target[8] = target[8] + tin[0, j] * ends[0]
        target[15] = target[15] + tin[1, j] * ends[1]
    for s in range(32):
        arrived(rzx, qz, s)
    zsum = rzx[0]
    for s in range(1, 32):
        zsum = zsum + rzx[s]
    got = rzx[...].reshape(256, 128)
    parts = [full(got, mz[256 * k : 256 * k + 256, :], TN) for k in range(2)]
    for f in range(2):
        m6[f] = parts[0][64 + 32 * f : 80 + 32 * f] + parts[1][80 + 32 * f : 96 + 32 * f]
    row = lax.broadcasted_iota(jnp.int32, (128, 32), 0)
    col = lax.broadcasted_iota(jnp.int32, (128, 32), 1)
    pick = jnp.where(a0 - 3 + 2 * (row // 8) + row % 8 == 32 * gx + col, 1.0, 0.0)
    spread_z = jnp.concatenate([jnp.where(lane == h, zsum, 0.0) for h in range(4)], axis=0)
    m5[:, 0] = full(pick, spread_z, NN).reshape(16, 8, 128)
    m5[:, 1] = jnp.zeros((16, 8, 128), F32)
    at_y = (gy == 0) | (gy == 15)

    @pl.when(at_y)
    def _():
        for s in range(32):
            arrived(ry, qy, s)
        lane8 = lax.broadcasted_iota(jnp.int32, (32, 128), 1) % 8
        group = lax.broadcasted_iota(jnp.int32, (16, 128), 0)
        member = lax.broadcasted_iota(jnp.int32, (16, 128), 1) // 8
        gather = jnp.where(group == member, 1.0, 0.0)
        part = []
        for t in range(2):
            total = None
            for h in range(2):
                v = ry[:, 2 * h + t, :]
                v = jnp.concatenate([jnp.where(lane8 == k, v, 0.0) for k in range(8)], axis=0)
                modes = jnp.concatenate(
                    [mz[pl.ds(256 * h + k, 32, stride=8), :] for k in range(8)], axis=0
                )
                w = full(v, modes, TN)
                total = w if total is None else total + w
            part.append(full(gather, total, NN))
        m5[:, 1] = full(pick, jnp.concatenate(part, axis=0), NN).reshape(16, 8, 128)

    t5 = []
    for k in range(1, 16):
        q = (gx + k) % 16
        copy = pltpu.make_async_remote_copy(
            src_ref=m5.at[q], dst_ref=r5.at[gx], send_sem=s5.at[k], recv_sem=q5.at[gx],
            device_id=real_row(q), device_id_type=MESH,
        )
        copy.start()
        t5.append(copy)
    r5[gx] = m5[gx]
    for f in range(2):
        end = 15 * f
        copy = pltpu.make_async_remote_copy(
            src_ref=m6.at[f], dst_ref=r6.at[gx], send_sem=s6.at[f], recv_sem=q6.at[gx],
            device_id=real_row(end), device_id_type=MESH,
        )

        @pl.when(gx != end)
        def _():
            copy.start()

        @pl.when(gx == end)
        def _():
            r6[gx] = m6[f]


    send_last(1, CUT4B, 32)
    for s in range(32):
        arrived(gg.at[0], q4.at[0], s)
    def inverse_third(h):
        swap_groups(gg.at[h], za, 0, 256 * h)
        rows_h = tuple(part[halves[h], :] for part in s_pair)
        return dot3(split(za[:, :, halves[h]].reshape(512, 256)), rows_h, NN).reshape(32, 16, 512)

    out_ref[...] = inverse_third(0)
    for s in range(32):
        arrived(gg.at[1], q4.at[1], s)
    out_ref[...] = out_ref[...] + inverse_third(1)
    for k in range(1, 16):
        arrived(r5, q5, (gx + k) % 16)
    def interpolate(fine, cell):
        scaled = 2 * fine + 5
        bottom = scaled // 8
        t = (scaled % 8).astype(F32) * 0.125
        return jnp.where(cell == bottom, 1.0 - t, 0.0) + jnp.where(cell == bottom + 1, t, 0.0)

    def grid(shape):
        return (lax.broadcasted_iota(jnp.int32, shape, 0), lax.broadcasted_iota(jnp.int32, shape, 1))

    row, col = grid((24, 8))
    int_x = interpolate(row, col)
    row, col = grid((128, 128))
    int_y = jnp.where((col < 64) & (row < 48), interpolate(row, col % 16), 0.0)
    zb5 = r5[0, 0]
    yb5 = r5[0, 1]
    for s in range(1, 16):
        zb5 = zb5 + r5[s, 0]
        yb5 = yb5 + r5[s, 1]
    ghost_z = full(full(int_x, zb5, NN), int_y, NT)
    row, col = grid((24, 128))
    inside = (row + 8 * gx >= 8) & (row + 8 * gx < 136) & (col < 48)
    inside = inside & (col + 32 * gy >= 8) & (col + 32 * gy < 520)
    sixth_z = jnp.where(inside, 1.0 / 6.0, 0.0)
    plane = []
    for j in range(8):
        new = []
        for k in range(j + 1):
            total = ghost_z if k == 0 else plane[k - 1]
            if k + 1 < j:
                total = total + plane[k + 1]
            if k < j:
                v = plane[k]
                total = total + (pltpu.roll(v, 1, 0) + pltpu.roll(v, 23, 0))
                total = total + (pltpu.roll(v, 1, 1) + pltpu.roll(v, 127, 1))
            new.append(total * sixth_z)
        plane = new
    for k in range(8):
        gz[pl.ds(k, 24, stride=8), :] = plane[k]
    row, col = grid((8, 128))
    place = jnp.where(col == jnp.where(core == 0, row, 127 - row), 1.0, 0.0)
    for k in range(8):
        part = full(gz[8 * (k + 8) : 8 * (k + 8) + 8, :], place, TN)
        fine_ref[k] = es[k + 8, 8:40, own] + part[8:40]

    row, col = grid((128, 256))
    int_z = jnp.where(row < 64, interpolate(col, row + 30 * core), 0.0)

    row8 = lax.broadcasted_iota(jnp.int32, (8, 256), 0)
    col8 = lax.broadcasted_iota(jnp.int32, (8, 256), 1)
    for f in range(2):
        @pl.when(gy == 15 * f)
        def _():
            ghost_y = full(full(int_x, yb5, NN), int_z, NN)
            edge = 7 * f
            for k in range(24):
                yd[k] = jnp.where(row8 == edge, ghost_y[k : k + 1], 0.0)
            for j in range(8):
                source, target = ((ya, yb), (yb, ya))[j % 2]

                def one(k, c, source=source, target=target, j=j):
                    total = yd[k]
                    if j:
                        v = source[k]
                        total = total + source[k - 1] + source[k + 1]
                        total = total + jnp.where(row8 == 0, 0.0, pltpu.roll(v, 1, 0))
                        total = total + jnp.where(row8 == 7, 0.0, pltpu.roll(v, 7, 0))
                        total = total + jnp.where(col8 == 0, 0.0, pltpu.roll(v, 1, 1))
                        total = total + jnp.where(col8 == 255, 0.0, pltpu.roll(v, 255, 1))
                    inside_x = (k + 8 * gx >= 8) & (k + 8 * gx < 136)
                    target[k] = total * jnp.where(inside_x, 1.0 / 6.0, 0.0)
                    return c

                for k in range(j + 1, 23 - j):
                    one(k, 0)
            rows = pl.ds(24 * f, 8)
            for k in range(8):
                fine_ref[k, rows, :] = fine_ref[k, rows, :] + ya[k + 8, :, own]

    for f in range(2):
        @pl.when(gx == 15 * f)
        def _():
            for k in range(16):
                if k != 15 * f:
                    arrived(r6, q6, k)
            xb6 = r6[0]
            for s in range(1, 16):
                xb6 = xb6 + r6[s]
            row, col = grid((48, 16))
            near_y = interpolate(row, col)
            ghost_x = full(full(near_y, xb6, NN), int_z, NN)
            for k in range(1, 9):
                fr[k] = jnp.zeros((48, 256), F32)
                fa[k] = jnp.zeros((48, 256), F32)
                fb[k] = jnp.zeros((48, 256), F32)
            fr[1 + 7 * f] = ghost_x
            for j in range(8):
                source, target = ((fa, fb), (fb, fa))[j % 2]
                for k in range(j + 1):
                    index = 8 - k if f else 1 + k
                    target[index] = layer(source, fr, index) * sixth
            for k in range(8):
                fine_ref[k] = fine_ref[k] + fa[k + 1, 8:40, own]

    for copy in t2 + t4[0] + t4[1] + tz + t5 + [te]:
        copy.wait_send()
    for copy, sent, *_ in halo + tt:
        pl.when(sent)(copy.wait_send)
    for f in range(2):
        @pl.when(gx != 15 * f)
        def _():
            pltpu.make_async_remote_copy(
                src_ref=m6.at[f], dst_ref=r6.at[gx], send_sem=s6.at[f], recv_sem=q6.at[gx],
                device_id=real_row(15 * f), device_id_type=MESH,
            ).wait_send()


def body(density, fine_density, fine_start, anchor):
    high, low, lam = tables()
    vm = pl.BlockSpec(memory_space=pltpu.VMEM)
    dma = pltpu.SemaphoreType.DMA

    def f32(*shape):
        return pltpu.VMEM(shape, F32)

    def b16(*shape):
        return pltpu.VMEM(shape, BF16)

    big = f32(32, 16, 512)
    return pl.pallas_call(
        kernel,
        out_shape=(
            jax.ShapeDtypeStruct((32, 16, 512), F32), jax.ShapeDtypeStruct((8, 32, 128), F32)
        ),
        in_specs=[pl.BlockSpec(memory_space=pl.ANY)] * 9,
        out_specs=(vm, vm),
        scratch_shapes=[
            pltpu.SMEM((3,), jnp.int32), f32(8, 512), f32(2, 8, 128), f32(8, 128),
            big, f32(8, 32, 128), f32(8, 32, 128), b16(512, 512), b16(512, 512),
            big, f32(2, 32, 16, 256), f32(2, 32, 16, 256), f32(2, 32, 16, 256),
            f32(2, 32, 8, 512), f32(2, 31, 8, 512),
            f32(128, 128), f32(16, 8, 128), f32(16, 8, 128), f32(128, 128),
            f32(2, 16, 2, 128), f32(2, 2, 128),
            b16(2, 256, 512), b16(2, 256, 512), b16(512, 256), b16(512, 256),
            f32(512, 128), f32(2, 80, 256), f32(16, 512),
            f32(32, 8, 128), f32(32, 8, 128), f32(2, 4, 128), f32(32, 4, 128),
            f32(16, 2, 8, 128), f32(16, 2, 8, 128), f32(2, 16, 128), f32(16, 16, 128),
            f32(24, 48, 256), f32(24, 48, 256), f32(24, 48, 256),
            f32(10, 48, 256), f32(10, 48, 256), f32(10, 48, 256),
            f32(2, 8, 48, 256), f32(2, 8, 48, 256), f32(192, 128),
            f32(24, 8, 256), f32(24, 8, 256), f32(24, 8, 256),
            dma((2, 32)), dma((2, 32)), dma((16,)), dma((16,)), dma((16,)), dma((16,)),
            dma((2, 32)), dma((2, 32)), dma((4,)), dma((4,)), dma((2,)), dma((2,)),
            dma((32,)), dma((32,)), dma((4,)), dma((32,)), dma((16,)), dma((16,)),
            dma((2,)), dma((16,)), dma((10,)), dma((2, 2)), dma((2, 2)), dma((1,)), dma((1,)), dma((2,)), dma((2,)),
        ],
        compiler_params=pltpu.CompilerParams(
            collective_id=0, has_side_effects=True, vmem_limit_bytes=56 << 20
        ),
    )(anchor, jnp.asarray(np.tile(lam.reshape(1, 512), (8, 1))),
      jnp.asarray(np.tile(lam.reshape(512, 1), (1, 128))),
      jnp.asarray(np.tile(lam.reshape(4, 128), (2, 1))), density, fine_density, fine_start,
      jnp.asarray(high), jnp.asarray(low))


def solution(mesh):
    return jax.shard_map(
        body,
        mesh=mesh,
        in_specs=(P("gx", ("grp", "gy"), None), P("gx", "gy", "grp"), P("gx", "gy", "grp"), P()),
        out_specs=(P("gx", ("grp", "gy"), None), P("gx", "gy", "grp")),
        check_vma=False,
    )
```

```python
import functools
import math

import jax
import jax.numpy as jnp
import numpy as np
from jax import lax
from jax.experimental import pallas as pl
from jax.experimental.pallas import tpu as pltpu
from jax.sharding import PartitionSpec as P

MESH = pl.DeviceIdType.MESH
NC = 512
F32 = jnp.float32
CUT1, CUT4A, CUT4B = 32, 16, 32
WIDE = 4
BF16 = jnp.bfloat16


def tables():
    index = np.arange(1, NC + 1, dtype=np.int64)
    angle = (index[:, None] * index[None, :]) % (2 * (NC + 1))
    sine = math.sqrt(2.0 / (NC + 1)) * np.sin(angle * (math.pi / (NC + 1)))
    sine = sine.astype(np.float32)
    high = sine.astype(jnp.bfloat16)
    low = (sine - high.astype(np.float32)).astype(jnp.bfloat16)
    lam = 4.0 * np.sin(index * (math.pi / (2 * (NC + 1)))) ** 2
    return high, low, lam.astype(np.float32)


def split(value):
    high = value.astype(BF16)
    low = (value - high.astype(F32)).astype(BF16)
    return high, low


def dot3(a, b, dims):
    ah, al = a
    bh, bl = b
    dd = functools.partial(
        lax.dot_general, dimension_numbers=(dims, ((), ())), preferred_element_type=F32
    )
    return dd(ah, bh) + (dd(al, bh) + dd(ah, bl))


def mm(a, b, dims):
    return lax.dot_general(a, b, (dims, ((), ())), preferred_element_type=F32)


def full(a, b, dims):
    return lax.dot_general(
        a, b, (dims, ((), ())), precision=lax.Precision.HIGHEST, preferred_element_type=F32
    )


NN = ((1,), (0,))
NT = ((1,), (1,))
TN = ((0,), (0,))


def exchange(v, lane):
    v = list(v)
    for bit in (1, 2, 4, 8):
        upper = (lane & bit) != 0
        for i in range(16):
            if i & bit:
                continue
            a, c = v[i], v[i | bit]
            v[i] = jnp.where(upper, pltpu.roll(c, 8 * bit, 1), a)
            v[i | bit] = jnp.where(upper, c, pltpu.roll(a, 128 - 8 * bit, 1))
    return v


def exchange8(v, lane):
    v = list(v)
    for bit in (1, 2, 4):
        upper = (lane & bit) != 0
        for i in range(8):
            if i & bit:
                continue
            a, c = v[i], v[i | bit]
            v[i] = jnp.where(upper, pltpu.roll(c, 16 * bit, 1), a)
            v[i | bit] = jnp.where(upper, c, pltpu.roll(a, 128 - 16 * bit, 1))
    return v


def swap_groups(source, target, first, out_first):
    lane = lax.broadcasted_iota(jnp.int32, (8, 128), 1) // 8
    for a in range(2):
        for b in range(2):
            cols = slice(first + 128 * b, first + 128 * b + 128)
            outs = slice(out_first + 128 * a, out_first + 128 * a + 128)
            for row in (0, 8):
                v = [source[16 * a + q, row : row + 8, cols] for q in range(16)]
                for q, w in enumerate(exchange(v, lane)):
                    target[16 * b + q, row : row + 8, outs] = w


def device(core, x, y, z):
    return (core, x * 4 + z % 4, (z // 4) * 8 + y)


ORDER = [
    (dy, side, core) for dy in (4, 3, 5, 2, 6, 1, 7, 0) for side in (0, 1) for core in (0, 1)
]
PEERS = [ORDER[i] for i in np.random.RandomState(3).permutation(32)]


def kernel(
    anchor_hbm, lamr_hbm, lamc_hbm, lamq_hbm, x_hbm, fd_hbm, fs_hbm, sh_hbm, sl_hbm, out_ref, fine_ref,
    anchor, lamr_ref, lamc_ref, lamq_ref, x_ref, fd_ref, fs_ref, sh_ref, sl_ref,
    za, zb, dd, gg, u, dtab, m1, r1, m2, r2, dint, rint, uh, ul, myh, myl, mz, wall, wys,
    mzx, rzx, my, ry, m5, r5, m6, r6, m7, r7, es, et, ed, fa, fb, fr, trace, tin, gz, ya, yb, yd,
    s1, q1, s2, q2, s3, q3, s4, q4, sh1, qh1, sd, qd, sz, qz, sy, qy, s5, q5, s6, q6, sin,
    st, qt, se, qe, sv, qv, sx, qx, s7, q7,
):
    core = lax.axis_index("grp")
    gx = lax.axis_index("gx")
    gy = lax.axis_index("gy")
    x, zl = gx // 4, gx % 4
    y, zh = gy % 8, gy // 8
    z = zh * 4 + zl
    me = core * 16 + gy
    zv = (z + 6) % 8
    lv, hv = zv % 4, zv // 4
    mid = core * 16 + hv * 8 + y
    pv = x * 4 + lv

    def to_mid(o):
        dy, side, oc = o
        ty = (y + dy + core * (8 - 2 * dy)) % 8
        tc = (core + oc) % 2
        return device(tc, x, ty, (zl + 4 * side + 2) % 8), tc * 16 + side * 8 + ty

    def to_real(o):
        dy, side, oc = o
        ty = (y + dy + core * (8 - 2 * dy)) % 8
        tc = (core + oc) % 2
        return device(tc, x, ty, lv + 4 * side), tc * 16 + side * 8 + ty

    def to_row(q):
        return device(core, q // 4, y, (q % 4 + 4 * hv + 2) % 8)

    def real_row(q):
        return device(core, q // 4, y, q % 4 + 4 * zh)

    here = (core, gx, gy)
    partner = (1 - core, gx, gy)
    own = pl.ds(pl.multiple_of(core * 128, 128), 128)

    def beside(ox, oy):
        return (core, (gx + ox + 16) % 16, (gy + oy + 16) % 16)

    fetch = []
    mine = [pl.ds(pl.multiple_of(256 * h + 8 * mid, 8), 8) for h in range(2)]
    for k, (src, dst) in enumerate((
        (x_hbm, x_ref), (sh_hbm, sh_ref), (sl_hbm, sl_ref), (fd_hbm, fd_ref), (fs_hbm, fs_ref),
        (lamr_hbm, lamr_ref), (lamq_hbm, lamq_ref), (lamc_hbm.at[mine[0], :], lamc_ref.at[0]),
        (lamc_hbm.at[mine[1], :], lamc_ref.at[1]), (anchor_hbm, anchor),
    )):
        copy = pltpu.make_async_copy(src, dst, sin.at[k])
        copy.start()
        fetch.append(copy)
    barrier = pltpu.get_barrier_semaphore()
    for o in PEERS:
        pl.semaphore_signal(barrier, inc=1, device_id=to_mid(o)[0], device_id_type=MESH)
    pl.semaphore_signal(barrier, inc=1, device_id=partner, device_id_type=MESH)
    for oy in (-1, 1):
        pl.semaphore_signal(barrier, inc=1, device_id=beside(0, oy), device_id_type=MESH)
    for k in range(1, 16):
        pl.semaphore_signal(barrier, inc=1, device_id=to_row((pv + k) % 16), device_id_type=MESH)
        pl.semaphore_signal(barrier, inc=1, device_id=real_row((gx + k) % 16), device_id_type=MESH)

    def arrived(ref, sem, index):
        pltpu.make_async_remote_copy(
            src_ref=ref.at[index], dst_ref=ref.at[index], send_sem=sem.at[index],
            recv_sem=sem.at[index], device_id=here, device_id_type=MESH,
        ).wait_recv()

    has_y = (gy > 0, gy < 15)
    has_x = (gx > 0, gx < 15)
    middle = (gy == 7) | (gy == 8)
    turns = ((gy > 0) & (gy != 8), (gy < 15) & (gy != 7))
    corner = pl.ds(pl.multiple_of((8 - gy) % 8 * 40, 8), 8)

    def prepare(src, dst, send_sem, recv_sem, target):
        return pltpu.make_async_remote_copy(
            src_ref=src, dst_ref=dst, send_sem=send_sem, recv_sem=recv_sem,
            device_id=target, device_id_type=MESH,
        )

    def send(*args):
        copy = prepare(*args)
        copy.start()
        return copy

    for copy in fetch[:3]:
        copy.wait()
    s_pair = (sh_ref[...], sl_ref[...])
    x_pair = split(x_ref[...].reshape(512, 512))
    halves = [slice(0, 256), slice(256, 512)]

    def forward_third(h):
        cols = tuple(part[:, halves[h]] for part in s_pair)
        za[:, :, halves[h]] = dot3(x_pair, cols, NN).reshape(32, 16, 256)
        swap_groups(za, zb.at[h], 256 * h, 0)

    t1 = [[], []]

    def send_first(h, lo, hi):
        for i in range(lo, hi):
            target, block = to_mid(PEERS[i])
            t1[h].append(
                send(zb.at[h, block], dd.at[h, me], s1.at[h, i], q1.at[h, me], target)
            )

    forward_third(0)
    for copy in fetch[3:]:
        copy.wait()
    a0, a1, a2 = anchor[0], anchor[1], anchor[2]
    fa[1:9, 8:40, own] = fs_ref[...]
    fr[1:9, 8:40, own] = fd_ref[...]
    pl.semaphore_wait(barrier, 65)
    halo = []
    for k, oy in enumerate((-1, 1)):
        rows = pl.ds(0, 8) if oy < 0 else pl.ds(24, 8)
        to_rows = pl.ds(40, 8) if oy < 0 else pl.ds(0, 8)
        for part, (src, dst) in enumerate(((fs_ref, fa), (fd_ref, fr))):
            copy = prepare(
                src.at[:, rows, :], dst.at[pl.ds(1, 8), to_rows, own],
                sh1.at[2 * k + part], qh1.at[2 * k + part], beside(0, oy),
            )
            pl.when(has_y[k])(copy.start)
            halo.append((copy, has_y[k], has_y[1 - k]))
    send_first(0, 0, 32)
    forward_third(1)
    send_first(1, 0, CUT1)
    for h in range(2):
        mu = lamr_ref[0:1, :] + jnp.concatenate([lamc_ref[h]] * 4, axis=1)

        def table(i, g, h=h, mu=mu):
            d = 1.0 / (1.0 + (mu + g))
            dtab[h, i] = d
            return (mu + g) * d

        lax.fori_loop(0, 31, table, jnp.ones((8, 512), F32))
        odd = pv % 2 == 1
        muq = jnp.where(odd, lamq_ref[2:4, :], lamq_ref[0:2, :]) + lamc_ref[h, pl.ds(pv // 2, 1), :]
        c = 0.5 * muq
        c1 = c
        r32 = 2.0 * (1.0 + c)
        for _ in range(4):
            c = 2.0 * c * (c + 2.0)
            r32 = r32 * (2.0 * (1.0 + c))
        c = 2.0 * c * (c + 2.0)
        rint[h] = r32
        g = jnp.ones((2, 128), F32)
        for i in range(15):
            d = 1.0 / (1.0 + (2.0 * c + g))
            dint[h, i] = d
            g = (2.0 * c + g) * d
        dint[h, 15] = 1.0 / (r32 * (1.0 + c1) + c + g)
    def cells(rows, cols, first):
        grid = lax.broadcasted_iota(jnp.int32, (rows, cols), 0)
        return jnp.where(grid == first, 1.0, 0.0).astype(BF16)

    lane = lax.broadcasted_iota(jnp.int32, (512, 256), 1)
    pick = cells(512, 256, a1 - 3 + 8 * (lane // 16) + lane % 16)
    myh[...] = mm(sh_ref[...], pick, NN).astype(BF16)
    myl[...] = mm(sl_ref[...], pick, NN).astype(BF16)
    lane = lax.broadcasted_iota(jnp.int32, (512, 128), 1)
    pick = cells(512, 128, a2 - 1 + 30 * core + lane)
    mz[...] = mm(sh_ref[...], pick, NN) + mm(sl_ref[...], pick, NN)
    def weights(cell, first, boxes, low_face, high_face):
        low_w = jnp.where(cell == first, 0.625, 0.0) + jnp.where(cell == first + 1, 0.375, 0.0)
        high_w = jnp.where(cell == first + boxes, 0.375, 0.0) + jnp.where(
            cell == first + boxes + 1, 0.625, 0.0
        )
        return jnp.where(low_face, low_w, 0.0) + jnp.where(high_face, high_w, 0.0)

    row = lax.broadcasted_iota(jnp.int32, (16, 512), 0)
    cell = lax.broadcasted_iota(jnp.int32, (16, 512), 1)
    wy = weights(cell, a1 - 1, 128, row == 0, row == 1).astype(BF16)
    wys[...] = mm(wy, sh_ref[...], NN) + mm(wy, sl_ref[...], NN)
    wz = weights(cell, a2 - 1, 64, row == 0, row == 1).astype(BF16)
    wz = mm(wz, sh_ref[...], NN) + mm(wz, sl_ref[...], NN)
    lane = lax.broadcasted_iota(jnp.int32, (512, 512), 1)
    pick = cells(512, 512, 256 * (lane // 256) + 8 * mid + lane % 8)
    wzh, wzl = split(wz)
    wz = mm(wzh, pick, NN) + mm(wzl, pick, NN)
    row = lax.broadcasted_iota(jnp.int32, (32, 256), 0)
    lane = lax.broadcasted_iota(jnp.int32, (32, 256), 1)
    row2 = lax.broadcasted_iota(jnp.int32, (16, 256), 0)
    lane2 = lax.broadcasted_iota(jnp.int32, (16, 256), 1)
    wx = weights(32 * pv + lane2 // 8, a0 - 1, 32, row2 < 8, row2 >= 8)
    wx = jnp.where(row2 % 8 == lane2 % 8, wx, 0.0)
    for h in range(2):
        for f in range(2):
            wall[h, 32 * f : 32 * f + 32, :] = jnp.where(
                row == lane // 8, wz[f : f + 1, halves[h]], 0.0
            )
        wall[h, 64:80, :] = wx
    for copy, _, comes in halo:
        pl.when(comes)(copy.wait_recv)
    pair = []
    for k, ref in enumerate((fa, fr)):
        view = ref.at[pl.ds(1, 8), :, own]
        copy = pltpu.make_async_remote_copy(
            src_ref=view, dst_ref=view, send_sem=sd.at[k], recv_sem=qd.at[k],
            device_id=partner, device_id_type=MESH,
        )
        copy.start()
        pair.append(copy)
    for copy in pair:
        copy.wait()
    fine_row = lax.broadcasted_iota(jnp.int32, (48, 256), 0) + 32 * gy
    fine_col = lax.broadcasted_iota(jnp.int32, (48, 256), 1)
    inside_y = (fine_row >= 8) & (fine_row < 520)
    sixth = jnp.where(inside_y, 1.0 / 6.0, 0.0)

    def layer(source, extra, k):
        v = source[k]
        total = (source[k - 1] + source[k + 1]) + extra[k]
        total = total + (pltpu.roll(v, 1, 0) + pltpu.roll(v, 47, 0))
        total = total + jnp.where(fine_col == 0, 0.0, pltpu.roll(v, 1, 1))
        return total + jnp.where(fine_col == 255, 0.0, pltpu.roll(v, 255, 1))

    for k in (0, 9):
        fa[k] = jnp.zeros((48, 256), F32)
        fb[k] = jnp.zeros((48, 256), F32)
    for k in range(1, 9):
        fa[k] = jnp.where(inside_y, fa[k], 0.0)
        fr[k] = jnp.where(inside_y, fr[k], 0.0) * (-1.0 / 16.0)
        es[k + 7] = fa[k]

    def alone(j, carry):
        for part, (source, target) in enumerate(((fa, fb), (fb, fa))):
            trace[0, 2 * j + part] = source[1]
            trace[1, 2 * j + part] = source[8]

            def four(k, c):
                for m in range(4):
                    index = 1 + 4 * k + m
                    target[index] = layer(source, fr, index) * sixth
                return c

            lax.fori_loop(0, 2, four, 0)
        return carry

    lax.fori_loop(0, 4, alone, 0)

    t2 = []
    t4 = [[], []]

    def second_and_eliminate(h):
        value = dd[h].reshape(512, 256)
        u[h] = dot3(split(value), s_pair, TN).reshape(32, 8, 512)
        first = -u[h, 0]
        u[h, 0] = first
        q0 = dtab[h, 30]

        def forward(i, carry):
            yv, q, e = carry
            w = u[h, i]
            yv = dtab[h, i - 1] * yv - w
            u[h, i] = yv
            q = q * dtab[h, 30 - i]
            return yv, q, e - q * w

        yv, _, e = lax.fori_loop(1, 31, forward, (first, q0, q0 * first))
        b = q0 * yv - u[h, 31]
        for j in range(4):
            start = 8 * (j // 2) + j % 2 + 4 * h
            m1[pl.ds(start, 8, stride=16), :] = e[:, 128 * j : 128 * j + 128]
            m1[pl.ds(start + 2, 8, stride=16), :] = b[:, 128 * j : 128 * j + 128]

    def send_ends():
        for k in range(1, 16):
            q = (pv + k) % 16
            t2.append(send(
                m1.at[pl.ds(pl.multiple_of(q * 8, 8), 8), :], r1.at[pv], s2.at[k], q2.at[pv],
                to_row(q),
            ))
        r1[pv] = m1[pl.ds(pl.multiple_of(pv * 8, 8), 8), :]

    def separators():
        for h in range(2):
            ys = []
            prev = None
            for p in range(16):
                end = r1[p, 4 * h + 2 : 4 * h + 4, :]
                if p < 15:
                    end = end + r1[p + 1, 4 * h : 4 * h + 2, :]
                end = rint[h] * end
                prev = end if p == 0 else end + dint[h, p - 1] * prev
                ys.append(prev)
            m2[0, 4 * h : 4 * h + 2, :] = jnp.zeros((2, 128), F32)
            sol = dint[h, 15] * ys[15]
            m2[15, 4 * h + 2 : 4 * h + 4, :] = sol
            for p in range(14, -1, -1):
                sol = dint[h, p] * (sol + ys[p])
                m2[p + 1, 4 * h : 4 * h + 2, :] = sol
                m2[p, 4 * h + 2 : 4 * h + 4, :] = sol
        for k in range(1, 16):
            q = (pv + k) % 16
            t2.append(send(
                m2.at[q], r2.at[pl.ds(pl.multiple_of(pv * 8, 8), 8), :], s3.at[k], q3.at[pv],
                to_row(q),
            ))
        r2[pl.ds(pl.multiple_of(pv * 8, 8), 8), :] = m2[pv]

    def wait_separators():
        for k in range(1, 16):
            q = (pv + k) % 16
            view = r2.at[pl.ds(pl.multiple_of(q * 8, 8), 8), :]
            pltpu.make_async_remote_copy(
                src_ref=view, dst_ref=view, send_sem=s3.at[k], recv_sem=q3.at[q],
                device_id=here, device_id_type=MESH,
            ).wait_recv()

    def substitute(h):
        starts = [8 * (j // 2) + j % 2 + 4 * h for j in range(4)]
        left = jnp.concatenate([r2[pl.ds(j, 8, stride=16), :] for j in starts], axis=1)
        right = jnp.concatenate([r2[pl.ds(j + 2, 8, stride=16), :] for j in starts], axis=1)

        def spread(i, t):
            u[h, i] = u[h, i] + t
            return dtab[h, i] * t

        lax.fori_loop(0, 31, spread, left)
        u[h, 31] = right

        def backward(k, v):
            i = 30 - k
            v = dtab[h, i] * (v + u[h, i])
            u[h, i] = v
            return v

        lax.fori_loop(0, 31, backward, right)
        high, low = split(u[h].reshape(256, 512))
        uh[h] = high
        ul[h] = low

    def inverse_second(h):
        for copy in t1[h]:
            copy.wait_send()
        zb[h] = dot3(s_pair, (uh[h], ul[h]), NT).reshape(32, 16, 256)

    def send_last(h, lo, hi):
        for i in range(lo, hi):
            target, block = to_real(PEERS[i])
            t4[h].append(
                send(zb.at[h, block], gg.at[h, mid], s4.at[h, i], q4.at[h, mid], target)
            )

    tt = []

    def send_traces(part):
        sweeps = pl.ds(4 * part, 4)
        for side, ox in enumerate((-1, 1)):
            copy = prepare(
                trace.at[side, sweeps, pl.ds(8, 32), own],
                tin.at[1 - side, sweeps, pl.ds(8, 32), own],
                st.at[side, part], qt.at[1 - side, part], beside(ox, 0),
            )
            pl.when(has_x[side])(copy.start)
            tt.append((copy, has_x[side]))

    def send_corners():
        for side, ox in enumerate((-1, 1)):
            copy = prepare(
                trace.at[side, :, corner, own], tin.at[1 - side, :, corner, own], sx.at[side],
                qx.at[1 - side], beside(ox, 0),
            )
            sent = has_x[side] & middle
            pl.when(sent)(copy.start)
            tt.append((copy, sent))

    for s in range(32):
        arrived(dd.at[0], q1.at[0], s)
    second_and_eliminate(0)
    for s in range(32):
        arrived(dd.at[1], q1.at[1], s)
    second_and_eliminate(1)
    send_ends()
    send_traces(0)
    send_traces(1)
    send_corners()
    for k in range(1, 16):
        arrived(r1, q2, (pv + k) % 16)
    separators()
    wait_separators()
    substitute(0)
    inverse_second(0)
    send_last(0, 0, CUT4A)
    for part in range(2):
        sweeps = pl.ds(4 * part, 4)
        for side in range(2):
            view = tin.at[side, sweeps, pl.ds(8, 32), own]
            copy = pltpu.make_async_remote_copy(
                src_ref=view, dst_ref=view, send_sem=st.at[side, part],
                recv_sem=qt.at[side, part], device_id=here, device_id_type=MESH,
            )
            pl.when(has_x[side])(copy.wait_recv)
    for side in range(2):
        copy = prepare(
            tin.at[side, :, corner, own], tin.at[side, :, corner, own], sx.at[side], qx.at[side],
            here,
        )
        pl.when(has_x[side] & middle)(copy.wait_recv)

        @pl.when(jnp.logical_not(has_x[side]))
        def _():
            tin[side, :, 8:40, own] = jnp.zeros((8, 32, 128), F32)

        @pl.when(jnp.logical_not(has_x[side]) & middle)
        def _():
            tin[side, :, corner, own] = jnp.zeros((8, 8, 128), F32)

        @pl.when(jnp.logical_not(has_y[side]))
        def _():
            tin[:, :, 40 * side : 40 * side + 8, own] = jnp.zeros((2, 8, 8, 128), F32)

    for k, oy in enumerate((-1, 1)):
        rows = pl.ds(8, 8) if oy < 0 else pl.ds(32, 8)
        to_rows = pl.ds(40, 8) if oy < 0 else pl.ds(0, 8)
        copy = prepare(
            tin.at[:, :, rows, own], tin.at[:, :, to_rows, own], sv.at[k], qv.at[k], beside(0, oy)
        )
        pl.when(turns[k])(copy.start)
        tt.append((copy, turns[k]))
    substitute(1)
    face = []
    cut_x = []

    def faces(h):
        pair_h = (uh[h], ul[h])
        rows = dot3(split(wall[h]), pair_h, NN)
        face.append(rows[:64])
        cut_x.append(rows[64:])
        line = dot3(split(wys[...]), pair_h, NT)
        for f in range(2):
            for t in range(2):
                my[f, 2 * h + t : 2 * h + t + 1, :] = line[f : f + 1, 128 * t : 128 * t + 128]

    faces(0)
    faces(1)
    rows = jnp.concatenate([face[0] + face[1], cut_x[0], cut_x[1]], axis=0)
    rows = dot3(split(rows), (myh[...], myl[...]), NN)
    lane = lax.broadcasted_iota(jnp.int32, (8, 128), 1) // 16
    for f in range(2):
        for t in range(2):
            cols = slice(128 * t, 128 * t + 128)
            v = [rows[32 * f + 8 * k : 32 * f + 8 * k + 8, cols] for k in range(4)]
            for g in range(2):
                for h in range(2):
                    start = 64 + 16 * h + 8 * g
                    v.append(rows[start : start + 8, cols])
            for q, w in enumerate(exchange8(v, lane)):
                mzx[16 * f + 8 * t + q] = w
    tz = []
    for i, o in enumerate(PEERS):
        target, block = to_real(o)
        tz.append(send(mzx.at[block], rzx.at[mid], sz.at[i], qz.at[mid], target))
    for f in range(2):
        for g in range(2):
            tz.append(send(
                my.at[f], ry.at[mid], sy.at[2 * f + g], qy.at[mid],
                device(g, x, 7 * f, lv + 4 * f),
            ))
    send_last(0, CUT4A, 32)
    inverse_second(1)
    send_last(1, 0, CUT4B)
    for k in range(2):
        view = tin.at[:, :, pl.ds(40 - 40 * k, 8), own]
        copy = pltpu.make_async_remote_copy(
            src_ref=view, dst_ref=view, send_sem=sv.at[k], recv_sem=qv.at[k], device_id=here,
            device_id_type=MESH,
        )
        pl.when(turns[1 - k])(copy.wait_recv)
    view = tin.at[:, :, :, own]
    te = send(view, view, se.at[0], qe.at[0], partner)
    te.wait_recv()
    def factor(k):
        inside_x = (k + 8 * gx >= 8) & (k + 8 * gx < 136)
        return jnp.where(inside_x, sixth, 0.0)

    ends = (jnp.where(gx == 0, 0.0, sixth), jnp.where(gx == 15, 0.0, sixth))
    for k in (4, 5, 6, 7, 16, 17, 18, 19):
        es[k] = jnp.zeros((48, 256), F32)
        ed[k] = jnp.zeros((48, 256), F32)
    for k in (3, 4, 5, 6, 17, 18, 19, 20):
        et[k] = jnp.zeros((48, 256), F32)
    for k in range(8, 16):
        ed[k] = fr[k - 7]
    for j in range(8):
        source, target = ((es, et), (et, es))[j % 2]
        depth = min(j + 1, 7 - j)

        def some(k, c, source=source, target=target, first=8 - depth, step=WIDE):
            for m in range(step):
                index = first + step * k + m
                target[index] = layer(source, ed, index) * factor(index)
            return c

        layers = 8 + 2 * depth
        lax.fori_loop(0, layers // WIDE, some, 0)
        if layers % WIDE:
            some(0, 0, first=8 - depth + layers // WIDE * WIDE, step=layers % WIDE)
        target[8] = target[8] + tin[0, j] * ends[0]
        target[15] = target[15] + tin[1, j] * ends[1]
    for s in range(32):
        arrived(rzx, qz, s)
    zsum = rzx[0]
    for s in range(1, 32):
        zsum = zsum + rzx[s]
    row = lax.broadcasted_iota(jnp.int32, (128, 512), 0)
    col = lax.broadcasted_iota(jnp.int32, (128, 512), 1)
    tile = jnp.where(row == col // 128 * 16 + col % 16, 1.0, 0.0)
    spread_z = full(zsum, tile, NN)
    spread_z = jnp.concatenate([spread_z[:, 128 * h : 128 * h + 128] for h in range(4)], axis=0)
    lane32 = lax.broadcasted_iota(jnp.int32, (32, 128), 1) // 16
    spread_z = jnp.concatenate(
        [jnp.where(lane32 == k, spread_z, 0.0) for k in range(8)], axis=0
    )
    row = lax.broadcasted_iota(jnp.int32, (16, 256), 0)
    col = lax.broadcasted_iota(jnp.int32, (16, 256), 1)
    pick = jnp.where(a0 - 3 + 2 * row + col // 32 == 32 * gx + col % 32, 1.0, 0.0)
    rows = full(pick, spread_z, NN)
    for q in range(16):
        m5[q] = rows[q : q + 1]
    t5 = []
    for k in range(1, 16):
        q = (gx + k) % 16
        t5.append(send(m5.at[q], r5.at[gx], s5.at[k], q5.at[gx], real_row(q)))
    r5[gx] = m5[gx]
    got = rzx[...].reshape(256, 128)
    parts = [full(got, mz[256 * k : 256 * k + 256, :], TN) for k in range(2)]
    left_half = lax.broadcasted_iota(jnp.int32, (8, 128), 1) < 64
    for f in range(2):
        cells_x = parts[0][64 + 32 * f : 80 + 32 * f] + parts[1][80 + 32 * f : 96 + 32 * f]
        m6[f] = jnp.where(left_half, cells_x[:8], pltpu.roll(cells_x[8:], 64, 1))
    for f in range(2):
        end = 15 * f
        copy = prepare(m6.at[f], r6.at[gx], s6.at[f], q6.at[gx], real_row(end))
        pl.when(gx != end)(copy.start)

        @pl.when(gx == end)
        def _():
            r6[gx] = m6[f]

    at_y = (gy == 0) | (gy == 15)

    @pl.when(at_y)
    def _():
        for s in range(32):
            arrived(ry, qy, s)
        lane8 = lax.broadcasted_iota(jnp.int32, (32, 128), 1) % 8
        group = lax.broadcasted_iota(jnp.int32, (16, 128), 0)
        member = lax.broadcasted_iota(jnp.int32, (16, 128), 1) // 8
        gather = jnp.where(group == member, 1.0, 0.0)
        part = []
        for t in range(2):
            total = None
            for h in range(2):
                v = ry[:, 2 * h + t, :]
                v = jnp.concatenate([jnp.where(lane8 == k, v, 0.0) for k in range(8)], axis=0)
                modes = jnp.concatenate(
                    [mz[pl.ds(256 * h + k, 32, stride=8), :] for k in range(8)], axis=0
                )
                w = full(v, modes, TN)
                total = w if total is None else total + w
            part.append(full(gather, total, NN))
        row = lax.broadcasted_iota(jnp.int32, (128, 32), 0)
        col = lax.broadcasted_iota(jnp.int32, (128, 32), 1)
        pick = jnp.where(a0 - 3 + 2 * (row // 8) + row % 8 == 32 * gx + col, 1.0, 0.0)
        m7[...] = full(pick, jnp.concatenate(part, axis=0), NN).reshape(16, 8, 128)
        for k in range(1, 16):
            q = (gx + k) % 16
            send(m7.at[q], r7.at[gx], s7.at[k], q7.at[gx], real_row(q))
        r7[gx] = m7[gx]

    send_last(1, CUT4B, 32)
    for s in range(32):
        arrived(gg.at[0], q4.at[0], s)
    def inverse_third(h):
        swap_groups(gg.at[h], za, 0, 256 * h)
        rows_h = tuple(part[halves[h], :] for part in s_pair)
        return dot3(split(za[:, :, halves[h]].reshape(512, 256)), rows_h, NN).reshape(32, 16, 512)

    out_ref[...] = inverse_third(0)
    for k in range(1, 16):
        arrived(r5, q5, (gx + k) % 16)
    def interpolate(fine, cell):
        scaled = 2 * fine + 5
        bottom = scaled // 8
        t = (scaled % 8).astype(F32) * 0.125
        return jnp.where(cell == bottom, 1.0 - t, 0.0) + jnp.where(cell == bottom + 1, t, 0.0)

    def grid(shape):
        return (lax.broadcasted_iota(jnp.int32, shape, 0), lax.broadcasted_iota(jnp.int32, shape, 1))

    row, col = grid((24, 8))
    int_x = interpolate(row, col)
    row, col = grid((128, 128))
    int_y = jnp.where(row < 48, interpolate(row, col % 16), 0.0)
    zb5 = r5[0]
    for s in range(1, 16):
        zb5 = zb5 + r5[s]
    row, col = grid((8, 128))
    zb5 = jnp.where(row == col // 16, jnp.broadcast_to(zb5, (8, 128)), 0.0)
    ghost_z = full(full(int_x, zb5, NN), int_y, NT)
    row, col = grid((24, 128))
    inside = (row + 8 * gx >= 8) & (row + 8 * gx < 136) & (col < 48)
    inside = inside & (col + 32 * gy >= 8) & (col + 32 * gy < 520)
    sixth_z = jnp.where(inside, 1.0 / 6.0, 0.0)
    plane = []
    for j in range(8):
        new = []
        for k in range(j + 1):
            total = ghost_z if k == 0 else plane[k - 1]
            if k + 1 < j:
                total = total + plane[k + 1]
            if k < j:
                v = plane[k]
                total = total + (pltpu.roll(v, 1, 0) + pltpu.roll(v, 23, 0))
                total = total + (pltpu.roll(v, 1, 1) + pltpu.roll(v, 127, 1))
            new.append(total * sixth_z)
        plane = new
    for k in range(8):
        gz[pl.ds(k, 24, stride=8), :] = plane[k]
    row, col = grid((8, 128))
    place = jnp.where(col == jnp.where(core == 0, row, 127 - row), 1.0, 0.0)
    for k in range(8):
        part = full(gz[8 * (k + 8) : 8 * (k + 8) + 8, :], place, TN)
        fine_ref[k] = es[k + 8, 8:40, own] + part[8:40]

    row, col = grid((128, 256))
    int_z = jnp.where(row < 64, interpolate(col, row + 30 * core), 0.0)

    for s in range(32):
        arrived(gg.at[1], q4.at[1], s)
    out_ref[...] = out_ref[...] + inverse_third(1)
    row8 = lax.broadcasted_iota(jnp.int32, (8, 256), 0)
    col8 = lax.broadcasted_iota(jnp.int32, (8, 256), 1)
    for f in range(2):
        @pl.when(gy == 15 * f)
        def _():
            for k in range(1, 16):
                arrived(r7, q7, (gx + k) % 16)
            yb7 = r7[0]
            for k in range(1, 16):
                yb7 = yb7 + r7[k]
            ghost_y = full(full(int_x, yb7, NN), int_z, NN)
            edge = 7 * f
            for k in range(24):
                yd[k] = jnp.where(row8 == edge, ghost_y[k : k + 1], 0.0)
            for j in range(8):
                source, target = ((ya, yb), (yb, ya))[j % 2]

                def one(k, c, source=source, target=target, j=j):
                    total = yd[k]
                    if j:
                        v = source[k]
                        total = total + source[k - 1] + source[k + 1]
                        total = total + jnp.where(row8 == 0, 0.0, pltpu.roll(v, 1, 0))
                        total = total + jnp.where(row8 == 7, 0.0, pltpu.roll(v, 7, 0))
                        total = total + jnp.where(col8 == 0, 0.0, pltpu.roll(v, 1, 1))
                        total = total + jnp.where(col8 == 255, 0.0, pltpu.roll(v, 255, 1))
                    inside_x = (k + 8 * gx >= 8) & (k + 8 * gx < 136)
                    target[k] = total * jnp.where(inside_x, 1.0 / 6.0, 0.0)
                    return c

                for k in range(j + 1, 23 - j):
                    one(k, 0)
            rows = pl.ds(24 * f, 8)
            for k in range(8):
                fine_ref[k, rows, :] = fine_ref[k, rows, :] + ya[k + 8, :, own]

    for f in range(2):
        @pl.when(gx == 15 * f)
        def _():
            for k in range(16):
                if k != 15 * f:
                    arrived(r6, q6, k)
            xb6 = r6[0]
            for s in range(1, 16):
                xb6 = xb6 + r6[s]
            row, col = grid((48, 8))
            near_y = full(interpolate(row, col), xb6, NN)
            far_y = full(interpolate(row, col + 8), xb6, NN)
            row, col = grid((48, 128))
            ghost_x = full(jnp.where(col < 64, near_y + pltpu.roll(far_y, 64, 1), 0.0), int_z, NN)
            for k in range(1, 9):
                fr[k] = jnp.zeros((48, 256), F32)
                fa[k] = jnp.zeros((48, 256), F32)
                fb[k] = jnp.zeros((48, 256), F32)
            fr[1 + 7 * f] = ghost_x
            for j in range(8):
                source, target = ((fa, fb), (fb, fa))[j % 2]
                for k in range(j + 1):
                    index = 8 - k if f else 1 + k
                    target[index] = layer(source, fr, index) * sixth
            for k in range(8):
                fine_ref[k] = fine_ref[k] + fa[k + 1, 8:40, own]

    for copy in t2 + t4[0] + t4[1] + tz + t5 + [te]:
        copy.wait_send()
    for copy, sent, *_ in halo + tt:
        pl.when(sent)(copy.wait_send)
    @pl.when(at_y)
    def _():
        for k in range(1, 16):
            prepare(m7.at[k], r7.at[gx], s7.at[k], q7.at[gx], here).wait_send()

    for f in range(2):
        @pl.when(gx != 15 * f)
        def _():
            pltpu.make_async_remote_copy(
                src_ref=m6.at[f], dst_ref=r6.at[gx], send_sem=s6.at[f], recv_sem=q6.at[gx],
                device_id=real_row(15 * f), device_id_type=MESH,
            ).wait_send()


def body(density, fine_density, fine_start, anchor):
    high, low, lam = tables()
    vm = pl.BlockSpec(memory_space=pltpu.VMEM)
    dma = pltpu.SemaphoreType.DMA

    def f32(*shape):
        return pltpu.VMEM(shape, F32)

    def b16(*shape):
        return pltpu.VMEM(shape, BF16)

    big = f32(32, 16, 512)
    return pl.pallas_call(
        kernel,
        out_shape=(
            jax.ShapeDtypeStruct((32, 16, 512), F32), jax.ShapeDtypeStruct((8, 32, 128), F32)
        ),
        in_specs=[pl.BlockSpec(memory_space=pl.ANY)] * 9,
        out_specs=(vm, vm),
        scratch_shapes=[
            pltpu.SMEM((3,), jnp.int32), f32(8, 512), f32(2, 8, 128), f32(8, 128),
            big, f32(8, 32, 128), f32(8, 32, 128), b16(512, 512), b16(512, 512),
            big, f32(2, 32, 16, 256), f32(2, 32, 16, 256), f32(2, 32, 16, 256),
            f32(2, 32, 8, 512), f32(2, 31, 8, 512),
            f32(128, 128), f32(16, 8, 128), f32(16, 8, 128), f32(128, 128),
            f32(2, 16, 2, 128), f32(2, 2, 128),
            b16(2, 256, 512), b16(2, 256, 512), b16(512, 256), b16(512, 256),
            f32(512, 128), f32(2, 80, 256), f32(16, 512),
            f32(32, 8, 128), f32(32, 8, 128), f32(2, 4, 128), f32(32, 4, 128),
            f32(16, 1, 128), f32(16, 1, 128), f32(2, 8, 128), f32(16, 8, 128),
            f32(16, 8, 128), f32(16, 8, 128),
            f32(24, 48, 256), f32(24, 48, 256), f32(24, 48, 256),
            f32(10, 48, 256), f32(10, 48, 256), f32(10, 48, 256),
            f32(2, 8, 48, 256), f32(2, 8, 48, 256), f32(192, 128),
            f32(24, 8, 256), f32(24, 8, 256), f32(24, 8, 256),
            dma((2, 32)), dma((2, 32)), dma((16,)), dma((16,)), dma((16,)), dma((16,)),
            dma((2, 32)), dma((2, 32)), dma((4,)), dma((4,)), dma((2,)), dma((2,)),
            dma((32,)), dma((32,)), dma((4,)), dma((32,)), dma((16,)), dma((16,)),
            dma((2,)), dma((16,)), dma((10,)), dma((2, 2)), dma((2, 2)), dma((1,)), dma((1,)), dma((2,)), dma((2,)),
            dma((2,)), dma((2,)), dma((16,)), dma((16,)),
        ],
        compiler_params=pltpu.CompilerParams(
            collective_id=0, has_side_effects=True, vmem_limit_bytes=56 << 20
        ),
    )(anchor, jnp.asarray(np.tile(lam.reshape(1, 512), (8, 1))),
      jnp.asarray(np.tile(lam.reshape(512, 1), (1, 128))),
      jnp.asarray(np.tile(lam.reshape(4, 128), (2, 1))), density, fine_density, fine_start,
      jnp.asarray(high), jnp.asarray(low))


def solution(mesh):
    return jax.shard_map(
        body,
        mesh=mesh,
        in_specs=(P("gx", ("grp", "gy"), None), P("gx", "gy", "grp"), P("gx", "gy", "grp"), P()),
        out_specs=(P("gx", ("grp", "gy"), None), P("gx", "gy", "grp")),
        check_vma=False,
    )
```

```python
import functools
import math

import jax
import jax.numpy as jnp
import numpy as np
from jax import lax
from jax.experimental import pallas as pl
from jax.experimental.pallas import tpu as pltpu
from jax.sharding import PartitionSpec as P

MESH = pl.DeviceIdType.MESH
NC = 512
F32 = jnp.float32
CUT1, CUT4A, CUT4B = 32, 16, 32
WIDE = 4
BF16 = jnp.bfloat16


def tables():
    index = np.arange(1, NC + 1, dtype=np.int64)
    angle = (index[:, None] * index[None, :]) % (2 * (NC + 1))
    sine = math.sqrt(2.0 / (NC + 1)) * np.sin(angle * (math.pi / (NC + 1)))
    sine = sine.astype(np.float32)
    high = sine.astype(jnp.bfloat16)
    low = (sine - high.astype(np.float32)).astype(jnp.bfloat16)
    lam = 4.0 * np.sin(index * (math.pi / (2 * (NC + 1)))) ** 2
    return high, low, lam.astype(np.float32)


def split(value):
    high = value.astype(BF16)
    low = (value - high.astype(F32)).astype(BF16)
    return high, low


def dot3(a, b, dims):
    ah, al = a
    bh, bl = b
    dd = functools.partial(
        lax.dot_general, dimension_numbers=(dims, ((), ())), preferred_element_type=F32
    )
    return dd(ah, bh) + (dd(al, bh) + dd(ah, bl))


def mm(a, b, dims):
    return lax.dot_general(a, b, (dims, ((), ())), preferred_element_type=F32)


def full(a, b, dims):
    return lax.dot_general(
        a, b, (dims, ((), ())), precision=lax.Precision.HIGHEST, preferred_element_type=F32
    )


NN = ((1,), (0,))
NT = ((1,), (1,))
TN = ((0,), (0,))


def exchange(v, lane):
    v = list(v)
    for bit in (1, 2, 4, 8):
        upper = (lane & bit) != 0
        for i in range(16):
            if i & bit:
                continue
            a, c = v[i], v[i | bit]
            v[i] = jnp.where(upper, pltpu.roll(c, 8 * bit, 1), a)
            v[i | bit] = jnp.where(upper, c, pltpu.roll(a, 128 - 8 * bit, 1))
    return v


def exchange8(v, lane):
    v = list(v)
    for bit in (1, 2, 4):
        upper = (lane & bit) != 0
        for i in range(8):
            if i & bit:
                continue
            a, c = v[i], v[i | bit]
            v[i] = jnp.where(upper, pltpu.roll(c, 16 * bit, 1), a)
            v[i | bit] = jnp.where(upper, c, pltpu.roll(a, 128 - 16 * bit, 1))
    return v


def swap_groups(source, target, first, out_first):
    lane = lax.broadcasted_iota(jnp.int32, (8, 128), 1) // 8
    for a in range(2):
        for b in range(2):
            cols = slice(first + 128 * b, first + 128 * b + 128)
            outs = slice(out_first + 128 * a, out_first + 128 * a + 128)
            for row in (0, 8):
                v = [source[16 * a + q, row : row + 8, cols] for q in range(16)]
                for q, w in enumerate(exchange(v, lane)):
                    target[16 * b + q, row : row + 8, outs] = w


def device(core, x, y, z):
    return (core, x * 4 + z % 4, (z // 4) * 8 + y)


ORDER = [
    (dy, side, core) for dy in (4, 3, 5, 2, 6, 1, 7, 0) for side in (0, 1) for core in (0, 1)
]
PEERS = [ORDER[i] for i in np.random.RandomState(3).permutation(32)]
SIDES = [[o for o in PEERS if o[1] == side] for side in (0, 1)]
PEERS = [o for both in zip(*SIDES) for o in both]


def kernel(
    anchor_hbm, lamr_hbm, lamc_hbm, lamq_hbm, x_hbm, fd_hbm, fs_hbm, sh_hbm, sl_hbm, out_ref, fine_ref,
    anchor, lamr_ref, lamc_ref, lamq_ref, x_ref, fd_ref, fs_ref, sh_ref, sl_ref,
    za, zb, dd, gg, u, dtab, m1, r1, m2, r2, dint, rint, uh, ul, myh, myl, mz, wall, wys,
    mzx, rzx, my, ry, m5, r5, m6, r6, m7, r7, es, et, ed, fa, fb, fr, trace, tin, gz, ya, yb, yd,
    s1, q1, s2, q2, s3, q3, s4, q4, sh1, qh1, sd, qd, sz, qz, sy, qy, s5, q5, s6, q6, sin,
    st, qt, se, qe, sv, qv, sx, qx, s7, q7,
):
    core = lax.axis_index("grp")
    gx = lax.axis_index("gx")
    gy = lax.axis_index("gy")
    x, zl = gx // 4, gx % 4
    y, zh = gy % 8, gy // 8
    z = zh * 4 + zl
    me = core * 16 + gy
    zv = (z + 6) % 8
    lv, hv = zv % 4, zv // 4
    mid = core * 16 + hv * 8 + y
    pv = x * 4 + lv

    def to_mid(o):
        dy, side, oc = o
        ty = (y + dy + core * (8 - 2 * dy)) % 8
        tc = (core + oc) % 2
        return device(tc, x, ty, (zl + 4 * side + 2) % 8), tc * 16 + side * 8 + ty

    def to_real(o):
        dy, side, oc = o
        ty = (y + dy + core * (8 - 2 * dy)) % 8
        tc = (core + oc) % 2
        return device(tc, x, ty, lv + 4 * side), tc * 16 + side * 8 + ty

    def to_row(q):
        return device(core, q // 4, y, (q % 4 + 4 * hv + 2) % 8)

    def real_row(q):
        return device(core, q // 4, y, q % 4 + 4 * zh)

    here = (core, gx, gy)
    partner = (1 - core, gx, gy)
    own = pl.ds(pl.multiple_of(core * 128, 128), 128)

    def beside(ox, oy):
        return (core, (gx + ox + 16) % 16, (gy + oy + 16) % 16)

    fetch = []
    mine = [pl.ds(pl.multiple_of(256 * h + 8 * mid, 8), 8) for h in range(2)]
    for k, (src, dst) in enumerate((
        (x_hbm, x_ref), (sh_hbm, sh_ref), (sl_hbm, sl_ref), (fd_hbm, fd_ref), (fs_hbm, fs_ref),
        (lamr_hbm, lamr_ref), (lamq_hbm, lamq_ref), (lamc_hbm.at[mine[0], :], lamc_ref.at[0]),
        (lamc_hbm.at[mine[1], :], lamc_ref.at[1]), (anchor_hbm, anchor),
    )):
        copy = pltpu.make_async_copy(src, dst, sin.at[k])
        copy.start()
        fetch.append(copy)
    barrier = pltpu.get_barrier_semaphore()
    for o in PEERS:
        pl.semaphore_signal(barrier, inc=1, device_id=to_mid(o)[0], device_id_type=MESH)
    pl.semaphore_signal(barrier, inc=1, device_id=partner, device_id_type=MESH)
    for oy in (-1, 1):
        pl.semaphore_signal(barrier, inc=1, device_id=beside(0, oy), device_id_type=MESH)
    for k in range(1, 16):
        pl.semaphore_signal(barrier, inc=1, device_id=to_row((pv + k) % 16), device_id_type=MESH)
        pl.semaphore_signal(barrier, inc=1, device_id=real_row((gx + k) % 16), device_id_type=MESH)

    def arrived(ref, sem, index):
        pltpu.make_async_remote_copy(
            src_ref=ref.at[index], dst_ref=ref.at[index], send_sem=sem.at[index],
            recv_sem=sem.at[index], device_id=here, device_id_type=MESH,
        ).wait_recv()

    has_y = (gy > 0, gy < 15)
    has_x = (gx > 0, gx < 15)
    middle = (gy == 7) | (gy == 8)
    turns = ((gy > 0) & (gy != 8), (gy < 15) & (gy != 7))
    corner = pl.ds(pl.multiple_of((8 - gy) % 8 * 40, 8), 8)

    def prepare(src, dst, send_sem, recv_sem, target):
        return pltpu.make_async_remote_copy(
            src_ref=src, dst_ref=dst, send_sem=send_sem, recv_sem=recv_sem,
            device_id=target, device_id_type=MESH,
        )

    def send(*args):
        copy = prepare(*args)
        copy.start()
        return copy

    for copy in fetch[:3]:
        copy.wait()
    s_pair = (sh_ref[...], sl_ref[...])
    x_pair = split(x_ref[...].reshape(512, 512))
    halves = [slice(0, 256), slice(256, 512)]

    def forward_third(h):
        cols = tuple(part[:, halves[h]] for part in s_pair)
        za[:, :, halves[h]] = dot3(x_pair, cols, NN).reshape(32, 16, 256)
        swap_groups(za, zb.at[h], 256 * h, 0)

    t1 = [[], []]

    def send_first(h, lo, hi):
        for i in range(lo, hi):
            target, block = to_mid(PEERS[i])
            t1[h].append(
                send(zb.at[h, block], dd.at[h, me], s1.at[h, i], q1.at[h, me], target)
            )

    forward_third(0)
    for copy in fetch[3:]:
        copy.wait()
    a0, a1, a2 = anchor[0], anchor[1], anchor[2]
    fa[1:9, 8:40, own] = fs_ref[...]
    fr[1:9, 8:40, own] = fd_ref[...]
    pl.semaphore_wait(barrier, 65)
    halo = []
    for k, oy in enumerate((-1, 1)):
        rows = pl.ds(0, 8) if oy < 0 else pl.ds(24, 8)
        to_rows = pl.ds(40, 8) if oy < 0 else pl.ds(0, 8)
        for part, (src, dst) in enumerate(((fs_ref, fa), (fd_ref, fr))):
            copy = prepare(
                src.at[:, rows, :], dst.at[pl.ds(1, 8), to_rows, own],
                sh1.at[2 * k + part], qh1.at[2 * k + part], beside(0, oy),
            )
            pl.when(has_y[k])(copy.start)
            halo.append((copy, has_y[k], has_y[1 - k]))
    send_first(0, 0, 32)
    forward_third(1)
    send_first(1, 0, CUT1)
    for h in range(2):
        mu = lamr_ref[0:1, :] + jnp.concatenate([lamc_ref[h]] * 4, axis=1)

        def table(i, g, h=h, mu=mu):
            d = 1.0 / (1.0 + (mu + g))
            dtab[h, i] = d
            return (mu + g) * d

        lax.fori_loop(0, 31, table, jnp.ones((8, 512), F32))
        odd = pv % 2 == 1
        muq = jnp.where(odd, lamq_ref[2:4, :], lamq_ref[0:2, :]) + lamc_ref[h, pl.ds(pv // 2, 1), :]
        c = 0.5 * muq
        c1 = c
        r32 = 2.0 * (1.0 + c)
        for _ in range(4):
            c = 2.0 * c * (c + 2.0)
            r32 = r32 * (2.0 * (1.0 + c))
        c = 2.0 * c * (c + 2.0)
        rint[h] = r32
        g = jnp.ones((2, 128), F32)
        for i in range(15):
            d = 1.0 / (1.0 + (2.0 * c + g))
            dint[h, i] = d
            g = (2.0 * c + g) * d
        dint[h, 15] = 1.0 / (r32 * (1.0 + c1) + c + g)
    def cells(rows, cols, first):
        grid = lax.broadcasted_iota(jnp.int32, (rows, cols), 0)
        return jnp.where(grid == first, 1.0, 0.0).astype(BF16)

    lane = lax.broadcasted_iota(jnp.int32, (512, 256), 1)
    pick = cells(512, 256, a1 - 3 + 8 * (lane // 16) + lane % 16)
    myh[...] = mm(sh_ref[...], pick, NN).astype(BF16)
    myl[...] = mm(sl_ref[...], pick, NN).astype(BF16)
    lane = lax.broadcasted_iota(jnp.int32, (512, 128), 1)
    pick = cells(512, 128, a2 - 1 + 30 * core + lane)
    mz[...] = mm(sh_ref[...], pick, NN) + mm(sl_ref[...], pick, NN)
    def weights(cell, first, boxes, low_face, high_face):
        low_w = jnp.where(cell == first, 0.625, 0.0) + jnp.where(cell == first + 1, 0.375, 0.0)
        high_w = jnp.where(cell == first + boxes, 0.375, 0.0) + jnp.where(
            cell == first + boxes + 1, 0.625, 0.0
        )
        return jnp.where(low_face, low_w, 0.0) + jnp.where(high_face, high_w, 0.0)

    row = lax.broadcasted_iota(jnp.int32, (16, 512), 0)
    cell = lax.broadcasted_iota(jnp.int32, (16, 512), 1)
    wy = weights(cell, a1 - 1, 128, row == 0, row == 1).astype(BF16)
    wys[...] = mm(wy, sh_ref[...], NN) + mm(wy, sl_ref[...], NN)
    wz = weights(cell, a2 - 1, 64, row == 0, row == 1).astype(BF16)
    wz = mm(wz, sh_ref[...], NN) + mm(wz, sl_ref[...], NN)
    lane = lax.broadcasted_iota(jnp.int32, (512, 512), 1)
    pick = cells(512, 512, 256 * (lane // 256) + 8 * mid + lane % 8)
    wzh, wzl = split(wz)
    wz = mm(wzh, pick, NN) + mm(wzl, pick, NN)
    row = lax.broadcasted_iota(jnp.int32, (32, 256), 0)
    lane = lax.broadcasted_iota(jnp.int32, (32, 256), 1)
    row2 = lax.broadcasted_iota(jnp.int32, (16, 256), 0)
    lane2 = lax.broadcasted_iota(jnp.int32, (16, 256), 1)
    wx = weights(32 * pv + lane2 // 8, a0 - 1, 32, row2 < 8, row2 >= 8)
    wx = jnp.where(row2 % 8 == lane2 % 8, wx, 0.0)
    for h in range(2):
        for f in range(2):
            wall[h, 32 * f : 32 * f + 32, :] = jnp.where(
                row == lane // 8, wz[f : f + 1, halves[h]], 0.0
            )
        wall[h, 64:80, :] = wx
    for copy, _, comes in halo:
        pl.when(comes)(copy.wait_recv)
    pair = []
    for k, ref in enumerate((fa, fr)):
        view = ref.at[pl.ds(1, 8), :, own]
        copy = pltpu.make_async_remote_copy(
            src_ref=view, dst_ref=view, send_sem=sd.at[k], recv_sem=qd.at[k],
            device_id=partner, device_id_type=MESH,
        )
        copy.start()
        pair.append(copy)
    for copy in pair:
        copy.wait()
    fine_row = lax.broadcasted_iota(jnp.int32, (48, 256), 0) + 32 * gy
    fine_col = lax.broadcasted_iota(jnp.int32, (48, 256), 1)
    inside_y = (fine_row >= 8) & (fine_row < 520)
    sixth = jnp.where(inside_y, 1.0 / 6.0, 0.0)

    def layer(source, extra, k):
        v = source[k]
        total = (source[k - 1] + source[k + 1]) + extra[k]
        total = total + (pltpu.roll(v, 1, 0) + pltpu.roll(v, 47, 0))
        total = total + jnp.where(fine_col == 0, 0.0, pltpu.roll(v, 1, 1))
        return total + jnp.where(fine_col == 255, 0.0, pltpu.roll(v, 255, 1))

    for k in (0, 9):
        fa[k] = jnp.zeros((48, 256), F32)
        fb[k] = jnp.zeros((48, 256), F32)
    for k in range(1, 9):
        fa[k] = jnp.where(inside_y, fa[k], 0.0)
        fr[k] = jnp.where(inside_y, fr[k], 0.0) * (-1.0 / 16.0)
        es[k + 7] = fa[k]

    def alone(j, carry):
        for part, (source, target) in enumerate(((fa, fb), (fb, fa))):
            trace[0, 2 * j + part] = source[1]
            trace[1, 2 * j + part] = source[8]

            def four(k, c):
                for m in range(4):
                    index = 1 + 4 * k + m
                    target[index] = layer(source, fr, index) * sixth
                return c

            lax.fori_loop(0, 2, four, 0)
        return carry

    lax.fori_loop(0, 4, alone, 0)

    t2 = []
    t4 = [[], []]

    def second_and_eliminate(h):
        value = dd[h].reshape(512, 256)
        u[h] = dot3(split(value), s_pair, TN).reshape(32, 8, 512)
        first = -u[h, 0]
        u[h, 0] = first
        q0 = dtab[h, 30]

        def forward(i, carry):
            yv, q, e = carry
            w = u[h, i]
            yv = dtab[h, i - 1] * yv - w
            u[h, i] = yv
            q = q * dtab[h, 30 - i]
            return yv, q, e - q * w

        yv, _, e = lax.fori_loop(1, 31, forward, (first, q0, q0 * first))
        b = q0 * yv - u[h, 31]
        for j in range(4):
            start = 8 * (j // 2) + j % 2 + 4 * h
            m1[pl.ds(start, 8, stride=16), :] = e[:, 128 * j : 128 * j + 128]
            m1[pl.ds(start + 2, 8, stride=16), :] = b[:, 128 * j : 128 * j + 128]

    def send_ends():
        for k in range(1, 16):
            q = (pv + k) % 16
            t2.append(send(
                m1.at[pl.ds(pl.multiple_of(q * 8, 8), 8), :], r1.at[pv], s2.at[k], q2.at[pv],
                to_row(q),
            ))
        r1[pv] = m1[pl.ds(pl.multiple_of(pv * 8, 8), 8), :]

    def separators():
        for h in range(2):
            ys = []
            prev = None
            for p in range(16):
                end = r1[p, 4 * h + 2 : 4 * h + 4, :]
                if p < 15:
                    end = end + r1[p + 1, 4 * h : 4 * h + 2, :]
                end = rint[h] * end
                prev = end if p == 0 else end + dint[h, p - 1] * prev
                ys.append(prev)
            m2[0, 4 * h : 4 * h + 2, :] = jnp.zeros((2, 128), F32)
            sol = dint[h, 15] * ys[15]
            m2[15, 4 * h + 2 : 4 * h + 4, :] = sol
            for p in range(14, -1, -1):
                sol = dint[h, p] * (sol + ys[p])
                m2[p + 1, 4 * h : 4 * h + 2, :] = sol
                m2[p, 4 * h + 2 : 4 * h + 4, :] = sol
        for k in range(1, 16):
            q = (pv + k) % 16
            t2.append(send(
                m2.at[q], r2.at[pl.ds(pl.multiple_of(pv * 8, 8), 8), :], s3.at[k], q3.at[pv],
                to_row(q),
            ))
        r2[pl.ds(pl.multiple_of(pv * 8, 8), 8), :] = m2[pv]

    def wait_separators():
        for k in range(1, 16):
            q = (pv + k) % 16
            view = r2.at[pl.ds(pl.multiple_of(q * 8, 8), 8), :]
            pltpu.make_async_remote_copy(
                src_ref=view, dst_ref=view, send_sem=s3.at[k], recv_sem=q3.at[q],
                device_id=here, device_id_type=MESH,
            ).wait_recv()

    def substitute(h):
        starts = [8 * (j // 2) + j % 2 + 4 * h for j in range(4)]
        left = jnp.concatenate([r2[pl.ds(j, 8, stride=16), :] for j in starts], axis=1)
        right = jnp.concatenate([r2[pl.ds(j + 2, 8, stride=16), :] for j in starts], axis=1)

        def spread(i, t):
            u[h, i] = u[h, i] + t
            return dtab[h, i] * t

        lax.fori_loop(0, 31, spread, left)
        u[h, 31] = right

        def backward(k, v):
            i = 30 - k
            v = dtab[h, i] * (v + u[h, i])
            u[h, i] = v
            return v

        lax.fori_loop(0, 31, backward, right)
        high, low = split(u[h].reshape(256, 512))
        uh[h] = high
        ul[h] = low

    def inverse_second(h):
        for copy in t1[h]:
            copy.wait_send()
        zb[h] = dot3(s_pair, (uh[h], ul[h]), NT).reshape(32, 16, 256)

    def send_last(h, lo, hi):
        for i in range(lo, hi):
            target, block = to_real(PEERS[i])
            t4[h].append(
                send(zb.at[h, block], gg.at[h, mid], s4.at[h, i], q4.at[h, mid], target)
            )

    tt = []

    def send_traces(part):
        sweeps = pl.ds(4 * part, 4)
        for side, ox in enumerate((-1, 1)):
            copy = prepare(
                trace.at[side, sweeps, pl.ds(8, 32), own],
                tin.at[1 - side, sweeps, pl.ds(8, 32), own],
                st.at[side, part], qt.at[1 - side, part], beside(ox, 0),
            )
            pl.when(has_x[side])(copy.start)
            tt.append((copy, has_x[side]))

    def send_corners():
        for side, ox in enumerate((-1, 1)):
            copy = prepare(
                trace.at[side, :, corner, own], tin.at[1 - side, :, corner, own], sx.at[side],
                qx.at[1 - side], beside(ox, 0),
            )
            sent = has_x[side] & middle
            pl.when(sent)(copy.start)
            tt.append((copy, sent))

    for s in range(32):
        arrived(dd.at[0], q1.at[0], s)
    second_and_eliminate(0)
    for s in range(32):
        arrived(dd.at[1], q1.at[1], s)
    second_and_eliminate(1)
    send_ends()
    send_traces(0)
    send_traces(1)
    send_corners()
    for k in range(1, 16):
        arrived(r1, q2, (pv + k) % 16)
    separators()
    wait_separators()
    substitute(0)
    inverse_second(0)
    send_last(0, 0, CUT4A)
    for part in range(2):
        sweeps = pl.ds(4 * part, 4)
        for side in range(2):
            view = tin.at[side, sweeps, pl.ds(8, 32), own]
            copy = pltpu.make_async_remote_copy(
                src_ref=view, dst_ref=view, send_sem=st.at[side, part],
                recv_sem=qt.at[side, part], device_id=here, device_id_type=MESH,
            )
            pl.when(has_x[side])(copy.wait_recv)
    for side in range(2):
        copy = prepare(
            tin.at[side, :, corner, own], tin.at[side, :, corner, own], sx.at[side], qx.at[side],
            here,
        )
        pl.when(has_x[side] & middle)(copy.wait_recv)

        @pl.when(jnp.logical_not(has_x[side]))
        def _():
            tin[side, :, 8:40, own] = jnp.zeros((8, 32, 128), F32)

        @pl.when(jnp.logical_not(has_x[side]) & middle)
        def _():
            tin[side, :, corner, own] = jnp.zeros((8, 8, 128), F32)

        @pl.when(jnp.logical_not(has_y[side]))
        def _():
            tin[:, :, 40 * side : 40 * side + 8, own] = jnp.zeros((2, 8, 8, 128), F32)

    for k, oy in enumerate((-1, 1)):
        rows = pl.ds(8, 8) if oy < 0 else pl.ds(32, 8)
        to_rows = pl.ds(40, 8) if oy < 0 else pl.ds(0, 8)
        copy = prepare(
            tin.at[:, :, rows, own], tin.at[:, :, to_rows, own], sv.at[k], qv.at[k], beside(0, oy)
        )
        pl.when(turns[k])(copy.start)
        tt.append((copy, turns[k]))
    substitute(1)
    face = []
    cut_x = []

    def faces(h):
        pair_h = (uh[h], ul[h])
        rows = dot3(split(wall[h]), pair_h, NN)
        face.append(rows[:64])
        cut_x.append(rows[64:])
        line = dot3(split(wys[...]), pair_h, NT)
        for f in range(2):
            for t in range(2):
                my[f, 2 * h + t : 2 * h + t + 1, :] = line[f : f + 1, 128 * t : 128 * t + 128]

    faces(0)
    faces(1)
    rows = jnp.concatenate([face[0] + face[1], cut_x[0], cut_x[1]], axis=0)
    rows = dot3(split(rows), (myh[...], myl[...]), NN)
    lane = lax.broadcasted_iota(jnp.int32, (8, 128), 1) // 16
    for f in range(2):
        for t in range(2):
            cols = slice(128 * t, 128 * t + 128)
            v = [rows[32 * f + 8 * k : 32 * f + 8 * k + 8, cols] for k in range(4)]
            for g in range(2):
                for h in range(2):
                    start = 64 + 16 * h + 8 * g
                    v.append(rows[start : start + 8, cols])
            for q, w in enumerate(exchange8(v, lane)):
                mzx[16 * f + 8 * t + q] = w
    tz = []
    for i, o in enumerate(PEERS):
        target, block = to_real(o)
        tz.append(send(mzx.at[block], rzx.at[mid], sz.at[i], qz.at[mid], target))
    for f in range(2):
        for g in range(2):
            tz.append(send(
                my.at[f], ry.at[mid], sy.at[2 * f + g], qy.at[mid],
                device(g, x, 7 * f, lv + 4 * f),
            ))
    send_last(0, CUT4A, 32)
    inverse_second(1)
    send_last(1, 0, CUT4B)
    for k in range(2):
        view = tin.at[:, :, pl.ds(40 - 40 * k, 8), own]
        copy = pltpu.make_async_remote_copy(
            src_ref=view, dst_ref=view, send_sem=sv.at[k], recv_sem=qv.at[k], device_id=here,
            device_id_type=MESH,
        )
        pl.when(turns[1 - k])(copy.wait_recv)
    view = tin.at[:, :, :, own]
    te = send(view, view, se.at[0], qe.at[0], partner)
    te.wait_recv()
    def factor(k):
        inside_x = (k + 8 * gx >= 8) & (k + 8 * gx < 136)
        return jnp.where(inside_x, sixth, 0.0)

    ends = (jnp.where(gx == 0, 0.0, sixth), jnp.where(gx == 15, 0.0, sixth))
    for k in (4, 5, 6, 7, 16, 17, 18, 19):
        es[k] = jnp.zeros((48, 256), F32)
        ed[k] = jnp.zeros((48, 256), F32)
    for k in (3, 4, 5, 6, 17, 18, 19, 20):
        et[k] = jnp.zeros((48, 256), F32)
    for k in range(8, 16):
        ed[k] = fr[k - 7]
    for j in range(8):
        source, target = ((es, et), (et, es))[j % 2]
        depth = min(j + 1, 7 - j)

        def some(k, c, source=source, target=target, first=8 - depth, step=WIDE):
            for m in range(step):
                index = first + step * k + m
                target[index] = layer(source, ed, index) * factor(index)
            return c

        layers = 8 + 2 * depth
        lax.fori_loop(0, layers // WIDE, some, 0)
        if layers % WIDE:
            some(0, 0, first=8 - depth + layers // WIDE * WIDE, step=layers % WIDE)
        target[8] = target[8] + tin[0, j] * ends[0]
        target[15] = target[15] + tin[1, j] * ends[1]
    for s in range(32):
        arrived(rzx, qz, s)
    zsum = rzx[0]
    for s in range(1, 32):
        zsum = zsum + rzx[s]
    row = lax.broadcasted_iota(jnp.int32, (128, 512), 0)
    col = lax.broadcasted_iota(jnp.int32, (128, 512), 1)
    tile = jnp.where(row == col // 128 * 16 + col % 16, 1.0, 0.0)
    spread_z = full(zsum, tile, NN)
    spread_z = jnp.concatenate([spread_z[:, 128 * h : 128 * h + 128] for h in range(4)], axis=0)
    lane32 = lax.broadcasted_iota(jnp.int32, (32, 128), 1) // 16
    spread_z = jnp.concatenate(
        [jnp.where(lane32 == k, spread_z, 0.0) for k in range(8)], axis=0
    )
    row = lax.broadcasted_iota(jnp.int32, (16, 256), 0)
    col = lax.broadcasted_iota(jnp.int32, (16, 256), 1)
    pick = jnp.where(a0 - 3 + 2 * row + col // 32 == 32 * gx + col % 32, 1.0, 0.0)
    rows = full(pick, spread_z, NN)
    for q in range(16):
        m5[q] = rows[q : q + 1]
    t5 = []
    for k in range(1, 16):
        q = (gx + k) % 16
        t5.append(send(m5.at[q], r5.at[gx], s5.at[k], q5.at[gx], real_row(q)))
    r5[gx] = m5[gx]
    got = rzx[...].reshape(256, 128)
    parts = [full(got, mz[256 * k : 256 * k + 256, :], TN) for k in range(2)]
    left_half = lax.broadcasted_iota(jnp.int32, (8, 128), 1) < 64
    for f in range(2):
        cells_x = parts[0][64 + 32 * f : 80 + 32 * f] + parts[1][80 + 32 * f : 96 + 32 * f]
        m6[f] = jnp.where(left_half, cells_x[:8], pltpu.roll(cells_x[8:], 64, 1))
    for f in range(2):
        end = 15 * f
        copy = prepare(m6.at[f], r6.at[gx], s6.at[f], q6.at[gx], real_row(end))
        pl.when(gx != end)(copy.start)

        @pl.when(gx == end)
        def _():
            r6[gx] = m6[f]

    at_y = (gy == 0) | (gy == 15)

    @pl.when(at_y)
    def _():
        for s in range(32):
            arrived(ry, qy, s)
        lane8 = lax.broadcasted_iota(jnp.int32, (32, 128), 1) % 8
        group = lax.broadcasted_iota(jnp.int32, (16, 128), 0)
        member = lax.broadcasted_iota(jnp.int32, (16, 128), 1) // 8
        gather = jnp.where(group == member, 1.0, 0.0)
        part = []
        for t in range(2):
            total = None
            for h in range(2):
                v = ry[:, 2 * h + t, :]
                v = jnp.concatenate([jnp.where(lane8 == k, v, 0.0) for k in range(8)], axis=0)
                modes = jnp.concatenate(
                    [mz[pl.ds(256 * h + k, 32, stride=8), :] for k in range(8)], axis=0
                )
                w = full(v, modes, TN)
                total = w if total is None else total + w
            part.append(full(gather, total, NN))
        row = lax.broadcasted_iota(jnp.int32, (128, 32), 0)
        col = lax.broadcasted_iota(jnp.int32, (128, 32), 1)
        pick = jnp.where(a0 - 3 + 2 * (row // 8) + row % 8 == 32 * gx + col, 1.0, 0.0)
        m7[...] = full(pick, jnp.concatenate(part, axis=0), NN).reshape(16, 8, 128)
        for k in range(1, 16):
            q = (gx + k) % 16
            send(m7.at[q], r7.at[gx], s7.at[k], q7.at[gx], real_row(q))
        r7[gx] = m7[gx]

    send_last(1, CUT4B, 32)
    for s in range(32):
        arrived(gg.at[0], q4.at[0], s)
    def inverse_third(h):
        swap_groups(gg.at[h], za, 0, 256 * h)
        rows_h = tuple(part[halves[h], :] for part in s_pair)
        return dot3(split(za[:, :, halves[h]].reshape(512, 256)), rows_h, NN).reshape(32, 16, 512)

    out_ref[...] = inverse_third(0)
    for k in range(1, 16):
        arrived(r5, q5, (gx + k) % 16)
    def interpolate(fine, cell):
        scaled = 2 * fine + 5
        bottom = scaled // 8
        t = (scaled % 8).astype(F32) * 0.125
        return jnp.where(cell == bottom, 1.0 - t, 0.0) + jnp.where(cell == bottom + 1, t, 0.0)

    def grid(shape):
        return (lax.broadcasted_iota(jnp.int32, shape, 0), lax.broadcasted_iota(jnp.int32, shape, 1))

    row, col = grid((24, 8))
    int_x = interpolate(row, col)
    row, col = grid((128, 128))
    int_y = jnp.where(row < 48, interpolate(row, col % 16), 0.0)
    zb5 = r5[0]
    for s in range(1, 16):
        zb5 = zb5 + r5[s]
    row, col = grid((8, 128))
    zb5 = jnp.where(row == col // 16, jnp.broadcast_to(zb5, (8, 128)), 0.0)
    ghost_z = full(full(int_x, zb5, NN), int_y, NT)
    row, col = grid((24, 128))
    inside = (row + 8 * gx >= 8) & (row + 8 * gx < 136) & (col < 48)
    inside = inside & (col + 32 * gy >= 8) & (col + 32 * gy < 520)
    sixth_z = jnp.where(inside, 1.0 / 6.0, 0.0)
    plane = []
    for j in range(8):
        new = []
        for k in range(j + 1):
            total = ghost_z if k == 0 else plane[k - 1]
            if k + 1 < j:
                total = total + plane[k + 1]
            if k < j:
                v = plane[k]
                total = total + (pltpu.roll(v, 1, 0) + pltpu.roll(v, 23, 0))
                total = total + (pltpu.roll(v, 1, 1) + pltpu.roll(v, 127, 1))
            new.append(total * sixth_z)
        plane = new
    for k in range(8):
        gz[pl.ds(k, 24, stride=8), :] = plane[k]
    row, col = grid((8, 128))
    place = jnp.where(col == jnp.where(core == 0, row, 127 - row), 1.0, 0.0)
    for k in range(8):
        part = full(gz[8 * (k + 8) : 8 * (k + 8) + 8, :], place, TN)
        fine_ref[k] = es[k + 8, 8:40, own] + part[8:40]

    row, col = grid((128, 256))
    int_z = jnp.where(row < 64, interpolate(col, row + 30 * core), 0.0)

    for s in range(32):
        arrived(gg.at[1], q4.at[1], s)
    out_ref[...] = out_ref[...] + inverse_third(1)
    row8 = lax.broadcasted_iota(jnp.int32, (8, 256), 0)
    col8 = lax.broadcasted_iota(jnp.int32, (8, 256), 1)
    for f in range(2):
        @pl.when(gy == 15 * f)
        def _():
            for k in range(1, 16):
                arrived(r7, q7, (gx + k) % 16)
            yb7 = r7[0]
            for k in range(1, 16):
                yb7 = yb7 + r7[k]
            ghost_y = full(full(int_x, yb7, NN), int_z, NN)
            edge = 7 * f
            for k in range(24):
                yd[k] = jnp.where(row8 == edge, ghost_y[k : k + 1], 0.0)
            for j in range(8):
                source, target = ((ya, yb), (yb, ya))[j % 2]

                def one(k, c, source=source, target=target, j=j):
                    total = yd[k]
                    if j:
                        v = source[k]
                        total = total + source[k - 1] + source[k + 1]
                        total = total + jnp.where(row8 == 0, 0.0, pltpu.roll(v, 1, 0))
                        total = total + jnp.where(row8 == 7, 0.0, pltpu.roll(v, 7, 0))
                        total = total + jnp.where(col8 == 0, 0.0, pltpu.roll(v, 1, 1))
                        total = total + jnp.where(col8 == 255, 0.0, pltpu.roll(v, 255, 1))
                    inside_x = (k + 8 * gx >= 8) & (k + 8 * gx < 136)
                    target[k] = total * jnp.where(inside_x, 1.0 / 6.0, 0.0)
                    return c

                for k in range(j + 1, 23 - j):
                    one(k, 0)
            rows = pl.ds(24 * f, 8)
            for k in range(8):
                fine_ref[k, rows, :] = fine_ref[k, rows, :] + ya[k + 8, :, own]

    for f in range(2):
        @pl.when(gx == 15 * f)
        def _():
            for k in range(16):
                if k != 15 * f:
                    arrived(r6, q6, k)
            xb6 = r6[0]
            for s in range(1, 16):
                xb6 = xb6 + r6[s]
            row, col = grid((48, 8))
            near_y = full(interpolate(row, col), xb6, NN)
            far_y = full(interpolate(row, col + 8), xb6, NN)
            row, col = grid((48, 128))
            ghost_x = full(jnp.where(col < 64, near_y + pltpu.roll(far_y, 64, 1), 0.0), int_z, NN)
            for k in range(1, 9):
                fr[k] = jnp.zeros((48, 256), F32)
                fa[k] = jnp.zeros((48, 256), F32)
                fb[k] = jnp.zeros((48, 256), F32)
            fr[1 + 7 * f] = ghost_x
            for j in range(8):
                source, target = ((fa, fb), (fb, fa))[j % 2]
                for k in range(j + 1):
                    index = 8 - k if f else 1 + k
                    target[index] = layer(source, fr, index) * sixth
            for k in range(8):
                fine_ref[k] = fine_ref[k] + fa[k + 1, 8:40, own]

    for copy in t2 + t4[0] + t4[1] + tz + t5 + [te]:
        copy.wait_send()
    for copy, sent, *_ in halo + tt:
        pl.when(sent)(copy.wait_send)
    @pl.when(at_y)
    def _():
        for k in range(1, 16):
            prepare(m7.at[k], r7.at[gx], s7.at[k], q7.at[gx], here).wait_send()

    for f in range(2):
        @pl.when(gx != 15 * f)
        def _():
            pltpu.make_async_remote_copy(
                src_ref=m6.at[f], dst_ref=r6.at[gx], send_sem=s6.at[f], recv_sem=q6.at[gx],
                device_id=real_row(15 * f), device_id_type=MESH,
            ).wait_send()


def body(density, fine_density, fine_start, anchor):
    high, low, lam = tables()
    vm = pl.BlockSpec(memory_space=pltpu.VMEM)
    dma = pltpu.SemaphoreType.DMA

    def f32(*shape):
        return pltpu.VMEM(shape, F32)

    def b16(*shape):
        return pltpu.VMEM(shape, BF16)

    big = f32(32, 16, 512)
    return pl.pallas_call(
        kernel,
        out_shape=(
            pltpu.VMEM((32, 16, 512), F32), pltpu.VMEM((8, 32, 128), F32)
        ),
        in_specs=[pl.BlockSpec(memory_space=pl.ANY)] * 9,
        out_specs=(vm, vm),
        scratch_shapes=[
            pltpu.SMEM((3,), jnp.int32), f32(8, 512), f32(2, 8, 128), f32(8, 128),
            big, f32(8, 32, 128), f32(8, 32, 128), b16(512, 512), b16(512, 512),
            big, f32(2, 32, 16, 256), f32(2, 32, 16, 256), f32(2, 32, 16, 256),
            f32(2, 32, 8, 512), f32(2, 31, 8, 512),
            f32(128, 128), f32(16, 8, 128), f32(16, 8, 128), f32(128, 128),
            f32(2, 16, 2, 128), f32(2, 2, 128),
            b16(2, 256, 512), b16(2, 256, 512), b16(512, 256), b16(512, 256),
            f32(512, 128), f32(2, 80, 256), f32(16, 512),
            f32(32, 8, 128), f32(32, 8, 128), f32(2, 4, 128), f32(32, 4, 128),
            f32(16, 1, 128), f32(16, 1, 128), f32(2, 8, 128), f32(16, 8, 128),
            f32(16, 8, 128), f32(16, 8, 128),
            f32(24, 48, 256), f32(24, 48, 256), f32(24, 48, 256),
            f32(10, 48, 256), f32(10, 48, 256), f32(10, 48, 256),
            f32(2, 8, 48, 256), f32(2, 8, 48, 256), f32(192, 128),
            f32(24, 8, 256), f32(24, 8, 256), f32(24, 8, 256),
            dma((2, 32)), dma((2, 32)), dma((16,)), dma((16,)), dma((16,)), dma((16,)),
            dma((2, 32)), dma((2, 32)), dma((4,)), dma((4,)), dma((2,)), dma((2,)),
            dma((32,)), dma((32,)), dma((4,)), dma((32,)), dma((16,)), dma((16,)),
            dma((2,)), dma((16,)), dma((10,)), dma((2, 2)), dma((2, 2)), dma((1,)), dma((1,)), dma((2,)), dma((2,)),
            dma((2,)), dma((2,)), dma((16,)), dma((16,)),
        ],
        compiler_params=pltpu.CompilerParams(
            collective_id=0, has_side_effects=True, vmem_limit_bytes=56 << 20
        ),
    )(anchor, jnp.asarray(np.tile(lam.reshape(1, 512), (8, 1))),
      jnp.asarray(np.tile(lam.reshape(512, 1), (1, 128))),
      jnp.asarray(np.tile(lam.reshape(4, 128), (2, 1))), density, fine_density, fine_start,
      jnp.asarray(high), jnp.asarray(low))


def solution(mesh):
    return jax.shard_map(
        body,
        mesh=mesh,
        in_specs=(P("gx", ("grp", "gy"), None), P("gx", "gy", "grp"), P("gx", "gy", "grp"), P()),
        out_specs=(P("gx", ("grp", "gy"), None), P("gx", "gy", "grp")),
        check_vma=False,
    )
```

```python
import functools
import math

import jax
import jax.numpy as jnp
import numpy as np
from jax import lax
from jax.experimental import pallas as pl
from jax.experimental.pallas import tpu as pltpu
from jax.sharding import PartitionSpec as P

MESH = pl.DeviceIdType.MESH
NC = 512
F32 = jnp.float32
CUT1, CUT4A, CUT4B = 32, 16, 32
WIDE = 4
BF16 = jnp.bfloat16


def tables():
    index = np.arange(1, NC + 1, dtype=np.int64)
    angle = (index[:, None] * index[None, :]) % (2 * (NC + 1))
    sine = math.sqrt(2.0 / (NC + 1)) * np.sin(angle * (math.pi / (NC + 1)))
    sine = sine.astype(np.float32)
    high = sine.astype(jnp.bfloat16)
    low = (sine - high.astype(np.float32)).astype(jnp.bfloat16)
    lam = 4.0 * np.sin(index * (math.pi / (2 * (NC + 1)))) ** 2
    return high, low, lam.astype(np.float32)


def split(value):
    high = value.astype(BF16)
    low = (value - high.astype(F32)).astype(BF16)
    return high, low


def dot3(a, b, dims):
    ah, al = a
    bh, bl = b
    dd = functools.partial(
        lax.dot_general, dimension_numbers=(dims, ((), ())), preferred_element_type=F32
    )
    return dd(ah, bh) + (dd(al, bh) + dd(ah, bl))


def mm(a, b, dims):
    return lax.dot_general(a, b, (dims, ((), ())), preferred_element_type=F32)


def full(a, b, dims):
    return lax.dot_general(
        a, b, (dims, ((), ())), precision=lax.Precision.HIGHEST, preferred_element_type=F32
    )


NN = ((1,), (0,))
NT = ((1,), (1,))
TN = ((0,), (0,))


def exchange(v, lane):
    v = list(v)
    for bit in (1, 2, 4, 8):
        upper = (lane & bit) != 0
        for i in range(16):
            if i & bit:
                continue
            a, c = v[i], v[i | bit]
            v[i] = jnp.where(upper, pltpu.roll(c, 8 * bit, 1), a)
            v[i | bit] = jnp.where(upper, c, pltpu.roll(a, 128 - 8 * bit, 1))
    return v


def exchange8(v, lane):
    v = list(v)
    for bit in (1, 2, 4):
        upper = (lane & bit) != 0
        for i in range(8):
            if i & bit:
                continue
            a, c = v[i], v[i | bit]
            v[i] = jnp.where(upper, pltpu.roll(c, 16 * bit, 1), a)
            v[i | bit] = jnp.where(upper, c, pltpu.roll(a, 128 - 16 * bit, 1))
    return v


def swap_groups(source, target, first, out_first):
    lane = lax.broadcasted_iota(jnp.int32, (8, 128), 1) // 8
    for a in range(2):
        for b in range(2):
            cols = slice(first + 128 * b, first + 128 * b + 128)
            outs = slice(out_first + 128 * a, out_first + 128 * a + 128)
            for row in (0, 8):
                v = [source[16 * a + q, row : row + 8, cols] for q in range(16)]
                for q, w in enumerate(exchange(v, lane)):
                    target[16 * b + q, row : row + 8, outs] = w


def device(core, x, y, z):
    return (core, x * 4 + z % 4, (z // 4) * 8 + y)


ORDER = [
    (dy, side, core) for dy in (4, 3, 5, 2, 6, 1, 7, 0) for side in (0, 1) for core in (0, 1)
]
PEERS = [ORDER[i] for i in np.random.RandomState(3).permutation(32)]
SIDES = [[o for o in PEERS if o[1] == side] for side in (0, 1)]
PEERS = [o for both in zip(*SIDES) for o in both]


def kernel(
    anchor_hbm, lamr_hbm, lamc_hbm, lamq_hbm, x_hbm, fd_hbm, fs_hbm, sh_hbm, sl_hbm, out_ref, fine_ref,
    anchor, lamr_ref, lamc_ref, lamq_ref, x_ref, fd_ref, fs_ref, sh_ref, sl_ref,
    za, zb, dd, gg, u, dtab, m1, r1, m2, r2, dint, rint, uh, ul, myh, myl, mz, wall, wys,
    mzx, rzx, my, ry, m5, r5, m6, r6, m7, r7, es, et, ed, fa, fb, fr, trace, tin, gz, ya, yb, yd,
    s1, q1, s2, q2, s3, q3, s4, q4, sh1, qh1, sd, qd, sz, qz, sy, qy, s5, q5, s6, q6, sin,
    st, qt, se, qe, sv, qv, sx, qx, s7, q7,
):
    core = lax.axis_index("grp")
    gx = lax.axis_index("gx")
    gy = lax.axis_index("gy")
    x, zl = gx // 4, gx % 4
    y, zh = gy % 8, gy // 8
    z = zh * 4 + zl
    me = core * 16 + gy
    zv = (z + 6) % 8
    lv, hv = zv % 4, zv // 4
    mid = core * 16 + hv * 8 + y
    pv = x * 4 + lv

    def to_mid(o):
        dy, side, oc = o
        ty = (y + dy + core * (8 - 2 * dy)) % 8
        tc = (core + oc) % 2
        return device(tc, x, ty, (zl + 4 * side + 2) % 8), tc * 16 + side * 8 + ty

    def to_real(o):
        dy, side, oc = o
        ty = (y + dy + core * (8 - 2 * dy)) % 8
        tc = (core + oc) % 2
        return device(tc, x, ty, lv + 4 * side), tc * 16 + side * 8 + ty

    def to_row(q):
        return device(core, q // 4, y, (q % 4 + 4 * hv + 2) % 8)

    def real_row(q):
        return device(core, q // 4, y, q % 4 + 4 * zh)

    here = (core, gx, gy)
    partner = (1 - core, gx, gy)
    own = pl.ds(pl.multiple_of(core * 128, 128), 128)

    def beside(ox, oy):
        return (core, (gx + ox + 16) % 16, (gy + oy + 16) % 16)

    fetch = []
    mine = [pl.ds(pl.multiple_of(256 * h + 8 * mid, 8), 8) for h in range(2)]
    for k, (src, dst) in enumerate((
        (x_hbm, x_ref), (sh_hbm, sh_ref), (sl_hbm, sl_ref), (fd_hbm, fd_ref), (fs_hbm, fs_ref),
        (lamr_hbm, lamr_ref), (lamq_hbm, lamq_ref), (lamc_hbm.at[mine[0], :], lamc_ref.at[0]),
        (lamc_hbm.at[mine[1], :], lamc_ref.at[1]), (anchor_hbm, anchor),
    )):
        copy = pltpu.make_async_copy(src, dst, sin.at[k])
        copy.start()
        fetch.append(copy)
    barrier = pltpu.get_barrier_semaphore()
    for o in PEERS:
        pl.semaphore_signal(barrier, inc=1, device_id=to_mid(o)[0], device_id_type=MESH)
    pl.semaphore_signal(barrier, inc=1, device_id=partner, device_id_type=MESH)
    for oy in (-1, 1):
        pl.semaphore_signal(barrier, inc=1, device_id=beside(0, oy), device_id_type=MESH)
    for k in range(1, 16):
        pl.semaphore_signal(barrier, inc=1, device_id=to_row((pv + k) % 16), device_id_type=MESH)
        pl.semaphore_signal(barrier, inc=1, device_id=real_row((gx + k) % 16), device_id_type=MESH)

    def arrived(ref, sem, index):
        pltpu.make_async_remote_copy(
            src_ref=ref.at[index], dst_ref=ref.at[index], send_sem=sem.at[index],
            recv_sem=sem.at[index], device_id=here, device_id_type=MESH,
        ).wait_recv()

    has_y = (gy > 0, gy < 15)
    has_x = (gx > 0, gx < 15)
    middle = (gy == 7) | (gy == 8)
    turns = ((gy > 0) & (gy != 8), (gy < 15) & (gy != 7))
    corner = pl.ds(pl.multiple_of((15 - gy) // 8 * 40, 8), 8)

    def prepare(src, dst, send_sem, recv_sem, target):
        return pltpu.make_async_remote_copy(
            src_ref=src, dst_ref=dst, send_sem=send_sem, recv_sem=recv_sem,
            device_id=target, device_id_type=MESH,
        )

    def send(*args):
        copy = prepare(*args)
        copy.start()
        return copy

    for copy in fetch[:3]:
        copy.wait()
    s_pair = (sh_ref[...], sl_ref[...])
    x_pair = split(x_ref[...].reshape(512, 512))
    halves = [slice(0, 256), slice(256, 512)]

    def forward_third(h):
        cols = tuple(part[:, halves[h]] for part in s_pair)
        za[:, :, halves[h]] = dot3(x_pair, cols, NN).reshape(32, 16, 256)
        swap_groups(za, zb.at[h], 256 * h, 0)

    t1 = [[], []]

    def send_first(h, lo, hi):
        for i in range(lo, hi):
            target, block = to_mid(PEERS[i])
            t1[h].append(
                send(zb.at[h, block], dd.at[h, me], s1.at[h, i], q1.at[h, me], target)
            )

    forward_third(0)
    for copy in fetch[3:]:
        copy.wait()
    a0, a1, a2 = anchor[0], anchor[1], anchor[2]
    fa[1:9, 8:40, own] = fs_ref[...]
    fr[1:9, 8:40, own] = fd_ref[...]
    pl.semaphore_wait(barrier, 65)
    halo = []
    for k, oy in enumerate((-1, 1)):
        rows = pl.ds(0, 8) if oy < 0 else pl.ds(24, 8)
        to_rows = pl.ds(40, 8) if oy < 0 else pl.ds(0, 8)
        for part, (src, dst) in enumerate(((fs_ref, fa), (fd_ref, fr))):
            copy = prepare(
                src.at[:, rows, :], dst.at[pl.ds(1, 8), to_rows, own],
                sh1.at[2 * k + part], qh1.at[2 * k + part], beside(0, oy),
            )
            pl.when(has_y[k])(copy.start)
            halo.append((copy, has_y[k], has_y[1 - k]))
    send_first(0, 0, 32)
    forward_third(1)
    send_first(1, 0, CUT1)
    for h in range(2):
        mu = lamr_ref[0:1, :] + jnp.concatenate([lamc_ref[h]] * 4, axis=1)

        def table(i, g, h=h, mu=mu):
            d = 1.0 / (1.0 + (mu + g))
            dtab[h, i] = d
            return (mu + g) * d

        lax.fori_loop(0, 31, table, jnp.ones((8, 512), F32))
        odd = pv % 2 == 1
        muq = jnp.where(odd, lamq_ref[2:4, :], lamq_ref[0:2, :]) + lamc_ref[h, pl.ds(pv // 2, 1), :]
        c = 0.5 * muq
        c1 = c
        r32 = 2.0 * (1.0 + c)
        for _ in range(4):
            c = 2.0 * c * (c + 2.0)
            r32 = r32 * (2.0 * (1.0 + c))
        c = 2.0 * c * (c + 2.0)
        rint[h] = r32
        g = jnp.ones((2, 128), F32)
        for i in range(15):
            d = 1.0 / (1.0 + (2.0 * c + g))
            dint[h, i] = d
            g = (2.0 * c + g) * d
        dint[h, 15] = 1.0 / (r32 * (1.0 + c1) + c + g)
    def cells(rows, cols, first):
        grid = lax.broadcasted_iota(jnp.int32, (rows, cols), 0)
        return jnp.where(grid == first, 1.0, 0.0).astype(BF16)

    lane = lax.broadcasted_iota(jnp.int32, (512, 256), 1)
    pick = cells(512, 256, a1 - 3 + 8 * (lane // 16) + lane % 16)
    myh[...] = mm(sh_ref[...], pick, NN).astype(BF16)
    myl[...] = mm(sl_ref[...], pick, NN).astype(BF16)
    lane = lax.broadcasted_iota(jnp.int32, (512, 128), 1)
    pick = cells(512, 128, a2 - 1 + 30 * core + lane)
    mz[...] = mm(sh_ref[...], pick, NN) + mm(sl_ref[...], pick, NN)
    def weights(cell, first, boxes, low_face, high_face):
        low_w = jnp.where(cell == first, 0.625, 0.0) + jnp.where(cell == first + 1, 0.375, 0.0)
        high_w = jnp.where(cell == first + boxes, 0.375, 0.0) + jnp.where(
            cell == first + boxes + 1, 0.625, 0.0
        )
        return jnp.where(low_face, low_w, 0.0) + jnp.where(high_face, high_w, 0.0)

    row = lax.broadcasted_iota(jnp.int32, (16, 512), 0)
    cell = lax.broadcasted_iota(jnp.int32, (16, 512), 1)
    wy = weights(cell, a1 - 1, 128, row == 0, row == 1).astype(BF16)
    wys[...] = mm(wy, sh_ref[...], NN) + mm(wy, sl_ref[...], NN)
    wz = weights(cell, a2 - 1, 64, row == 0, row == 1).astype(BF16)
    wz = mm(wz, sh_ref[...], NN) + mm(wz, sl_ref[...], NN)
    lane = lax.broadcasted_iota(jnp.int32, (512, 512), 1)
    pick = cells(512, 512, 256 * (lane // 256) + 8 * mid + lane % 8)
    wzh, wzl = split(wz)
    wz = mm(wzh, pick, NN) + mm(wzl, pick, NN)
    row = lax.broadcasted_iota(jnp.int32, (32, 256), 0)
    lane = lax.broadcasted_iota(jnp.int32, (32, 256), 1)
    row2 = lax.broadcasted_iota(jnp.int32, (16, 256), 0)
    lane2 = lax.broadcasted_iota(jnp.int32, (16, 256), 1)
    wx = weights(32 * pv + lane2 // 8, a0 - 1, 32, row2 < 8, row2 >= 8)
    wx = jnp.where(row2 % 8 == lane2 % 8, wx, 0.0)
    for h in range(2):
        for f in range(2):
            wall[h, 32 * f : 32 * f + 32, :] = jnp.where(
                row == lane // 8, wz[f : f + 1, halves[h]], 0.0
            )
        wall[h, 64:80, :] = wx
    for copy, _, comes in halo:
        pl.when(comes)(copy.wait_recv)
    pair = []
    for k, ref in enumerate((fa, fr)):
        view = ref.at[pl.ds(1, 8), :, own]
        copy = pltpu.make_async_remote_copy(
            src_ref=view, dst_ref=view, send_sem=sd.at[k], recv_sem=qd.at[k],
            device_id=partner, device_id_type=MESH,
        )
        copy.start()
        pair.append(copy)
    for copy in pair:
        copy.wait()
    fine_row = lax.broadcasted_iota(jnp.int32, (48, 256), 0) + 32 * gy
    fine_col = lax.broadcasted_iota(jnp.int32, (48, 256), 1)
    inside_y = (fine_row >= 8) & (fine_row < 520)
    sixth = jnp.where(inside_y, 1.0 / 6.0, 0.0)

    def layer(source, extra, k):
        v = source[k]
        total = (source[k - 1] + source[k + 1]) + extra[k]
        total = total + (pltpu.roll(v, 1, 0) + pltpu.roll(v, 47, 0))
        total = total + jnp.where(fine_col == 0, 0.0, pltpu.roll(v, 1, 1))
        return total + jnp.where(fine_col == 255, 0.0, pltpu.roll(v, 255, 1))

    for k in (0, 9):
        fa[k] = jnp.zeros((48, 256), F32)
        fb[k] = jnp.zeros((48, 256), F32)
    for k in range(1, 9):
        fa[k] = jnp.where(inside_y, fa[k], 0.0)
        fr[k] = jnp.where(inside_y, fr[k], 0.0) * (-1.0 / 16.0)
        es[k + 7] = fa[k]

    def alone(j, carry):
        for part, (source, target) in enumerate(((fa, fb), (fb, fa))):
            trace[0, 2 * j + part] = source[1]
            trace[1, 2 * j + part] = source[8]

            def four(k, c):
                for m in range(4):
                    index = 1 + 4 * k + m
                    target[index] = layer(source, fr, index) * sixth
                return c

            lax.fori_loop(0, 2, four, 0)
        return carry

    lax.fori_loop(0, 4, alone, 0)

    t2 = []
    t4 = [[], []]

    def second_and_eliminate(h):
        value = dd[h].reshape(512, 256)
        u[h] = dot3(split(value), s_pair, TN).reshape(32, 8, 512)
        first = -u[h, 0]
        u[h, 0] = first
        q0 = dtab[h, 30]

        def forward(i, carry):
            yv, q, e = carry
            w = u[h, i]
            yv = dtab[h, i - 1] * yv - w
            u[h, i] = yv
            q = q * dtab[h, 30 - i]
            return yv, q, e - q * w

        yv, _, e = lax.fori_loop(1, 31, forward, (first, q0, q0 * first))
        b = q0 * yv - u[h, 31]
        for j in range(4):
            start = 8 * (j // 2) + j % 2 + 4 * h
            m1[pl.ds(start, 8, stride=16), :] = e[:, 128 * j : 128 * j + 128]
            m1[pl.ds(start + 2, 8, stride=16), :] = b[:, 128 * j : 128 * j + 128]

    def send_ends():
        for k in range(1, 16):
            q = (pv + k) % 16
            t2.append(send(
                m1.at[pl.ds(pl.multiple_of(q * 8, 8), 8), :], r1.at[pv], s2.at[k], q2.at[pv],
                to_row(q),
            ))
        r1[pv] = m1[pl.ds(pl.multiple_of(pv * 8, 8), 8), :]

    def separators():
        for h in range(2):
            ys = []
            prev = None
            for p in range(16):
                end = r1[p, 4 * h + 2 : 4 * h + 4, :]
                if p < 15:
                    end = end + r1[p + 1, 4 * h : 4 * h + 2, :]
                end = rint[h] * end
                prev = end if p == 0 else end + dint[h, p - 1] * prev
                ys.append(prev)
            m2[0, 4 * h : 4 * h + 2, :] = jnp.zeros((2, 128), F32)
            sol = dint[h, 15] * ys[15]
            m2[15, 4 * h + 2 : 4 * h + 4, :] = sol
            for p in range(14, -1, -1):
                sol = dint[h, p] * (sol + ys[p])
                m2[p + 1, 4 * h : 4 * h + 2, :] = sol
                m2[p, 4 * h + 2 : 4 * h + 4, :] = sol
        for k in range(1, 16):
            q = (pv + k) % 16
            t2.append(send(
                m2.at[q], r2.at[pl.ds(pl.multiple_of(pv * 8, 8), 8), :], s3.at[k], q3.at[pv],
                to_row(q),
            ))
        r2[pl.ds(pl.multiple_of(pv * 8, 8), 8), :] = m2[pv]

    def wait_separators():
        for k in range(1, 16):
            q = (pv + k) % 16
            view = r2.at[pl.ds(pl.multiple_of(q * 8, 8), 8), :]
            pltpu.make_async_remote_copy(
                src_ref=view, dst_ref=view, send_sem=s3.at[k], recv_sem=q3.at[q],
                device_id=here, device_id_type=MESH,
            ).wait_recv()

    def substitute(h):
        starts = [8 * (j // 2) + j % 2 + 4 * h for j in range(4)]
        left = jnp.concatenate([r2[pl.ds(j, 8, stride=16), :] for j in starts], axis=1)
        right = jnp.concatenate([r2[pl.ds(j + 2, 8, stride=16), :] for j in starts], axis=1)

        def spread(i, t):
            u[h, i] = u[h, i] + t
            return dtab[h, i] * t

        lax.fori_loop(0, 31, spread, left)
        u[h, 31] = right

        def backward(k, v):
            i = 30 - k
            v = dtab[h, i] * (v + u[h, i])
            u[h, i] = v
            return v

        lax.fori_loop(0, 31, backward, right)
        high, low = split(u[h].reshape(256, 512))
        uh[h] = high
        ul[h] = low

    def inverse_second(h):
        for copy in t1[h]:
            copy.wait_send()
        zb[h] = dot3(s_pair, (uh[h], ul[h]), NT).reshape(32, 16, 256)

    def send_last(h, lo, hi):
        for i in range(lo, hi):
            target, block = to_real(PEERS[i])
            t4[h].append(
                send(zb.at[h, block], gg.at[h, mid], s4.at[h, i], q4.at[h, mid], target)
            )

    tt = []

    def send_traces(part):
        sweeps = pl.ds(4 * part, 4)
        for side, ox in enumerate((-1, 1)):
            copy = prepare(
                trace.at[side, sweeps, pl.ds(8, 32), own],
                tin.at[1 - side, sweeps, pl.ds(8, 32), own],
                st.at[side, part], qt.at[1 - side, part], beside(ox, 0),
            )
            pl.when(has_x[side])(copy.start)
            tt.append((copy, has_x[side]))

    def send_corners():
        for side, ox in enumerate((-1, 1)):
            copy = prepare(
                trace.at[side, :, corner, own], tin.at[1 - side, :, corner, own], sx.at[side],
                qx.at[1 - side], beside(ox, 0),
            )
            sent = has_x[side] & middle
            pl.when(sent)(copy.start)
            tt.append((copy, sent))

    for s in range(32):
        arrived(dd.at[0], q1.at[0], s)
    second_and_eliminate(0)
    for s in range(32):
        arrived(dd.at[1], q1.at[1], s)
    second_and_eliminate(1)
    send_ends()
    send_traces(0)
    send_traces(1)
    send_corners()
    for k in range(1, 16):
        arrived(r1, q2, (pv + k) % 16)
    separators()
    wait_separators()
    for part in range(2):
        sweeps = pl.ds(4 * part, 4)
        for side in range(2):
            view = tin.at[side, sweeps, pl.ds(8, 32), own]
            copy = pltpu.make_async_remote_copy(
                src_ref=view, dst_ref=view, send_sem=st.at[side, part],
                recv_sem=qt.at[side, part], device_id=here, device_id_type=MESH,
            )
            pl.when(has_x[side])(copy.wait_recv)
    for side in range(2):
        copy = prepare(
            tin.at[side, :, corner, own], tin.at[side, :, corner, own], sx.at[side], qx.at[side],
            here,
        )
        pl.when(has_x[side] & middle)(copy.wait_recv)

        @pl.when(jnp.logical_not(has_x[side]))
        def _():
            tin[side, :, 8:40, own] = jnp.zeros((8, 32, 128), F32)

        @pl.when(jnp.logical_not(has_x[side]) & middle)
        def _():
            tin[side, :, corner, own] = jnp.zeros((8, 8, 128), F32)

        @pl.when(jnp.logical_not(has_y[side]))
        def _():
            tin[:, :, 40 * side : 40 * side + 8, own] = jnp.zeros((2, 8, 8, 128), F32)

    for k, oy in enumerate((-1, 1)):
        rows = pl.ds(8, 8) if oy < 0 else pl.ds(32, 8)
        to_rows = pl.ds(40, 8) if oy < 0 else pl.ds(0, 8)
        copy = prepare(
            tin.at[:, :, rows, own], tin.at[:, :, to_rows, own], sv.at[k], qv.at[k], beside(0, oy)
        )
        pl.when(turns[k])(copy.start)
        tt.append((copy, turns[k]))
    substitute(0)
    inverse_second(0)
    send_last(0, 0, CUT4A)
    substitute(1)
    face = []
    cut_x = []

    def faces(h):
        pair_h = (uh[h], ul[h])
        rows = dot3(split(wall[h]), pair_h, NN)
        face.append(rows[:64])
        cut_x.append(rows[64:])
        line = dot3(split(wys[...]), pair_h, NT)
        for f in range(2):
            for t in range(2):
                my[f, 2 * h + t : 2 * h + t + 1, :] = line[f : f + 1, 128 * t : 128 * t + 128]

    faces(0)
    faces(1)
    rows = jnp.concatenate([face[0] + face[1], cut_x[0], cut_x[1]], axis=0)
    rows = dot3(split(rows), (myh[...], myl[...]), NN)
    lane = lax.broadcasted_iota(jnp.int32, (8, 128), 1) // 16
    for f in range(2):
        for t in range(2):
            cols = slice(128 * t, 128 * t + 128)
            v = [rows[32 * f + 8 * k : 32 * f + 8 * k + 8, cols] for k in range(4)]
            for g in range(2):
                for h in range(2):
                    start = 64 + 16 * h + 8 * g
                    v.append(rows[start : start + 8, cols])
            for q, w in enumerate(exchange8(v, lane)):
                mzx[16 * f + 8 * t + q] = w
    tz = []
    for i, o in enumerate(PEERS):
        target, block = to_real(o)
        tz.append(send(mzx.at[block], rzx.at[mid], sz.at[i], qz.at[mid], target))
    for f in range(2):
        for g in range(2):
            tz.append(send(
                my.at[f], ry.at[mid], sy.at[2 * f + g], qy.at[mid],
                device(g, x, 7 * f, lv + 4 * f),
            ))
    send_last(0, CUT4A, 32)
    inverse_second(1)
    send_last(1, 0, CUT4B)
    for k in range(2):
        view = tin.at[:, :, pl.ds(40 - 40 * k, 8), own]
        copy = pltpu.make_async_remote_copy(
            src_ref=view, dst_ref=view, send_sem=sv.at[k], recv_sem=qv.at[k], device_id=here,
            device_id_type=MESH,
        )
        pl.when(turns[1 - k])(copy.wait_recv)
    view = tin.at[:, :, :, own]
    te = send(view, view, se.at[0], qe.at[0], partner)
    te.wait_recv()
    def factor(k):
        inside_x = (k + 8 * gx >= 8) & (k + 8 * gx < 136)
        return jnp.where(inside_x, sixth, 0.0)

    ends = (jnp.where(gx == 0, 0.0, sixth), jnp.where(gx == 15, 0.0, sixth))
    for k in (4, 5, 6, 7, 16, 17, 18, 19):
        es[k] = jnp.zeros((48, 256), F32)
        ed[k] = jnp.zeros((48, 256), F32)
    for k in (3, 4, 5, 6, 17, 18, 19, 20):
        et[k] = jnp.zeros((48, 256), F32)
    for k in range(8, 16):
        ed[k] = fr[k - 7]
    for j in range(8):
        source, target = ((es, et), (et, es))[j % 2]
        depth = min(j + 1, 7 - j)

        def some(k, c, source=source, target=target, first=8 - depth, step=WIDE):
            for m in range(step):
                index = first + step * k + m
                target[index] = layer(source, ed, index) * factor(index)
            return c

        layers = 8 + 2 * depth
        lax.fori_loop(0, layers // WIDE, some, 0)
        if layers % WIDE:
            some(0, 0, first=8 - depth + layers // WIDE * WIDE, step=layers % WIDE)
        target[8] = target[8] + tin[0, j] * ends[0]
        target[15] = target[15] + tin[1, j] * ends[1]
    for s in range(32):
        arrived(rzx, qz, s)
    zsum = rzx[0]
    for s in range(1, 32):
        zsum = zsum + rzx[s]
    row = lax.broadcasted_iota(jnp.int32, (128, 512), 0)
    col = lax.broadcasted_iota(jnp.int32, (128, 512), 1)
    tile = jnp.where(row == col // 128 * 16 + col % 16, 1.0, 0.0)
    spread_z = full(zsum, tile, NN)
    spread_z = jnp.concatenate([spread_z[:, 128 * h : 128 * h + 128] for h in range(4)], axis=0)
    lane32 = lax.broadcasted_iota(jnp.int32, (32, 128), 1) // 16
    spread_z = jnp.concatenate(
        [jnp.where(lane32 == k, spread_z, 0.0) for k in range(8)], axis=0
    )
    row = lax.broadcasted_iota(jnp.int32, (16, 256), 0)
    col = lax.broadcasted_iota(jnp.int32, (16, 256), 1)
    pick = jnp.where(a0 - 3 + 2 * row + col // 32 == 32 * gx + col % 32, 1.0, 0.0)
    rows = full(pick, spread_z, NN)
    for q in range(16):
        m5[q] = rows[q : q + 1]
    t5 = []
    for k in range(1, 16):
        q = (gx + k) % 16
        t5.append(send(m5.at[q], r5.at[gx], s5.at[k], q5.at[gx], real_row(q)))
    r5[gx] = m5[gx]
    got = rzx[...].reshape(256, 128)
    parts = [full(got, mz[256 * k : 256 * k + 256, :], TN) for k in range(2)]
    left_half = lax.broadcasted_iota(jnp.int32, (8, 128), 1) < 64
    for f in range(2):
        cells_x = parts[0][64 + 32 * f : 80 + 32 * f] + parts[1][80 + 32 * f : 96 + 32 * f]
        m6[f] = jnp.where(left_half, cells_x[:8], pltpu.roll(cells_x[8:], 64, 1))
    for f in range(2):
        end = 15 * f
        copy = prepare(m6.at[f], r6.at[gx], s6.at[f], q6.at[gx], real_row(end))
        pl.when(gx != end)(copy.start)

        @pl.when(gx == end)
        def _():
            r6[gx] = m6[f]

    at_y = (gy == 0) | (gy == 15)

    @pl.when(at_y)
    def _():
        for s in range(32):
            arrived(ry, qy, s)
        lane8 = lax.broadcasted_iota(jnp.int32, (32, 128), 1) % 8
        group = lax.broadcasted_iota(jnp.int32, (16, 128), 0)
        member = lax.broadcasted_iota(jnp.int32, (16, 128), 1) // 8
        gather = jnp.where(group == member, 1.0, 0.0)
        part = []
        for t in range(2):
            total = None
            for h in range(2):
                v = ry[:, 2 * h + t, :]
                v = jnp.concatenate([jnp.where(lane8 == k, v, 0.0) for k in range(8)], axis=0)
                modes = jnp.concatenate(
                    [mz[pl.ds(256 * h + k, 32, stride=8), :] for k in range(8)], axis=0
                )
                w = full(v, modes, TN)
                total = w if total is None else total + w
            part.append(full(gather, total, NN))
        row = lax.broadcasted_iota(jnp.int32, (128, 32), 0)
        col = lax.broadcasted_iota(jnp.int32, (128, 32), 1)
        pick = jnp.where(a0 - 3 + 2 * (row // 8) + row % 8 == 32 * gx + col, 1.0, 0.0)
        m7[...] = full(pick, jnp.concatenate(part, axis=0), NN).reshape(16, 8, 128)
        for k in range(1, 16):
            q = (gx + k) % 16
            send(m7.at[q], r7.at[gx], s7.at[k], q7.at[gx], real_row(q))
        r7[gx] = m7[gx]

    send_last(1, CUT4B, 32)
    for s in range(32):
        arrived(gg.at[0], q4.at[0], s)
    def inverse_third(h):
        swap_groups(gg.at[h], za, 0, 256 * h)
        rows_h = tuple(part[halves[h], :] for part in s_pair)
        return dot3(split(za[:, :, halves[h]].reshape(512, 256)), rows_h, NN).reshape(32, 16, 512)

    out_ref[...] = inverse_third(0)
    for k in range(1, 16):
        arrived(r5, q5, (gx + k) % 16)
    def interpolate(fine, cell):
        scaled = 2 * fine + 5
        bottom = scaled // 8
        t = (scaled % 8).astype(F32) * 0.125
        return jnp.where(cell == bottom, 1.0 - t, 0.0) + jnp.where(cell == bottom + 1, t, 0.0)

    def grid(shape):
        return (lax.broadcasted_iota(jnp.int32, shape, 0), lax.broadcasted_iota(jnp.int32, shape, 1))

    row, col = grid((24, 8))
    int_x = interpolate(row, col)
    row, col = grid((128, 128))
    int_y = jnp.where(row < 48, interpolate(row, col % 16), 0.0)
    zb5 = r5[0]
    for s in range(1, 16):
        zb5 = zb5 + r5[s]
    row, col = grid((8, 128))
    zb5 = jnp.where(row == col // 16, jnp.broadcast_to(zb5, (8, 128)), 0.0)
    ghost_z = full(full(int_x, zb5, NN), int_y, NT)
    row, col = grid((24, 128))
    inside = (row + 8 * gx >= 8) & (row + 8 * gx < 136) & (col < 48)
    inside = inside & (col + 32 * gy >= 8) & (col + 32 * gy < 520)
    sixth_z = jnp.where(inside, 1.0 / 6.0, 0.0)
    plane = []
    for j in range(8):
        new = []
        for k in range(j + 1):
            total = ghost_z if k == 0 else plane[k - 1]
            if k + 1 < j:
                total = total + plane[k + 1]
            if k < j:
                v = plane[k]
                total = total + (pltpu.roll(v, 1, 0) + pltpu.roll(v, 23, 0))
                total = total + (pltpu.roll(v, 1, 1) + pltpu.roll(v, 127, 1))
            new.append(total * sixth_z)
        plane = new
    for k in range(8):
        gz[pl.ds(k, 24, stride=8), :] = plane[k]
    row, col = grid((8, 128))
    place = jnp.where(col == jnp.where(core == 0, row, 127 - row), 1.0, 0.0)
    for k in range(8):
        part = full(gz[8 * (k + 8) : 8 * (k + 8) + 8, :], place, TN)
        fine_ref[k] = es[k + 8, 8:40, own] + part[8:40]

    row, col = grid((128, 256))
    int_z = jnp.where(row < 64, interpolate(col, row + 30 * core), 0.0)

    for copy in t2 + t4[0] + t4[1] + tz + t5 + [te]:
        copy.wait_send()
    for copy, sent, *_ in halo + tt:
        pl.when(sent)(copy.wait_send)
    @pl.when(at_y)
    def _():
        for k in range(1, 16):
            prepare(m7.at[k], r7.at[gx], s7.at[k], q7.at[gx], here).wait_send()

    for f in range(2):
        @pl.when(gx != 15 * f)
        def _():
            pltpu.make_async_remote_copy(
                src_ref=m6.at[f], dst_ref=r6.at[gx], send_sem=s6.at[f], recv_sem=q6.at[gx],
                device_id=real_row(15 * f), device_id_type=MESH,
            ).wait_send()

    for s in range(32):
        arrived(gg.at[1], q4.at[1], s)
    out_ref[...] = out_ref[...] + inverse_third(1)
    row8 = lax.broadcasted_iota(jnp.int32, (8, 256), 0)
    col8 = lax.broadcasted_iota(jnp.int32, (8, 256), 1)
    for f in range(2):
        @pl.when(gy == 15 * f)
        def _():
            for k in range(1, 16):
                arrived(r7, q7, (gx + k) % 16)
            yb7 = r7[0]
            for k in range(1, 16):
                yb7 = yb7 + r7[k]
            ghost_y = full(full(int_x, yb7, NN), int_z, NN)
            edge = 7 * f
            for k in range(24):
                yd[k] = jnp.where(row8 == edge, ghost_y[k : k + 1], 0.0)
            for j in range(8):
                source, target = ((ya, yb), (yb, ya))[j % 2]

                def one(k, c, source=source, target=target, j=j):
                    total = yd[k]
                    if j:
                        v = source[k]
                        total = total + source[k - 1] + source[k + 1]
                        total = total + jnp.where(row8 == 0, 0.0, pltpu.roll(v, 1, 0))
                        total = total + jnp.where(row8 == 7, 0.0, pltpu.roll(v, 7, 0))
                        total = total + jnp.where(col8 == 0, 0.0, pltpu.roll(v, 1, 1))
                        total = total + jnp.where(col8 == 255, 0.0, pltpu.roll(v, 255, 1))
                    inside_x = (k + 8 * gx >= 8) & (k + 8 * gx < 136)
                    target[k] = total * jnp.where(inside_x, 1.0 / 6.0, 0.0)
                    return c

                for k in range(j + 1, 23 - j):
                    one(k, 0)
            rows = pl.ds(24 * f, 8)
            for k in range(8):
                fine_ref[k, rows, :] = fine_ref[k, rows, :] + ya[k + 8, :, own]

    for f in range(2):
        @pl.when(gx == 15 * f)
        def _():
            for k in range(16):
                if k != 15 * f:
                    arrived(r6, q6, k)
            xb6 = r6[0]
            for s in range(1, 16):
                xb6 = xb6 + r6[s]
            row, col = grid((48, 8))
            near_y = full(interpolate(row, col), xb6, NN)
            far_y = full(interpolate(row, col + 8), xb6, NN)
            row, col = grid((48, 128))
            ghost_x = full(jnp.where(col < 64, near_y + pltpu.roll(far_y, 64, 1), 0.0), int_z, NN)
            for k in range(1, 9):
                fr[k] = jnp.zeros((48, 256), F32)
                fa[k] = jnp.zeros((48, 256), F32)
                fb[k] = jnp.zeros((48, 256), F32)
            fr[1 + 7 * f] = ghost_x
            for j in range(8):
                source, target = ((fa, fb), (fb, fa))[j % 2]
                for k in range(j + 1):
                    index = 8 - k if f else 1 + k
                    target[index] = layer(source, fr, index) * sixth
            for k in range(8):
                fine_ref[k] = fine_ref[k] + fa[k + 1, 8:40, own]


def body(density, fine_density, fine_start, anchor):
    high, low, lam = tables()
    vm = pl.BlockSpec(memory_space=pltpu.VMEM)
    dma = pltpu.SemaphoreType.DMA

    def f32(*shape):
        return pltpu.VMEM(shape, F32)

    def b16(*shape):
        return pltpu.VMEM(shape, BF16)

    big = f32(32, 16, 512)
    return pl.pallas_call(
        kernel,
        out_shape=(
            pltpu.VMEM((32, 16, 512), F32), pltpu.VMEM((8, 32, 128), F32)
        ),
        in_specs=[pl.BlockSpec(memory_space=pl.ANY)] * 9,
        out_specs=(vm, vm),
        scratch_shapes=[
            pltpu.SMEM((3,), jnp.int32), f32(8, 512), f32(2, 8, 128), f32(8, 128),
            big, f32(8, 32, 128), f32(8, 32, 128), b16(512, 512), b16(512, 512),
            big, f32(2, 32, 16, 256), f32(2, 32, 16, 256), f32(2, 32, 16, 256),
            f32(2, 32, 8, 512), f32(2, 31, 8, 512),
            f32(128, 128), f32(16, 8, 128), f32(16, 8, 128), f32(128, 128),
            f32(2, 16, 2, 128), f32(2, 2, 128),
            b16(2, 256, 512), b16(2, 256, 512), b16(512, 256), b16(512, 256),
            f32(512, 128), f32(2, 80, 256), f32(16, 512),
            f32(32, 8, 128), f32(32, 8, 128), f32(2, 4, 128), f32(32, 4, 128),
            f32(16, 1, 128), f32(16, 1, 128), f32(2, 8, 128), f32(16, 8, 128),
            f32(16, 8, 128), f32(16, 8, 128),
            f32(24, 48, 256), f32(24, 48, 256), f32(24, 48, 256),
            f32(10, 48, 256), f32(10, 48, 256), f32(10, 48, 256),
            f32(2, 8, 48, 256), f32(2, 8, 48, 256), f32(192, 128),
            f32(24, 8, 256), f32(24, 8, 256), f32(24, 8, 256),
            dma((2, 32)), dma((2, 32)), dma((16,)), dma((16,)), dma((16,)), dma((16,)),
            dma((2, 32)), dma((2, 32)), dma((4,)), dma((4,)), dma((2,)), dma((2,)),
            dma((32,)), dma((32,)), dma((4,)), dma((32,)), dma((16,)), dma((16,)),
            dma((2,)), dma((16,)), dma((10,)), dma((2, 2)), dma((2, 2)), dma((1,)), dma((1,)), dma((2,)), dma((2,)),
            dma((2,)), dma((2,)), dma((16,)), dma((16,)),
        ],
        compiler_params=pltpu.CompilerParams(
            collective_id=0, has_side_effects=True, vmem_limit_bytes=56 << 20
        ),
    )(anchor, jnp.asarray(np.tile(lam.reshape(1, 512), (8, 1))),
      jnp.asarray(np.tile(lam.reshape(512, 1), (1, 128))),
      jnp.asarray(np.tile(lam.reshape(4, 128), (2, 1))), density, fine_density, fine_start,
      jnp.asarray(high), jnp.asarray(low))


def solution(mesh):
    return jax.shard_map(
        body,
        mesh=mesh,
        in_specs=(P("gx", ("grp", "gy"), None), P("gx", "gy", "grp"), P("gx", "gy", "grp"), P()),
        out_specs=(P("gx", ("grp", "gy"), None), P("gx", "gy", "grp")),
        check_vma=False,
    )
```

```python
import functools
import math

import jax
import jax.numpy as jnp
import numpy as np
from jax import lax
from jax.experimental import pallas as pl
from jax.experimental.pallas import tpu as pltpu
from jax.sharding import PartitionSpec as P

MESH = pl.DeviceIdType.MESH
NC = 512
F32 = jnp.float32
CUT1, CUT4A, CUT4B = 32, 16, 32
WIDE = 4
BF16 = jnp.bfloat16


def tables():
    index = np.arange(1, NC + 1, dtype=np.int64)
    angle = (index[:, None] * index[None, :]) % (2 * (NC + 1))
    sine = math.sqrt(2.0 / (NC + 1)) * np.sin(angle * (math.pi / (NC + 1)))
    sine = sine.astype(np.float32)
    high = sine.astype(jnp.bfloat16)
    low = (sine - high.astype(np.float32)).astype(jnp.bfloat16)
    lam = 4.0 * np.sin(index * (math.pi / (2 * (NC + 1)))) ** 2
    return high, low, lam.astype(np.float32)


def split(value):
    high = value.astype(BF16)
    low = (value - high.astype(F32)).astype(BF16)
    return high, low


def dot3(a, b, dims):
    ah, al = a
    bh, bl = b
    dd = functools.partial(
        lax.dot_general, dimension_numbers=(dims, ((), ())), preferred_element_type=F32
    )
    return dd(ah, bh) + (dd(al, bh) + dd(ah, bl))


def mm(a, b, dims):
    return lax.dot_general(a, b, (dims, ((), ())), preferred_element_type=F32)


def full(a, b, dims):
    return lax.dot_general(
        a, b, (dims, ((), ())), precision=lax.Precision.HIGHEST, preferred_element_type=F32
    )


NN = ((1,), (0,))
NT = ((1,), (1,))
TN = ((0,), (0,))


def exchange(v, lane):
    v = list(v)
    for bit in (1, 2, 4, 8):
        upper = (lane & bit) != 0
        for i in range(16):
            if i & bit:
                continue
            a, c = v[i], v[i | bit]
            v[i] = jnp.where(upper, pltpu.roll(c, 8 * bit, 1), a)
            v[i | bit] = jnp.where(upper, c, pltpu.roll(a, 128 - 8 * bit, 1))
    return v


def exchange8(v, lane):
    v = list(v)
    for bit in (1, 2, 4):
        upper = (lane & bit) != 0
        for i in range(8):
            if i & bit:
                continue
            a, c = v[i], v[i | bit]
            v[i] = jnp.where(upper, pltpu.roll(c, 16 * bit, 1), a)
            v[i | bit] = jnp.where(upper, c, pltpu.roll(a, 128 - 16 * bit, 1))
    return v


def swap_groups(source, target, first, out_first):
    lane = lax.broadcasted_iota(jnp.int32, (8, 128), 1) // 8
    for a in range(2):
        for b in range(2):
            cols = slice(first + 128 * b, first + 128 * b + 128)
            outs = slice(out_first + 128 * a, out_first + 128 * a + 128)
            for row in (0, 8):
                v = [source[16 * a + q, row : row + 8, cols] for q in range(16)]
                for q, w in enumerate(exchange(v, lane)):
                    target[16 * b + q, row : row + 8, outs] = w


def device(core, x, y, z):
    return (core, x * 4 + z % 4, (z // 4) * 8 + y)


ORDER = [
    (dy, side, core) for dy in (4, 3, 5, 2, 6, 1, 7, 0) for side in (0, 1) for core in (0, 1)
]
PEERS = [ORDER[i] for i in np.random.RandomState(3).permutation(32)]
SIDES = [[o for o in PEERS if o[1] == side] for side in (0, 1)]
PEERS = [o for both in zip(*SIDES) for o in both]


def kernel(
    anchor_hbm, lamr_hbm, lamc_hbm, lamq_hbm, x_hbm, fd_hbm, fs_hbm, sh_hbm, sl_hbm, out_ref, fine_ref,
    anchor, lamr_ref, lamc_ref, lamq_ref, x_ref, fd_ref, fs_ref, sh_ref, sl_ref,
    za, zb, dd, gg, u, dtab, m1, r1, m2, r2, dint, rint, uh, ul, myh, myl, mz, wall, wys,
    mzx, rzx, my, ry, m5, r5, m6, r6, m7, r7, es, et, ed, fa, fb, fr, trace, tin, gz, ya, yb, yd,
    s1, q1, s2, q2, s3, q3, s4, q4, sh1, qh1, sd, qd, sz, qz, sy, qy, s5, q5, s6, q6, sin,
    st, qt, se, qe, sv, qv, sx, qx, s7, q7,
):
    core = lax.axis_index("grp")
    gx = lax.axis_index("gx")
    gy = lax.axis_index("gy")
    x, zl = gx // 4, gx % 4
    y, zh = gy % 8, gy // 8
    z = zh * 4 + zl
    me = core * 16 + gy
    zv = (z + 6) % 8
    lv, hv = zv % 4, zv // 4
    mid = core * 16 + hv * 8 + y
    pv = x * 4 + lv

    def to_mid(o):
        dy, side, oc = o
        ty = (y + dy + core * (8 - 2 * dy)) % 8
        tc = (core + oc) % 2
        return device(tc, x, ty, (zl + 4 * side + 2) % 8), tc * 16 + side * 8 + ty

    def to_real(o):
        dy, side, oc = o
        ty = (y + dy + core * (8 - 2 * dy)) % 8
        tc = (core + oc) % 2
        return device(tc, x, ty, lv + 4 * side), tc * 16 + side * 8 + ty

    def to_row(q):
        return device(core, q // 4, y, (q % 4 + 4 * hv + 2) % 8)

    def real_row(q):
        return device(core, q // 4, y, q % 4 + 4 * zh)

    here = (core, gx, gy)
    partner = (1 - core, gx, gy)
    own = pl.ds(pl.multiple_of(core * 128, 128), 128)

    def beside(ox, oy):
        return (core, (gx + ox + 16) % 16, (gy + oy + 16) % 16)

    fetch = []
    mine = [pl.ds(pl.multiple_of(256 * h + 8 * mid, 8), 8) for h in range(2)]
    for k, (src, dst) in enumerate((
        (x_hbm, x_ref), (sh_hbm, sh_ref), (sl_hbm, sl_ref), (fd_hbm, fd_ref), (fs_hbm, fs_ref),
        (lamr_hbm, lamr_ref), (lamq_hbm, lamq_ref), (lamc_hbm.at[mine[0], :], lamc_ref.at[0]),
        (lamc_hbm.at[mine[1], :], lamc_ref.at[1]), (anchor_hbm, anchor),
    )):
        copy = pltpu.make_async_copy(src, dst, sin.at[k])
        copy.start()
        fetch.append(copy)
    barrier = pltpu.get_barrier_semaphore()
    for o in PEERS:
        pl.semaphore_signal(barrier, inc=1, device_id=to_mid(o)[0], device_id_type=MESH)
    pl.semaphore_signal(barrier, inc=1, device_id=partner, device_id_type=MESH)
    for oy in (-1, 1):
        pl.semaphore_signal(barrier, inc=1, device_id=beside(0, oy), device_id_type=MESH)
    for k in range(1, 16):
        pl.semaphore_signal(barrier, inc=1, device_id=to_row((pv + k) % 16), device_id_type=MESH)
        pl.semaphore_signal(barrier, inc=1, device_id=real_row((gx + k) % 16), device_id_type=MESH)

    def arrived(ref, sem, index):
        pltpu.make_async_remote_copy(
            src_ref=ref.at[index], dst_ref=ref.at[index], send_sem=sem.at[index],
            recv_sem=sem.at[index], device_id=here, device_id_type=MESH,
        ).wait_recv()

    has_y = (gy > 0, gy < 15)
    has_x = (gx > 0, gx < 15)
    middle = (gy == 7) | (gy == 8)
    turns = ((gy > 0) & (gy != 8), (gy < 15) & (gy != 7))
    corner = pl.ds(pl.multiple_of((15 - gy) // 8 * 40, 8), 8)

    def prepare(src, dst, send_sem, recv_sem, target):
        return pltpu.make_async_remote_copy(
            src_ref=src, dst_ref=dst, send_sem=send_sem, recv_sem=recv_sem,
            device_id=target, device_id_type=MESH,
        )

    def send(*args):
        copy = prepare(*args)
        copy.start()
        return copy

    for copy in fetch[:3]:
        copy.wait()
    s_pair = (sh_ref[...], sl_ref[...])
    x_pair = split(x_ref[...].reshape(512, 512))
    halves = [slice(0, 256), slice(256, 512)]

    def forward_third(h):
        cols = tuple(part[:, halves[h]] for part in s_pair)
        za[:, :, halves[h]] = dot3(x_pair, cols, NN).reshape(32, 16, 256)
        swap_groups(za, zb.at[h], 256 * h, 0)

    t1 = [[], []]

    def send_first(h, lo, hi):
        for i in range(lo, hi):
            target, block = to_mid(PEERS[i])
            t1[h].append(
                send(zb.at[h, block], dd.at[h, me], s1.at[h, i], q1.at[h, me], target)
            )

    forward_third(0)
    for copy in fetch[3:]:
        copy.wait()
    a0, a1, a2 = anchor[0], anchor[1], anchor[2]
    fa[1:9, 8:40, own] = fs_ref[...]
    fr[1:9, 8:40, own] = fd_ref[...]
    pl.semaphore_wait(barrier, 65)
    halo = []
    for k, oy in enumerate((-1, 1)):
        rows = pl.ds(0, 8) if oy < 0 else pl.ds(24, 8)
        to_rows = pl.ds(40, 8) if oy < 0 else pl.ds(0, 8)
        for part, (src, dst) in enumerate(((fs_ref, fa), (fd_ref, fr))):
            copy = prepare(
                src.at[:, rows, :], dst.at[pl.ds(1, 8), to_rows, own],
                sh1.at[2 * k + part], qh1.at[2 * k + part], beside(0, oy),
            )
            pl.when(has_y[k])(copy.start)
            halo.append((copy, has_y[k], has_y[1 - k]))
    send_first(0, 0, 32)
    forward_third(1)
    send_first(1, 0, CUT1)
    for h in range(2):
        mu = lamr_ref[0:1, :] + jnp.concatenate([lamc_ref[h]] * 4, axis=1)

        def table(i, g, h=h, mu=mu):
            d = 1.0 / (1.0 + (mu + g))
            dtab[h, i] = d
            return (mu + g) * d

        lax.fori_loop(0, 31, table, jnp.ones((8, 512), F32))
        odd = pv % 2 == 1
        muq = jnp.where(odd, lamq_ref[2:4, :], lamq_ref[0:2, :]) + lamc_ref[h, pl.ds(pv // 2, 1), :]
        c = 0.5 * muq
        c1 = c
        r32 = 2.0 * (1.0 + c)
        for _ in range(4):
            c = 2.0 * c * (c + 2.0)
            r32 = r32 * (2.0 * (1.0 + c))
        c = 2.0 * c * (c + 2.0)
        rint[h] = r32
        g = jnp.ones((2, 128), F32)
        for i in range(15):
            d = 1.0 / (1.0 + (2.0 * c + g))
            dint[h, i] = d
            g = (2.0 * c + g) * d
        dint[h, 15] = 1.0 / (r32 * (1.0 + c1) + c + g)
    def cells(rows, cols, first):
        grid = lax.broadcasted_iota(jnp.int32, (rows, cols), 0)
        return jnp.where(grid == first, 1.0, 0.0).astype(BF16)

    lane = lax.broadcasted_iota(jnp.int32, (512, 256), 1)
    pick = cells(512, 256, a1 - 3 + 8 * (lane // 16) + lane % 16)
    myh[...] = mm(sh_ref[...], pick, NN).astype(BF16)
    myl[...] = mm(sl_ref[...], pick, NN).astype(BF16)
    lane = lax.broadcasted_iota(jnp.int32, (512, 128), 1)
    pick = cells(512, 128, a2 - 1 + 30 * core + lane)
    mz[...] = mm(sh_ref[...], pick, NN) + mm(sl_ref[...], pick, NN)
    def weights(cell, first, boxes, low_face, high_face):
        low_w = jnp.where(cell == first, 0.625, 0.0) + jnp.where(cell == first + 1, 0.375, 0.0)
        high_w = jnp.where(cell == first + boxes, 0.375, 0.0) + jnp.where(
            cell == first + boxes + 1, 0.625, 0.0
        )
        return jnp.where(low_face, low_w, 0.0) + jnp.where(high_face, high_w, 0.0)

    row = lax.broadcasted_iota(jnp.int32, (16, 512), 0)
    cell = lax.broadcasted_iota(jnp.int32, (16, 512), 1)
    wy = weights(cell, a1 - 1, 128, row == 0, row == 1).astype(BF16)
    wys[...] = mm(wy, sh_ref[...], NN) + mm(wy, sl_ref[...], NN)
    wz = weights(cell, a2 - 1, 64, row == 0, row == 1).astype(BF16)
    wz = mm(wz, sh_ref[...], NN) + mm(wz, sl_ref[...], NN)
    lane = lax.broadcasted_iota(jnp.int32, (512, 512), 1)
    pick = cells(512, 512, 256 * (lane // 256) + 8 * mid + lane % 8)
    wzh, wzl = split(wz)
    wz = mm(wzh, pick, NN) + mm(wzl, pick, NN)
    row = lax.broadcasted_iota(jnp.int32, (32, 256), 0)
    lane = lax.broadcasted_iota(jnp.int32, (32, 256), 1)
    row2 = lax.broadcasted_iota(jnp.int32, (16, 256), 0)
    lane2 = lax.broadcasted_iota(jnp.int32, (16, 256), 1)
    wx = weights(32 * pv + lane2 // 8, a0 - 1, 32, row2 < 8, row2 >= 8)
    wx = jnp.where(row2 % 8 == lane2 % 8, wx, 0.0)
    for h in range(2):
        for f in range(2):
            wall[h, 32 * f : 32 * f + 32, :] = jnp.where(
                row == lane // 8, wz[f : f + 1, halves[h]], 0.0
            )
        wall[h, 64:80, :] = wx
    for copy, _, comes in halo:
        pl.when(comes)(copy.wait_recv)
    pair = []
    for k, ref in enumerate((fa, fr)):
        view = ref.at[pl.ds(1, 8), :, own]
        copy = pltpu.make_async_remote_copy(
            src_ref=view, dst_ref=view, send_sem=sd.at[k], recv_sem=qd.at[k],
            device_id=partner, device_id_type=MESH,
        )
        copy.start()
        pair.append(copy)
    for copy in pair:
        copy.wait()
    fine_row = lax.broadcasted_iota(jnp.int32, (48, 256), 0) + 32 * gy
    fine_col = lax.broadcasted_iota(jnp.int32, (48, 256), 1)
    inside_y = (fine_row >= 8) & (fine_row < 520)
    sixth = jnp.where(inside_y, 1.0 / 6.0, 0.0)

    def layer(source, extra, k):
        v = source[k]
        total = (source[k - 1] + source[k + 1]) + extra[k]
        total = total + (pltpu.roll(v, 1, 0) + pltpu.roll(v, 47, 0))
        total = total + jnp.where(fine_col == 0, 0.0, pltpu.roll(v, 1, 1))
        return total + jnp.where(fine_col == 255, 0.0, pltpu.roll(v, 255, 1))

    for k in (0, 9):
        fa[k] = jnp.zeros((48, 256), F32)
        fb[k] = jnp.zeros((48, 256), F32)
    for k in range(1, 9):
        fa[k] = jnp.where(inside_y, fa[k], 0.0)
        fr[k] = jnp.where(inside_y, fr[k], 0.0) * (-1.0 / 16.0)
        es[k + 7] = fa[k]

    def alone(j, carry):
        for part, (source, target) in enumerate(((fa, fb), (fb, fa))):
            trace[0, 2 * j + part] = source[1]
            trace[1, 2 * j + part] = source[8]

            def four(k, c):
                for m in range(4):
                    index = 1 + 4 * k + m
                    target[index] = layer(source, fr, index) * sixth
                return c

            lax.fori_loop(0, 2, four, 0)
        return carry

    lax.fori_loop(0, 4, alone, 0)

    t2 = []
    t4 = [[], []]

    def second_and_eliminate(h):
        value = dd[h].reshape(512, 256)
        u[h] = dot3(split(value), s_pair, TN).reshape(32, 8, 512)
        first = -u[h, 0]
        u[h, 0] = first
        q0 = dtab[h, 30]

        def forward(i, carry):
            yv, q, e = carry
            w = u[h, i]
            yv = dtab[h, i - 1] * yv - w
            u[h, i] = yv
            q = q * dtab[h, 30 - i]
            return yv, q, e - q * w

        yv, _, e = lax.fori_loop(1, 31, forward, (first, q0, q0 * first))
        b = q0 * yv - u[h, 31]
        for j in range(4):
            start = 8 * (j // 2) + j % 2 + 4 * h
            m1[pl.ds(start, 8, stride=16), :] = e[:, 128 * j : 128 * j + 128]
            m1[pl.ds(start + 2, 8, stride=16), :] = b[:, 128 * j : 128 * j + 128]

    def send_ends():
        for k in range(1, 16):
            q = (pv + k) % 16
            t2.append(send(
                m1.at[pl.ds(pl.multiple_of(q * 8, 8), 8), :], r1.at[pv], s2.at[k], q2.at[pv],
                to_row(q),
            ))
        r1[pv] = m1[pl.ds(pl.multiple_of(pv * 8, 8), 8), :]

    def separators():
        for h in range(2):
            ys = []
            prev = None
            for p in range(16):
                end = r1[p, 4 * h + 2 : 4 * h + 4, :]
                if p < 15:
                    end = end + r1[p + 1, 4 * h : 4 * h + 2, :]
                end = rint[h] * end
                prev = end if p == 0 else end + dint[h, p - 1] * prev
                ys.append(prev)
            m2[0, 4 * h : 4 * h + 2, :] = jnp.zeros((2, 128), F32)
            sol = dint[h, 15] * ys[15]
            m2[15, 4 * h + 2 : 4 * h + 4, :] = sol
            for p in range(14, -1, -1):
                sol = dint[h, p] * (sol + ys[p])
                m2[p + 1, 4 * h : 4 * h + 2, :] = sol
                m2[p, 4 * h + 2 : 4 * h + 4, :] = sol
        for k in range(1, 16):
            q = (pv + k) % 16
            t2.append(send(
                m2.at[q], r2.at[pl.ds(pl.multiple_of(pv * 8, 8), 8), :], s3.at[k], q3.at[pv],
                to_row(q),
            ))
        r2[pl.ds(pl.multiple_of(pv * 8, 8), 8), :] = m2[pv]

    def wait_separators():
        for k in range(1, 16):
            q = (pv + k) % 16
            view = r2.at[pl.ds(pl.multiple_of(q * 8, 8), 8), :]
            pltpu.make_async_remote_copy(
                src_ref=view, dst_ref=view, send_sem=s3.at[k], recv_sem=q3.at[q],
                device_id=here, device_id_type=MESH,
            ).wait_recv()

    def substitute(h):
        starts = [8 * (j // 2) + j % 2 + 4 * h for j in range(4)]
        left = jnp.concatenate([r2[pl.ds(j, 8, stride=16), :] for j in starts], axis=1)
        right = jnp.concatenate([r2[pl.ds(j + 2, 8, stride=16), :] for j in starts], axis=1)

        def spread(i, t):
            u[h, i] = u[h, i] + t
            return dtab[h, i] * t

        lax.fori_loop(0, 31, spread, left)
        u[h, 31] = right

        def backward(k, v):
            i = 30 - k
            v = dtab[h, i] * (v + u[h, i])
            u[h, i] = v
            return v

        lax.fori_loop(0, 31, backward, right)
        high, low = split(u[h].reshape(256, 512))
        uh[h] = high
        ul[h] = low

    def inverse_second(h):
        for copy in t1[h]:
            copy.wait_send()
        zb[h] = dot3(s_pair, (uh[h], ul[h]), NT).reshape(32, 16, 256)

    def send_last(h, lo, hi):
        for i in range(lo, hi):
            target, block = to_real(PEERS[i])
            t4[h].append(
                send(zb.at[h, block], gg.at[h, mid], s4.at[h, i], q4.at[h, mid], target)
            )

    tt = []

    def send_traces(part):
        sweeps = pl.ds(4 * part, 4)
        for side, ox in enumerate((-1, 1)):
            copy = prepare(
                trace.at[side, sweeps, pl.ds(8, 32), own],
                tin.at[1 - side, sweeps, pl.ds(8, 32), own],
                st.at[side, part], qt.at[1 - side, part], beside(ox, 0),
            )
            pl.when(has_x[side])(copy.start)
            tt.append((copy, has_x[side]))

    def send_corners():
        for side, ox in enumerate((-1, 1)):
            copy = prepare(
                trace.at[side, :, corner, own], tin.at[1 - side, :, corner, own], sx.at[side],
                qx.at[1 - side], beside(ox, 0),
            )
            sent = has_x[side] & middle
            pl.when(sent)(copy.start)
            tt.append((copy, sent))

    for s in range(32):
        arrived(dd.at[0], q1.at[0], s)
    second_and_eliminate(0)
    for s in range(32):
        arrived(dd.at[1], q1.at[1], s)
    second_and_eliminate(1)
    send_ends()
    send_traces(0)
    send_traces(1)
    send_corners()
    for k in range(1, 16):
        arrived(r1, q2, (pv + k) % 16)
    separators()
    wait_separators()
    for part in range(2):
        sweeps = pl.ds(4 * part, 4)
        for side in range(2):
            view = tin.at[side, sweeps, pl.ds(8, 32), own]
            copy = pltpu.make_async_remote_copy(
                src_ref=view, dst_ref=view, send_sem=st.at[side, part],
                recv_sem=qt.at[side, part], device_id=here, device_id_type=MESH,
            )
            pl.when(has_x[side])(copy.wait_recv)
    for side in range(2):
        copy = prepare(
            tin.at[side, :, corner, own], tin.at[side, :, corner, own], sx.at[side], qx.at[side],
            here,
        )
        pl.when(has_x[side] & middle)(copy.wait_recv)

        @pl.when(jnp.logical_not(has_x[side]))
        def _():
            tin[side, :, 8:40, own] = jnp.zeros((8, 32, 128), F32)

        @pl.when(jnp.logical_not(has_x[side]) & middle)
        def _():
            tin[side, :, corner, own] = jnp.zeros((8, 8, 128), F32)

        @pl.when(jnp.logical_not(has_y[side]))
        def _():
            tin[:, :, 40 * side : 40 * side + 8, own] = jnp.zeros((2, 8, 8, 128), F32)

    for k, oy in enumerate((-1, 1)):
        rows = pl.ds(8, 8) if oy < 0 else pl.ds(32, 8)
        to_rows = pl.ds(40, 8) if oy < 0 else pl.ds(0, 8)
        copy = prepare(
            tin.at[:, :, rows, own], tin.at[:, :, to_rows, own], sv.at[k], qv.at[k], beside(0, oy)
        )
        pl.when(turns[k])(copy.start)
        tt.append((copy, turns[k]))
    substitute(0)
    inverse_second(0)
    send_last(0, 0, CUT4A)
    substitute(1)
    face = []
    cut_x = []

    def faces(h):
        pair_h = (uh[h], ul[h])
        rows = dot3(split(wall[h]), pair_h, NN)
        face.append(rows[:64])
        cut_x.append(rows[64:])
        line = dot3(split(wys[...]), pair_h, NT)
        for f in range(2):
            for t in range(2):
                my[f, 2 * h + t : 2 * h + t + 1, :] = line[f : f + 1, 128 * t : 128 * t + 128]

    faces(0)
    faces(1)
    rows = jnp.concatenate([face[0] + face[1], cut_x[0], cut_x[1]], axis=0)
    rows = dot3(split(rows), (myh[...], myl[...]), NN)
    lane = lax.broadcasted_iota(jnp.int32, (8, 128), 1) // 16
    for f in range(2):
        for t in range(2):
            cols = slice(128 * t, 128 * t + 128)
            v = [rows[32 * f + 8 * k : 32 * f + 8 * k + 8, cols] for k in range(4)]
            for g in range(2):
                for h in range(2):
                    start = 64 + 16 * h + 8 * g
                    v.append(rows[start : start + 8, cols])
            for q, w in enumerate(exchange8(v, lane)):
                mzx[16 * f + 8 * t + q] = w
    tz = []
    for i, o in enumerate(PEERS):
        target, block = to_real(o)
        tz.append(send(mzx.at[block], rzx.at[mid], sz.at[i], qz.at[mid], target))
    for f in range(2):
        for g in range(2):
            tz.append(send(
                my.at[f], ry.at[mid], sy.at[2 * f + g], qy.at[mid],
                device(g, x, 7 * f, lv + 4 * f),
            ))
    send_last(0, CUT4A, 32)
    inverse_second(1)
    send_last(1, 0, CUT4B)
    for k in range(2):
        view = tin.at[:, :, pl.ds(40 - 40 * k, 8), own]
        copy = pltpu.make_async_remote_copy(
            src_ref=view, dst_ref=view, send_sem=sv.at[k], recv_sem=qv.at[k], device_id=here,
            device_id_type=MESH,
        )
        pl.when(turns[1 - k])(copy.wait_recv)
    view = tin.at[:, :, :, own]
    te = send(view, view, se.at[0], qe.at[0], partner)
    te.wait_recv()
    def factor(k):
        inside_x = (k + 8 * gx >= 8) & (k + 8 * gx < 136)
        return jnp.where(inside_x, sixth, 0.0)

    ends = (jnp.where(gx == 0, 0.0, sixth), jnp.where(gx == 15, 0.0, sixth))
    for k in (4, 5, 6, 7, 16, 17, 18, 19):
        es[k] = jnp.zeros((48, 256), F32)
        ed[k] = jnp.zeros((48, 256), F32)
    for k in (3, 4, 5, 6, 17, 18, 19, 20):
        et[k] = jnp.zeros((48, 256), F32)
    for k in range(8, 16):
        ed[k] = fr[k - 7]
    for j in range(8):
        source, target = ((es, et), (et, es))[j % 2]
        depth = min(j + 1, 7 - j)

        def some(k, c, source=source, target=target, first=8 - depth, step=WIDE):
            for m in range(step):
                index = first + step * k + m
                target[index] = layer(source, ed, index) * factor(index)
            return c

        layers = 8 + 2 * depth
        lax.fori_loop(0, layers // WIDE, some, 0)
        if layers % WIDE:
            some(0, 0, first=8 - depth + layers // WIDE * WIDE, step=layers % WIDE)
        target[8] = target[8] + tin[0, j] * ends[0]
        target[15] = target[15] + tin[1, j] * ends[1]
    for s in range(32):
        arrived(rzx, qz, s)
    zsum = rzx[0]
    for s in range(1, 32):
        zsum = zsum + rzx[s]
    row = lax.broadcasted_iota(jnp.int32, (128, 512), 0)
    col = lax.broadcasted_iota(jnp.int32, (128, 512), 1)
    tile = jnp.where(row == col // 128 * 16 + col % 16, 1.0, 0.0)
    spread_z = full(zsum, tile, NN)
    spread_z = jnp.concatenate([spread_z[:, 128 * h : 128 * h + 128] for h in range(4)], axis=0)
    lane32 = lax.broadcasted_iota(jnp.int32, (32, 128), 1) // 16
    spread_z = jnp.concatenate(
        [jnp.where(lane32 == k, spread_z, 0.0) for k in range(8)], axis=0
    )
    row = lax.broadcasted_iota(jnp.int32, (16, 256), 0)
    col = lax.broadcasted_iota(jnp.int32, (16, 256), 1)
    pick = jnp.where(a0 - 3 + 2 * row + col // 32 == 32 * gx + col % 32, 1.0, 0.0)
    rows = full(pick, spread_z, NN)
    for q in range(16):
        m5[q] = rows[q : q + 1]
    t5 = []
    for k in range(1, 16):
        q = (gx + k) % 16
        t5.append(send(m5.at[q], r5.at[gx], s5.at[k], q5.at[gx], real_row(q)))
    r5[gx] = m5[gx]
    got = rzx[...].reshape(256, 128)
    parts = [full(got, mz[256 * k : 256 * k + 256, :], TN) for k in range(2)]
    left_half = lax.broadcasted_iota(jnp.int32, (8, 128), 1) < 64
    for f in range(2):
        cells_x = parts[0][64 + 32 * f : 80 + 32 * f] + parts[1][80 + 32 * f : 96 + 32 * f]
        m6[f] = jnp.where(left_half, cells_x[:8], pltpu.roll(cells_x[8:], 64, 1))
    for f in range(2):
        end = 15 * f
        copy = prepare(m6.at[f], r6.at[gx], s6.at[f], q6.at[gx], real_row(end))
        pl.when(gx != end)(copy.start)

        @pl.when(gx == end)
        def _():
            r6[gx] = m6[f]

    at_y = (gy == 0) | (gy == 15)

    @pl.when(at_y)
    def _():
        for s in range(32):
            arrived(ry, qy, s)
        lane8 = lax.broadcasted_iota(jnp.int32, (32, 128), 1) % 8
        group = lax.broadcasted_iota(jnp.int32, (16, 128), 0)
        member = lax.broadcasted_iota(jnp.int32, (16, 128), 1) // 8
        gather = jnp.where(group == member, 1.0, 0.0)
        part = []
        for t in range(2):
            total = None
            for h in range(2):
                v = ry[:, 2 * h + t, :]
                v = jnp.concatenate([jnp.where(lane8 == k, v, 0.0) for k in range(8)], axis=0)
                modes = jnp.concatenate(
                    [mz[pl.ds(256 * h + k, 32, stride=8), :] for k in range(8)], axis=0
                )
                w = full(v, modes, TN)
                total = w if total is None else total + w
            part.append(full(gather, total, NN))
        row = lax.broadcasted_iota(jnp.int32, (128, 32), 0)
        col = lax.broadcasted_iota(jnp.int32, (128, 32), 1)
        pick = jnp.where(a0 - 3 + 2 * (row // 8) + row % 8 == 32 * gx + col, 1.0, 0.0)
        m7[...] = full(pick, jnp.concatenate(part, axis=0), NN).reshape(16, 8, 128)
        for k in range(1, 16):
            q = (gx + k) % 16
            send(m7.at[q], r7.at[gx], s7.at[k], q7.at[gx], real_row(q))
        r7[gx] = m7[gx]

    send_last(1, CUT4B, 32)
    for s in range(32):
        arrived(gg.at[0], q4.at[0], s)
    def inverse_third(h):
        swap_groups(gg.at[h], za, 0, 256 * h)
        rows_h = tuple(part[halves[h], :] for part in s_pair)
        return dot3(split(za[:, :, halves[h]].reshape(512, 256)), rows_h, NN).reshape(32, 16, 512)

    out_ref[...] = inverse_third(0)
    for k in range(1, 16):
        arrived(r5, q5, (gx + k) % 16)
    def interpolate(fine, cell):
        scaled = 2 * fine + 5
        bottom = scaled // 8
        t = (scaled % 8).astype(F32) * 0.125
        return jnp.where(cell == bottom, 1.0 - t, 0.0) + jnp.where(cell == bottom + 1, t, 0.0)

    def grid(shape):
        return (lax.broadcasted_iota(jnp.int32, shape, 0), lax.broadcasted_iota(jnp.int32, shape, 1))

    row, col = grid((24, 8))
    int_x = interpolate(row, col)
    row, col = grid((128, 128))
    int_y = jnp.where(row < 48, interpolate(row, col % 16), 0.0)
    zb5 = r5[0]
    for s in range(1, 16):
        zb5 = zb5 + r5[s]
    row, col = grid((8, 128))
    zb5 = jnp.where(row == col // 16, jnp.broadcast_to(zb5, (8, 128)), 0.0)
    ghost_z = full(full(int_x, zb5, NN), int_y, NT)
    row, col = grid((24, 128))
    inside = (row + 8 * gx >= 8) & (row + 8 * gx < 136) & (col < 48)
    inside = inside & (col + 32 * gy >= 8) & (col + 32 * gy < 520)
    sixth_z = jnp.where(inside, 1.0 / 6.0, 0.0)
    plane = []
    for j in range(8):
        new = []
        for k in range(j + 1):
            total = ghost_z if k == 0 else plane[k - 1]
            if k + 1 < j:
                total = total + plane[k + 1]
            if k < j:
                v = plane[k]
                total = total + (pltpu.roll(v, 1, 0) + pltpu.roll(v, 23, 0))
                total = total + (pltpu.roll(v, 1, 1) + pltpu.roll(v, 127, 1))
            new.append(total * sixth_z)
        plane = new
    for k in range(8):
        gz[pl.ds(k, 24, stride=8), :] = plane[k]
    row, col = grid((8, 128))
    place = jnp.where(col == jnp.where(core == 0, row, 127 - row), 1.0, 0.0)
    for k in range(8):
        part = full(gz[8 * (k + 8) : 8 * (k + 8) + 8, :], place, TN)
        fine_ref[k] = es[k + 8, 8:40, own] + part[8:40]

    row, col = grid((128, 256))
    int_z = jnp.where(row < 64, interpolate(col, row + 30 * core), 0.0)

    for copy in t2 + t4[0] + t4[1] + tz + t5 + [te]:
        copy.wait_send()
    for copy, sent, *_ in halo + tt:
        pl.when(sent)(copy.wait_send)
    @pl.when(at_y)
    def _():
        for k in range(1, 16):
            prepare(m7.at[k], r7.at[gx], s7.at[k], q7.at[gx], here).wait_send()

    for f in range(2):
        @pl.when(gx != 15 * f)
        def _():
            pltpu.make_async_remote_copy(
                src_ref=m6.at[f], dst_ref=r6.at[gx], send_sem=s6.at[f], recv_sem=q6.at[gx],
                device_id=real_row(15 * f), device_id_type=MESH,
            ).wait_send()

    for s in range(32):
        arrived(gg.at[1], q4.at[1], s)
    out_ref[...] = out_ref[...] + inverse_third(1)
    row8 = lax.broadcasted_iota(jnp.int32, (8, 256), 0)
    col8 = lax.broadcasted_iota(jnp.int32, (8, 256), 1)
    for f in range(2):
        @pl.when(gy == 15 * f)
        def _():
            for k in range(1, 16):
                arrived(r7, q7, (gx + k) % 16)
            yb7 = r7[0]
            for k in range(1, 16):
                yb7 = yb7 + r7[k]
            ghost_y = full(full(int_x, yb7, NN), int_z, NN)
            edge = 7 * f
            for k in range(24):
                yd[k] = jnp.where(row8 == edge, ghost_y[k : k + 1], 0.0)
            for j in range(8):
                source, target = ((ya, yb), (yb, ya))[j % 2]

                def one(k, c, source=source, target=target, j=j):
                    total = yd[k]
                    if j:
                        v = source[k]
                        total = total + source[k - 1] + source[k + 1]
                        total = total + jnp.where(row8 == 0, 0.0, pltpu.roll(v, 1, 0))
                        total = total + jnp.where(row8 == 7, 0.0, pltpu.roll(v, 7, 0))
                        total = total + jnp.where(col8 == 0, 0.0, pltpu.roll(v, 1, 1))
                        total = total + jnp.where(col8 == 255, 0.0, pltpu.roll(v, 255, 1))
                    inside_x = (k + 8 * gx >= 8) & (k + 8 * gx < 136)
                    target[k] = total * jnp.where(inside_x, 1.0 / 6.0, 0.0)
                    return c

                for k in range(j + 1, 23 - j):
                    one(k, 0)
            rows = pl.ds(24 * f, 8)
            for k in range(8):
                fine_ref[k, rows, :] = fine_ref[k, rows, :] + ya[k + 8, :, own]

    for f in range(2):
        @pl.when(gx == 15 * f)
        def _():
            for k in range(16):
                if k != 15 * f:
                    arrived(r6, q6, k)
            xb6 = r6[0]
            for s in range(1, 16):
                xb6 = xb6 + r6[s]
            row, col = grid((48, 8))
            near_y = full(interpolate(row, col), xb6, NN)
            far_y = full(interpolate(row, col + 8), xb6, NN)
            row, col = grid((48, 128))
            ghost_x = full(jnp.where(col < 64, near_y + pltpu.roll(far_y, 64, 1), 0.0), int_z, NN)
            for k in range(1, 9):
                fr[k] = jnp.zeros((48, 256), F32)
                fa[k] = jnp.zeros((48, 256), F32)
                fb[k] = jnp.zeros((48, 256), F32)
            fr[1 + 7 * f] = ghost_x
            for j in range(8):
                source, target = ((fa, fb), (fb, fa))[j % 2]
                for k in range(j + 1):
                    index = 8 - k if f else 1 + k
                    target[index] = layer(source, fr, index) * sixth
            for k in range(8):
                fine_ref[k] = fine_ref[k] + fa[k + 1, 8:40, own]


def store(potential, fine, potential_out, fine_out, sem):
    copies = [
        pltpu.make_async_copy(potential, potential_out, sem.at[0]),
        pltpu.make_async_copy(fine, fine_out, sem.at[1]),
    ]
    for copy in copies:
        copy.start()
    for copy in copies:
        copy.wait()


def body(density, fine_density, fine_start, anchor):
    high, low, lam = tables()
    vm = pl.BlockSpec(memory_space=pltpu.VMEM)
    dma = pltpu.SemaphoreType.DMA

    def f32(*shape):
        return pltpu.VMEM(shape, F32)

    def b16(*shape):
        return pltpu.VMEM(shape, BF16)

    big = f32(32, 16, 512)
    results = pl.pallas_call(
        kernel,
        out_shape=(
            pltpu.VMEM((32, 16, 512), F32), pltpu.VMEM((8, 32, 128), F32)
        ),
        in_specs=[pl.BlockSpec(memory_space=pl.ANY)] * 9,
        out_specs=(vm, vm),
        scratch_shapes=[
            pltpu.SMEM((3,), jnp.int32), f32(8, 512), f32(2, 8, 128), f32(8, 128),
            big, f32(8, 32, 128), f32(8, 32, 128), b16(512, 512), b16(512, 512),
            big, f32(2, 32, 16, 256), f32(2, 32, 16, 256), f32(2, 32, 16, 256),
            f32(2, 32, 8, 512), f32(2, 31, 8, 512),
            f32(128, 128), f32(16, 8, 128), f32(16, 8, 128), f32(128, 128),
            f32(2, 16, 2, 128), f32(2, 2, 128),
            b16(2, 256, 512), b16(2, 256, 512), b16(512, 256), b16(512, 256),
            f32(512, 128), f32(2, 80, 256), f32(16, 512),
            f32(32, 8, 128), f32(32, 8, 128), f32(2, 4, 128), f32(32, 4, 128),
            f32(16, 1, 128), f32(16, 1, 128), f32(2, 8, 128), f32(16, 8, 128),
            f32(16, 8, 128), f32(16, 8, 128),
            f32(24, 48, 256), f32(24, 48, 256), f32(24, 48, 256),
            f32(10, 48, 256), f32(10, 48, 256), f32(10, 48, 256),
            f32(2, 8, 48, 256), f32(2, 8, 48, 256), f32(192, 128),
            f32(24, 8, 256), f32(24, 8, 256), f32(24, 8, 256),
            dma((2, 32)), dma((2, 32)), dma((16,)), dma((16,)), dma((16,)), dma((16,)),
            dma((2, 32)), dma((2, 32)), dma((4,)), dma((4,)), dma((2,)), dma((2,)),
            dma((32,)), dma((32,)), dma((4,)), dma((32,)), dma((16,)), dma((16,)),
            dma((2,)), dma((16,)), dma((10,)), dma((2, 2)), dma((2, 2)), dma((1,)), dma((1,)), dma((2,)), dma((2,)),
            dma((2,)), dma((2,)), dma((16,)), dma((16,)),
        ],
        compiler_params=pltpu.CompilerParams(
            collective_id=0, has_side_effects=True, vmem_limit_bytes=56 << 20
        ),
    )(anchor, jnp.asarray(np.tile(lam.reshape(1, 512), (8, 1))),
      jnp.asarray(np.tile(lam.reshape(512, 1), (1, 128))),
      jnp.asarray(np.tile(lam.reshape(4, 128), (2, 1))), density, fine_density, fine_start,
      jnp.asarray(high), jnp.asarray(low))
    return pl.pallas_call(
        store,
        out_shape=(
            jax.ShapeDtypeStruct((32, 16, 512), F32), jax.ShapeDtypeStruct((8, 32, 128), F32)
        ),
        in_specs=[vm] * 2,
        out_specs=(pl.BlockSpec(memory_space=pl.ANY),) * 2,
        scratch_shapes=[dma((2,))],
        compiler_params=pltpu.CompilerParams(vmem_limit_bytes=4 << 20),
    )(*results)


def solution(mesh):
    return jax.shard_map(
        body,
        mesh=mesh,
        in_specs=(P("gx", ("grp", "gy"), None), P("gx", "gy", "grp"), P("gx", "gy", "grp"), P()),
        out_specs=(P("gx", ("grp", "gy"), None), P("gx", "gy", "grp")),
        check_vma=False,
    )
```
